32 devices in a mesh: dp: 1 (over z), pool: 4 (over y), ep: 8 (over x, core).
Axes of the slice: x: 4, y: 4, z: 1, core: 2. Of those that a mesh axis runs over, the one named last changes fastest.
The devices are a block of a 4x4x8 slice.
Arguments:
- hidden_in: bfloat16 [512, 1024], P(('dp', 'ep'))
- k_cache: bfloat16 [2, 512, 1024, 2, 128], P(None, ('dp', 'ep'), 'pool')
- v_cache: bfloat16 [2, 512, 1024, 2, 128], P(None, ('dp', 'ep'), 'pool')
- cache_len: int32 [512], P(('dp', 'ep'))
- w_q: bfloat16 [2, 1024, 1024], replicated
- w_k: bfloat16 [2, 1024, 256], replicated
- w_v: bfloat16 [2, 1024, 256], replicated
- w_o: bfloat16 [2, 1024, 1024], replicated
- w_router: float32 [2, 1024, 8], replicated
- expert_ids: int32 [2, 512, 2], P(None, ('dp', 'ep'))
- w_one: bfloat16 [2, 8, 1024, 3584], P(None, 'ep', None, 'pool')
- w_three: bfloat16 [2, 8, 1024, 3584], P(None, 'ep', None, 'pool')
- w_two: bfloat16 [2, 8, 3584, 1024], P(None, 'ep', 'pool')
Outputs:
- output: bfloat16 [512, 1024], P(('dp', 'ep'))
All inputs are finite; a program needn't handle non-finite values.
Results may differ from the reference program's by a relative error of at most 0.02.
Values are sent between devices in bfloat16 or wider.
A program may use at most 768 MiB of HBM per device.

```python
import jax
import jax.numpy as jnp
from jax import lax

D_MODEL = 1024
N_HEADS = 8
KV_HEADS = 2
HEAD_DIM = 128
N_EXPERTS = 8
TOP_K = 2
FF_DIM = 3584
NUM_LAYERS = 2
EP_GROUP = 8
BATCH_TOK = 512
SEQ_LEN = 1024

GROUP_SIZE = N_HEADS // KV_HEADS
LOCAL_EXP = N_EXPERTS // EP_GROUP
TOK_SHARD = BATCH_TOK // EP_GROUP


def draw_ids(rkey):
    k_shift, k_first, k_second = jax.random.split(rkey, 3)
    shift_dev = jax.random.randint(k_shift, (NUM_LAYERS, EP_GROUP, 1, 1), 0, EP_GROUP)
    pair_idx = jnp.arange(TOK_SHARD)[:, None] * TOP_K + jnp.arange(TOP_K)[None, :]
    dest_dev = (pair_idx[None, None] + shift_dev) % EP_GROUP
    first_draw = jax.random.randint(k_first, (NUM_LAYERS, EP_GROUP, TOK_SHARD, 1), 0, LOCAL_EXP)
    second_draw = jax.random.randint(k_second, (NUM_LAYERS, EP_GROUP, TOK_SHARD, 1), 0, LOCAL_EXP)
    start_exp = (first_draw * second_draw) // LOCAL_EXP
    local_id = (start_exp + jnp.arange(TOP_K)[None, None, None, :] // EP_GROUP) % LOCAL_EXP
    chosen = dest_dev * LOCAL_EXP + local_id
    return chosen.reshape(NUM_LAYERS, BATCH_TOK, TOP_K).astype(jnp.int32)


def draw_lens(lkey):
    lens_drawn = jax.random.randint(lkey, (BATCH_TOK,), 1, SEQ_LEN + 1)
    return lens_drawn.at[0].set(SEQ_LEN).astype(jnp.int32)


def setup_inputs(seed: int = 0, part: int = 0) -> dict:
    base_key = jax.random.key(seed)
    part_key = jax.random.fold_in(base_key, part)
    share_keys = jax.random.split(base_key, 8)
    part_keys = jax.random.split(part_key, 5)
    attn_in = N_HEADS * HEAD_DIM
    kv_in = KV_HEADS * HEAD_DIM
    cache_shape = (NUM_LAYERS, BATCH_TOK, SEQ_LEN, KV_HEADS, HEAD_DIM)
    hidden_in = jax.random.normal(part_keys[0], (BATCH_TOK, D_MODEL), jnp.float32).astype(jnp.bfloat16)
    k_cache = jax.random.normal(part_keys[1], cache_shape, jnp.float32).astype(jnp.bfloat16)
    v_cache = jax.random.normal(part_keys[2], cache_shape, jnp.float32).astype(jnp.bfloat16)
    cache_len = draw_lens(part_keys[3])
    expert_ids = draw_ids(part_keys[4])
    w_q = (jax.random.normal(share_keys[0], (NUM_LAYERS, D_MODEL, attn_in), jnp.float32) * (2.0 * D_MODEL ** -0.5)).astype(jnp.bfloat16)
    w_k = (jax.random.normal(share_keys[1], (NUM_LAYERS, D_MODEL, kv_in), jnp.float32) * D_MODEL ** -0.5).astype(jnp.bfloat16)
    w_v = (jax.random.normal(share_keys[2], (NUM_LAYERS, D_MODEL, kv_in), jnp.float32) * D_MODEL ** -0.5).astype(jnp.bfloat16)
    w_o = (jax.random.normal(share_keys[3], (NUM_LAYERS, attn_in, D_MODEL), jnp.float32) * (2.0 * attn_in ** -0.5)).astype(jnp.bfloat16)
    w_router = jax.random.normal(share_keys[4], (NUM_LAYERS, D_MODEL, N_EXPERTS), jnp.float32) * (1.5 * D_MODEL ** -0.5)
    w_one = (jax.random.normal(share_keys[5], (NUM_LAYERS, N_EXPERTS, D_MODEL, FF_DIM), jnp.float32) * D_MODEL ** -0.5).astype(jnp.bfloat16)
    w_three = (jax.random.normal(share_keys[6], (NUM_LAYERS, N_EXPERTS, D_MODEL, FF_DIM), jnp.float32) * D_MODEL ** -0.5).astype(jnp.bfloat16)
    w_two = (jax.random.normal(share_keys[7], (NUM_LAYERS, N_EXPERTS, FF_DIM, D_MODEL), jnp.float32) * (2.0 * FF_DIM ** -0.5)).astype(jnp.bfloat16)
    return dict(hidden_in=hidden_in, k_cache=k_cache, v_cache=v_cache, cache_len=cache_len, w_q=w_q, w_k=w_k, w_v=w_v, w_o=w_o, w_router=w_router, expert_ids=expert_ids, w_one=w_one, w_three=w_three, w_two=w_two)


def rms_norm(in_vals):
    in_vals = in_vals.astype(jnp.float32)
    return in_vals * lax.rsqrt(jnp.mean(in_vals * in_vals, axis=-1, keepdims=True) + 1e-6)


def attend_token(packed):
    q_tok, k_new, v_new, k_rows, v_rows, valid_len = packed
    att_scale = HEAD_DIM ** -0.5
    q_grp = q_tok.reshape(KV_HEADS, GROUP_SIZE, HEAD_DIM).astype(jnp.float32)
    score_vals = jnp.einsum('gqd,sgd->gqs', q_grp, k_rows.astype(jnp.float32)) * att_scale
    pos_mask = jnp.arange(SEQ_LEN) < valid_len
    score_vals = jnp.where(pos_mask[None, None, :], score_vals, -1e30)
    new_score = jnp.einsum('gqd,gd->gq', q_grp, k_new.astype(jnp.float32)) * att_scale
    top_score = jnp.maximum(jnp.max(score_vals, axis=-1), new_score)
    prob_vals = jnp.exp(score_vals - top_score[..., None])
    new_prob = jnp.exp(new_score - top_score)
    denom_sum = jnp.sum(prob_vals, axis=-1) + new_prob
    numer_sum = jnp.einsum('gqs,sgd->gqd', prob_vals.astype(jnp.bfloat16).astype(jnp.float32), v_rows.astype(jnp.float32))
    numer_sum = numer_sum + new_prob[..., None] * v_new.astype(jnp.float32)[:, None, :]
    return (numer_sum / denom_sum[..., None]).reshape(N_HEADS * HEAD_DIM)


def moe_experts(u_rows, ids_layer, w_one, w_three, w_two):
    flat_ids = ids_layer.reshape(-1)
    sort_order = jnp.argsort(flat_ids, stable=True)
    tok_rows = u_rows[sort_order // TOP_K].astype(jnp.float32)
    group_sizes = jnp.bincount(flat_ids, length=N_EXPERTS).astype(jnp.int32)
    h_one = lax.ragged_dot(tok_rows, w_one.astype(jnp.float32), group_sizes)
    h_three = lax.ragged_dot(tok_rows, w_three.astype(jnp.float32), group_sizes)
    act_rows = (jax.nn.silu(h_one) * h_three).astype(jnp.bfloat16).astype(jnp.float32)
    out_rows = lax.ragged_dot(act_rows, w_two.astype(jnp.float32), group_sizes).astype(jnp.bfloat16)
    back_order = jnp.argsort(sort_order)
    return out_rows[back_order].reshape(BATCH_TOK, TOP_K, D_MODEL)


def reference(hidden_in, k_cache, v_cache, cache_len, w_q, w_k, w_v, w_o, w_router, expert_ids, w_one, w_three, w_two):
    def layer_step(hidden, layer_in):
        kc_l, vc_l, wq_l, wk_l, wv_l, wo_l, wr_l, ids_l, w1_l, w3_l, w2_l = layer_in
        normed = rms_norm(hidden).astype(jnp.bfloat16)
        q_rows = jnp.dot(normed, wq_l, preferred_element_type=jnp.float32).astype(jnp.bfloat16)
        k_new = jnp.dot(normed, wk_l, preferred_element_type=jnp.float32).astype(jnp.bfloat16).reshape(BATCH_TOK, KV_HEADS, HEAD_DIM)
        v_new = jnp.dot(normed, wv_l, preferred_element_type=jnp.float32).astype(jnp.bfloat16).reshape(BATCH_TOK, KV_HEADS, HEAD_DIM)
        attn_out = lax.map(attend_token, (q_rows, k_new, v_new, kc_l, vc_l, cache_len)).astype(jnp.bfloat16)
        resid_rows = (hidden.astype(jnp.float32) + jnp.dot(attn_out, wo_l, preferred_element_type=jnp.float32)).astype(jnp.bfloat16)
        u_rows = rms_norm(resid_rows).astype(jnp.bfloat16)
        logits = jnp.dot(u_rows.astype(jnp.float32), wr_l)
        gate_vals = jax.nn.softmax(jnp.take_along_axis(logits, ids_l, axis=1), axis=-1)
        pair_rows = moe_experts(u_rows, ids_l, w1_l, w3_l, w2_l)
        mixed_sum = jnp.sum(gate_vals[..., None] * pair_rows.astype(jnp.float32), axis=1)
        return (resid_rows.astype(jnp.float32) + mixed_sum).astype(jnp.bfloat16), None
    hidden_out, unused_ys = lax.scan(layer_step, hidden_in, (k_cache, v_cache, w_q, w_k, w_v, w_o, w_router, expert_ids, w_one, w_three, w_two))
    return hidden_out
```

```python
import functools

import jax
import jax.numpy as jnp
from jax import lax
from jax.experimental import pallas as pl
from jax.experimental.pallas import tpu as pltpu
from jax.sharding import PartitionSpec as P

MESH = pl.DeviceIdType.MESH
NORM_EPS = 1e-6
NEG = -1e30
BF = jnp.bfloat16
F32 = jnp.float32
NT = (((1,), (1,)), ((), ()))


def rms_norm(v):
    return v * lax.rsqrt(jnp.mean(v * v, axis=-1, keepdims=True) + NORM_EPS)


def dot(a, b):
    return jnp.dot(a, b, preferred_element_type=F32)


def layers_kernel(dims, len_ref, x_hbm, ids_ref, k_hbm, v_hbm, wq_hbm, wk_hbm, wv_hbm, wo_hbm, wr_ref,
                  w1_hbm, w3_hbm, w2_hbm, out_ref,
                  xb, xs, wqkv, kbuf, vbuf, wob, w1b, w3b, w2b, qrows, kvs, kx, vx, zst, msg, arx, orow, oag,
                  a_s, uperm, xin, act, ysend, yrecv, ybf, yret, dmat, rmat, wr3,
                  ld_sem, kv_sem, att_s, att_r, og_s, og_r, dis_s, dis_r, ys_s, ys_r, ret_s, ret_r):
    L, T, D, S, G, HD, NH, NP, NE, TC, K, FF = dims
    QG = NH // G
    SLOTS = T * K
    RE = SLOTS // NE
    CB = D // NP
    ROWS = TC * NH
    SG = S * G
    QW = NH * HD
    KW = G * HD
    scale = HD ** -0.5
    p = lax.axis_index("pool")
    e = lax.axis_index("ep")

    def pool_of(d):
        return lax.rem(p + d, NP)

    def ep_of(d):
        return lax.rem(e + d, NE)

    barrier = pltpu.get_barrier_semaphore()
    for dp_ in range(NP):
        for de in range(NE):
            if dp_ or de:
                pl.semaphore_signal(barrier, inc=1, device_id={"pool": pool_of(dp_), "ep": ep_of(de)},
                                    device_id_type=MESH)

    def qkv_copies(l):
        return [pltpu.make_async_copy(wq_hbm.at[l], wqkv.at[:, pl.ds(0, QW)], ld_sem.at[0]),
                pltpu.make_async_copy(wk_hbm.at[l], wqkv.at[:, pl.ds(QW, KW)], ld_sem.at[1]),
                pltpu.make_async_copy(wv_hbm.at[l], wqkv.at[:, pl.ds(QW + KW, KW)], ld_sem.at[2])]

    def kv_copies(l, i):
        c = pool_of(i + 1)
        tok = pl.ds(pl.multiple_of(c * TC, TC), TC)
        return [pltpu.make_async_copy(k_hbm.at[l, tok], kbuf.at[i], kv_sem.at[0, i]),
                pltpu.make_async_copy(v_hbm.at[l, tok], vbuf.at[i], kv_sem.at[1, i])]

    def wo_copies(l):
        return [pltpu.make_async_copy(wo_hbm.at[l], wob, ld_sem.at[3])]

    def up_copies(l):
        return [pltpu.make_async_copy(w1_hbm.at[l, 0], w1b, ld_sem.at[4]),
                pltpu.make_async_copy(w3_hbm.at[l, 0], w3b, ld_sem.at[5])]

    def down_copies(l):
        return [pltpu.make_async_copy(w2_hbm.at[l, 0, :, pl.ds(q * CB, CB)], w2b.at[q], ld_sem.at[6 + q])
                for q in range(NP)]

    def start(copies):
        for c in copies:
            c.start()

    def wait(copies):
        for c in copies:
            c.wait()

    xcopy = pltpu.make_async_copy(x_hbm, xb, ld_sem.at[6 + NP])
    xcopy.start()
    start(qkv_copies(0))
    for i in range(NP):
        start(kv_copies(0, i))
    start(wo_copies(0))
    start(up_copies(0))
    start(down_copies(0))

    slot_col = lax.broadcasted_iota(jnp.int32, (SLOTS, SLOTS), 0)
    pair_row = lax.broadcasted_iota(jnp.int32, (SLOTS, SLOTS), 1)
    upper = (slot_col < pair_row).astype(F32).astype(BF)
    want_rank = lax.rem(slot_col, RE).astype(F32)
    for l in range(L):
        idrow = jnp.concatenate([ids_ref[l, k:k + 1, :] for k in range(K)], axis=1)
        same = (jnp.broadcast_to(idrow, (SLOTS, SLOTS)) == lax.div(slot_col, RE))
        rank = dot(same.astype(F32).astype(BF), upper)
        pick = jnp.where(jnp.logical_and(same, rank == want_rank), 1.0, 0.0).astype(F32)
        rmat[l] = pick.T.astype(BF)
        tot = pick[:, 0:T]
        for k in range(1, K):
            tot = tot + pick[:, k * T:(k + 1) * T]
        dmat[l] = tot.astype(BF)
        wr = wr_ref[l]
        hi = wr.astype(BF).astype(F32)
        mid = (wr - hi).astype(BF).astype(F32)
        lo = wr - hi - mid
        wr3[l] = jnp.concatenate([hi, mid, lo, jnp.zeros_like(lo)], axis=0).astype(BF)

    hrow = lax.broadcasted_iota(jnp.int32, (NH, SG), 0)
    pcol = lax.broadcasted_iota(jnp.int32, (NH, SG), 1)
    posm = jnp.where(lax.rem(pcol, G) == lax.div(hrow, QG), lax.div(pcol, G), jnp.int32(1 << 30))
    lane = lax.broadcasted_iota(jnp.int32, (NH, HD), 1)
    ecol = lax.broadcasted_iota(jnp.int32, (wr_ref.shape[1], T), 0)

    xcopy.wait()
    xs[...] = xb[...].astype(F32)

    def layer(l, carry):
        more = l + 1 < L
        wait(qkv_copies(l))
        hn = rms_norm(xs[...]).astype(BF)
        for b in range((QW + 2 * KW) // (2 * HD)):
            r = dot(hn, wqkv[:, b * 2 * HD:(b + 1) * 2 * HD]).astype(BF).astype(F32)
            if b * 2 * HD < QW:
                for j in range(2):
                    qrows[pl.ds(2 * b + j, T, stride=NH), :] = r[:, j * HD:(j + 1) * HD]
            else:
                kvs[:, b * 2 * HD - QW:(b + 1) * 2 * HD - QW] = r

        @pl.when(more)
        def _():
            start(qkv_copies(l + 1))

        own_tok = pl.ds(pl.multiple_of(p * TC, TC), TC)
        for h in range(NH):
            g = h // QG
            kx[pl.ds(h, TC, stride=NH), :] = kvs[own_tok, g * HD:(g + 1) * HD]
            vx[pl.ds(h, TC, stride=NH), :] = kvs[own_tok, KW + g * HD:KW + (g + 1) * HD]

        @pl.when(l == 0)
        def _():
            pl.semaphore_wait(barrier, NP * NE - 1)

        def att_send(i):
            return pltpu.make_async_remote_copy(
                src_ref=msg.at[l, i], dst_ref=arx.at[l, i], send_sem=att_s.at[l, i], recv_sem=att_r.at[l, i],
                device_id={"pool": pool_of(i + 1), "ep": e}, device_id_type=MESH)

        def chunk(i, c2):
            c = pool_of(i + 1)
            wait(kv_copies(l, i))
            for j0 in range(0, TC, 8):
                sc = []
                for j in range(j0, j0 + 8):
                    t = c * TC + j
                    qt = qrows[pl.ds(pl.multiple_of(t * NH, NH), NH), :].astype(BF)
                    s = lax.dot_general(qt, kbuf[i, j], NT, preferred_element_type=F32) * scale
                    sc.append(jnp.where(posm < len_ref[t] - p * S, s, NEG))
                mx = [jnp.max(s, axis=1, keepdims=True) for s in sc]
                pr = [jnp.exp(s - m) for s, m in zip(sc, mx)]
                ls = [jnp.sum(q, axis=1, keepdims=True) for q in pr]
                for n, j in enumerate(range(j0, j0 + 8)):
                    msg[l, i, j * NH:(j + 1) * NH, :] = dot(pr[n].astype(BF), vbuf[i, j])
                    zst[j * NH:(j + 1) * NH, :] = jnp.where(lane == 0, mx[n], ls[n])
            msg[l, i, ROWS:ROWS + 8, :] = zst[...].T[0:8, :]

            @pl.when(i < NP - 1)
            def _():
                att_send(i).start()

            @pl.when(more)
            def _():
                start(kv_copies(l + 1, i))

            return c2

        lax.fori_loop(0, NP, chunk, 0)

        q_own = qrows[pl.ds(pl.multiple_of(p * ROWS, ROWS), ROWS), :]
        s_new = jnp.sum(q_own * kx[...], axis=1, keepdims=True) * scale
        for i in range(NP - 1):
            att_send(i).wait_recv()
            zst[8 * i:8 * i + 8, :] = arx[l, i, ROWS:ROWS + 8, :]
        zst[8 * (NP - 1):8 * NP, :] = msg[l, NP - 1, ROWS:ROWS + 8, :]
        zc = zst[...].T
        ms = [zc[:, 8 * i:8 * i + 1] for i in range(NP)]
        top = s_new
        for m in ms:
            top = jnp.maximum(top, m)
        p_new = jnp.exp(s_new - top)
        den = p_new
        num = p_new * vx[...]
        for i in range(NP):
            w = jnp.exp(ms[i] - top)
            den = den + w * zc[:, 8 * i + 1:8 * i + 2]
            num = num + w * (arx[l, i, 0:ROWS, :] if i < NP - 1 else msg[l, i, 0:ROWS, :])
        orow[...] = num / den
        for h in range(NH):
            oag[l, own_tok, h * HD:(h + 1) * HD] = orow[pl.ds(h, TC, stride=NH), :].astype(BF)

        def og_send(d):
            return pltpu.make_async_remote_copy(
                src_ref=oag.at[l, own_tok], dst_ref=oag.at[l, own_tok], send_sem=og_s.at[l, d - 1],
                recv_sem=og_r.at[l, d - 1], device_id={"pool": pool_of(d), "ep": e}, device_id_type=MESH)

        for d in range(1, NP):
            og_send(d).start()
        wait(wo_copies(l))
        for d in range(1, NP):
            og_send(d).wait_recv()

        for b in range(NP):
            cols = slice(b * CB, (b + 1) * CB)
            a_s[:, cols] = (xs[:, cols] + dot(oag[l], wob[:, cols])).astype(BF).astype(F32)

        @pl.when(more)
        def _():
            start(wo_copies(l + 1))

        u = rms_norm(a_s[...]).astype(BF)
        for b in range(NP):
            cols = slice(b * CB, (b + 1) * CB)
            uperm[l, :, cols] = dot(dmat[l], u[:, cols]).astype(BF)

        def dis_send(d):
            dst = ep_of(d)
            return pltpu.make_async_remote_copy(
                src_ref=uperm.at[l, pl.ds(pl.multiple_of(dst * RE, RE), RE)],
                dst_ref=xin.at[l, pl.ds(pl.multiple_of(e * RE, RE), RE)],
                send_sem=dis_s.at[l, d - 1], recv_sem=dis_r.at[l, d - 1],
                device_id={"pool": p, "ep": dst}, device_id_type=MESH)

        for d in range(1, NE):
            dis_send(d).start()
        mine = pl.ds(pl.multiple_of(e * RE, RE), RE)
        xin[l, mine, :] = uperm[l, mine, :]

        lg3 = lax.dot_general(wr3[l], u, NT, preferred_element_type=F32)
        ne = wr_ref.shape[1]
        lg = lg3[0:ne] + lg3[ne:2 * ne] + lg3[2 * ne:3 * ne]
        picked = [jnp.sum(jnp.where(ecol == ids_ref[l, k:k + 1, :], lg, 0.0), axis=0, keepdims=True)
                  for k in range(K)]
        gtop = picked[0]
        for k in range(1, K):
            gtop = jnp.maximum(gtop, picked[k])
        ex = [jnp.exp(v - gtop) for v in picked]
        tot = ex[0]
        for k in range(1, K):
            tot = tot + ex[k]
        grow = jnp.concatenate([v / tot for v in ex], axis=1)
        gcol = jnp.broadcast_to(grow, (SLOTS, SLOTS)).T[:, 0:1]

        wait(up_copies(l))
        for d in range(1, NE):
            dis_send(d).wait_recv()

        xe = xin[l]
        f0 = 0
        while f0 < FF:
            fw = min(2 * HD, FF - f0)
            h1 = dot(xe, w1b[:, f0:f0 + fw])
            h3 = dot(xe, w3b[:, f0:f0 + fw])
            act[:, f0:f0 + fw] = (h1 * jax.nn.sigmoid(h1) * h3).astype(BF)
            f0 += fw

        @pl.when(more)
        def _():
            start(up_copies(l + 1))

        def ys_send(d):
            return pltpu.make_async_remote_copy(
                src_ref=ysend.at[l, d - 1], dst_ref=yrecv.at[l, d - 1], send_sem=ys_s.at[l, d - 1],
                recv_sem=ys_r.at[l, d - 1], device_id={"pool": pool_of(d), "ep": e}, device_id_type=MESH)

        wait(down_copies(l))
        for d in (2, 1, 3, 0) if NP == 4 else list(range(1, NP)) + [0]:
            ysend[l, (d - 1) % NP] = dot(act[...], w2b[pool_of(d)])
            if d:
                ys_send(d).start()

        @pl.when(more)
        def _():
            start(down_copies(l + 1))

        acc = ysend[l, NP - 1]
        for d in range(1, NP):
            ys_send(d).wait_recv()
            acc = acc + yrecv[l, d - 1]
        ybf[l] = acc.astype(BF)

        def ret_send(dp_, de):
            dst = ep_of(de)
            return pltpu.make_async_remote_copy(
                src_ref=ybf.at[l, pl.ds(pl.multiple_of(dst * RE, RE), RE)],
                dst_ref=yret.at[l, p, pl.ds(pl.multiple_of(e * RE, RE), RE)],
                send_sem=ret_s.at[l, dp_ * NE + de], recv_sem=ret_r.at[l, dp_ * NE + de],
                device_id={"pool": pool_of(dp_), "ep": dst}, device_id_type=MESH)

        others = [(a, b) for a in range(NP) for b in range(NE) if a or b]
        for a, b in others:
            ret_send(a, b).start()
        yret[l, p, mine, :] = ybf[l, mine, :]
        for a, b in others:
            ret_send(a, b).wait_recv()

        for b in range(NP):
            cols = slice(b * CB, (b + 1) * CB)
            yp = dot(rmat[l], yret[l, b]) * gcol
            mixed = yp[0:T]
            for k in range(1, K):
                mixed = mixed + yp[k * T:(k + 1) * T]
            xs[:, cols] = (a_s[:, cols] + mixed).astype(BF).astype(F32)

        for i in range(NP - 1):
            att_send(i).wait_send()
            og_send(i + 1).wait_send()
            ys_send(i + 1).wait_send()
        for d in range(1, NE):
            dis_send(d).wait_send()
        for a, b in others:
            ret_send(a, b).wait_send()
        return carry

    lax.fori_loop(0, L, layer, 0)
    out_ref[...] = xs[...].astype(BF)


def solution(mesh):
    tok_spec = P(("dp", "ep"), None)
    cache_spec = P(None, ("dp", "ep"), "pool", None, None)
    up_spec = P(None, "ep", None, "pool")
    down_spec = P(None, "ep", "pool", None)
    in_specs = (tok_spec, cache_spec, cache_spec, P(("dp", "ep")), P(), P(), P(), P(), P(),
                P(None, ("dp", "ep"), None), up_spec, up_spec, down_spec)
    NP, NE = mesh.shape["pool"], mesh.shape["ep"]

    def body(hidden, k_cache, v_cache, cache_len, w_q, w_k, w_v, w_o, w_router, ids, w_one, w_three, w_two):
        L = w_q.shape[0]
        T, D = hidden.shape
        S, G, HD = k_cache.shape[2:]
        NH = w_q.shape[2] // HD
        K = ids.shape[2]
        FF = w_one.shape[3]
        TC = T // NP
        SLOTS, CB, ROWS, SG = T * K, D // NP, TC * NH, S * G
        assert w_one.shape[1] == 1 and SLOTS == HD and ROWS == HD and w_router.shape[2] == 8
        dims = (L, T, D, S, G, HD, NH, NP, NE, TC, K, FF)
        kc = k_cache.reshape(L, T, SG, HD)
        vc = v_cache.reshape(L, T, SG, HD)
        wr_t = jnp.swapaxes(w_router, 1, 2)
        ids_t = jnp.swapaxes(ids, 1, 2)
        V = pltpu.VMEM
        dma = pltpu.SemaphoreType.DMA
        anyspec = pl.BlockSpec(memory_space=pl.ANY)
        vspec = pl.BlockSpec(memory_space=pltpu.VMEM)
        scratch = [
            V((T, D), BF), V((T, D), F32), V((D, (NH + 2 * G) * HD), BF),
            V((NP, TC, SG, HD), BF), V((NP, TC, SG, HD), BF), V((D, D), BF),
            V((D, FF), BF), V((D, FF), BF), V((NP, FF, CB), BF),
            V((T * NH, HD), F32), V((T, 2 * G * HD), F32), V((ROWS, HD), F32), V((ROWS, HD), F32),
            V((ROWS, HD), F32), V((L, NP, ROWS + 8, HD), F32), V((L, NP - 1, ROWS + 8, HD), F32),
            V((ROWS, HD), F32), V((L, T, NH * HD), BF),
            V((T, D), F32), V((L, SLOTS, D), BF), V((L, SLOTS, D), BF), V((SLOTS, FF), BF),
            V((L, NP, SLOTS, CB), F32), V((L, NP - 1, SLOTS, CB), F32),
            V((L, SLOTS, CB), BF), V((L, NP, SLOTS, CB), BF),
            V((L, SLOTS, T), BF), V((L, SLOTS, SLOTS), BF), V((L, 32, D), BF),
            dma((7 + NP,)), dma((2, NP)),
            dma((L, NP - 1)), dma((L, NP - 1)), dma((L, NP - 1)), dma((L, NP - 1)),
            dma((L, NE - 1)), dma((L, NE - 1)), dma((L, NP - 1)), dma((L, NP - 1)),
            dma((L, NP * NE)), dma((L, NP * NE)),
        ]
        return pl.pallas_call(
            functools.partial(layers_kernel, dims),
            out_shape=jax.ShapeDtypeStruct((T, D), BF),
            in_specs=[pl.BlockSpec(memory_space=pltpu.SMEM), anyspec, vspec, anyspec, anyspec, anyspec, anyspec,
                      anyspec, anyspec, vspec, anyspec, anyspec, anyspec],
            out_specs=vspec,
            scratch_shapes=scratch,
            name="moe_layers",
            compiler_params=pltpu.CompilerParams(collective_id=0, has_side_effects=True,
                                                 vmem_limit_bytes=60 * 1024 * 1024),
        )(cache_len, hidden, ids_t, kc, vc, w_q, w_k, w_v, w_o, wr_t, w_one, w_three, w_two)

    return jax.shard_map(body, mesh=mesh, in_specs=in_specs, out_specs=tok_spec, check_vma=False)
```

```python
import functools

import jax
import jax.numpy as jnp
from jax import lax
from jax.experimental import pallas as pl
from jax.experimental.pallas import tpu as pltpu
from jax.sharding import PartitionSpec as P

MESH = pl.DeviceIdType.MESH
NORM_EPS = 1e-6
NEG = -1e30
BF = jnp.bfloat16
F32 = jnp.float32
NT = (((1,), (1,)), ((), ()))


def rms_norm(v):
    return v * lax.rsqrt(jnp.mean(v * v, axis=-1, keepdims=True) + NORM_EPS)


def dot(a, b):
    return jnp.dot(a, b, preferred_element_type=F32)


def layers_kernel(dims, len_ref, x_hbm, ids_hbm, k_hbm, v_hbm, wq_hbm, wk_hbm, wv_hbm, wo_hbm, wr_hbm,
                  w1_hbm, w3_hbm, w2_hbm, out_ref,
                  xb, xs, idb, wrb, wqkv, kbuf, vbuf, wob, w1b, w3b, w2b, qrows, kvs, kx, vx, zst, msg, arx, orow, oag,
                  a_s, uperm, xin, act, ys, ysum, rlr, drr, srr, ybf, yret,
                  ld_sem, kv_sem, att_s, att_r, og_s, og_r, dis_s, dis_r, rl_s, rl_r, dr_s, dr_r, sr_s, sr_r,
                  ret_s, ret_r):
    L, T, D, S, G, HD, NH, NP, NE, TC, K, FF = dims
    QG = NH // G
    SLOTS = T * K
    RE = SLOTS // NE
    CB = D // NP
    SG = S * G
    QW = NH * HD
    KW = G * HD
    TU = TC // 2
    TH = T // 2
    UR = TU * NH
    NU = 2 * NP
    NX = NE // 2
    RG = SLOTS // 2
    RH = RG // 2
    BW = 2 * HD
    scale = HD ** -0.5
    p = lax.axis_index("pool")
    e = lax.axis_index("ep")
    chip = lax.div(e, 2)
    core = lax.rem(e, 2)

    def pool_of(d):
        return lax.rem(p + d, NP)

    rel = [(0, 0), (0, 1), (1, 0), (NX - 1, 0), (1, 1), (NX - 1, 1)]
    rel += [(dx, dc) for dx in range(2, NX - 1) for dc in range(2)]
    NR = len(rel)

    def ep_sender(r):
        return lax.rem(chip + rel[r][0], NX) * 2 + lax.rem(core + rel[r][1], 2)

    def ep_receiver(r):
        return lax.rem(chip + NX - rel[r][0], NX) * 2 + lax.rem(core + rel[r][1], 2)

    barrier = pltpu.get_barrier_semaphore()
    for dp_ in range(NP):
        for de in range(NE):
            if dp_ or de:
                pl.semaphore_signal(barrier, inc=1,
                                    device_id={"pool": pool_of(dp_), "ep": lax.rem(e + de, NE)},
                                    device_id_type=MESH)

    def block(ref, l, b, n):
        return ref.at[l, :, pl.ds(b * BW, n)]

    def qkv_copies(l):
        out = [pltpu.make_async_copy(block(wq_hbm, l, b, BW), wqkv.at[b], ld_sem.at[b]) for b in range(QW // BW)]
        n = QW // BW
        out.append(pltpu.make_async_copy(wk_hbm.at[l], wqkv.at[n], ld_sem.at[n]))
        out.append(pltpu.make_async_copy(wv_hbm.at[l], wqkv.at[n + 1], ld_sem.at[n + 1]))
        return out

    s0 = QW // BW + 2

    def kv_copies(l, n):
        half, i = divmod(n, NP) if isinstance(n, int) else (lax.div(n, NP), lax.rem(n, NP))
        tok = pl.ds(pl.multiple_of(half * TH + lax.rem(p + i + 1, NP) * TU, TU), TU)
        return [pltpu.make_async_copy(k_hbm.at[l, tok], kbuf.at[n], kv_sem.at[0, n]),
                pltpu.make_async_copy(v_hbm.at[l, tok], vbuf.at[n], kv_sem.at[1, n])]

    def wo_copies(l):
        return [pltpu.make_async_copy(wo_hbm.at[l], wob, ld_sem.at[s0])]

    def up_copies(l):
        return [pltpu.make_async_copy(w1_hbm.at[l, 0], w1b, ld_sem.at[s0 + 1]),
                pltpu.make_async_copy(w3_hbm.at[l, 0], w3b, ld_sem.at[s0 + 2])]

    def down_copies(l):
        return [pltpu.make_async_copy(w2_hbm.at[l, 0, :, pl.ds(q * CB, CB)], w2b.at[q], ld_sem.at[s0 + 3 + q])
                for q in range(NP)]

    def start(copies):
        for c in copies:
            c.start()

    def wait(copies):
        for c in copies:
            c.wait()

    small = [pltpu.make_async_copy(x_hbm, xb, ld_sem.at[s0 + 3 + NP]),
             pltpu.make_async_copy(ids_hbm, idb, ld_sem.at[s0 + 4 + NP]),
             pltpu.make_async_copy(wr_hbm, wrb, ld_sem.at[s0 + 5 + NP])]
    small[0].start()
    start(qkv_copies(0))
    start(small[1:])
    for n in range(2):
        start(kv_copies(0, n))

    hrow = lax.broadcasted_iota(jnp.int32, (NH, SG), 0)
    pcol = lax.broadcasted_iota(jnp.int32, (NH, SG), 1)
    posm = jnp.where(lax.rem(pcol, G) == lax.div(hrow, QG), lax.div(pcol, G), jnp.int32(1 << 30))
    lane = lax.broadcasted_iota(jnp.int32, (NH, HD), 1)
    NEX = wrb.shape[1]
    ecol = lax.broadcasted_iota(jnp.int32, (NEX, T), 0)

    small[0].wait()
    xs[...] = xb[...].astype(F32)
    wait(small[1:])

    def layer(l, carry):
        more = l + 1 < L
        first = l == 0

        def att_send(half, i):
            return pltpu.make_async_remote_copy(
                src_ref=msg.at[l, half, i], dst_ref=arx.at[l, half, i], send_sem=att_s.at[l, half, i],
                recv_sem=att_r.at[l, half, i], device_id={"pool": pool_of(i + 1), "ep": e}, device_id_type=MESH)

        def own_tok(half):
            return pl.ds(pl.multiple_of(half * TH + p * TU, TU), TU)

        def og_send(half, d):
            return pltpu.make_async_remote_copy(
                src_ref=oag.at[l, own_tok(half)], dst_ref=oag.at[l, own_tok(half)], send_sem=og_s.at[l, half, d - 1],
                recv_sem=og_r.at[l, half, d - 1], device_id={"pool": pool_of(d), "ep": e}, device_id_type=MESH)

        def dis_send(r):
            dst = ep_receiver(r)
            return pltpu.make_async_remote_copy(
                src_ref=uperm.at[l, pl.ds(pl.multiple_of(dst * RE, RE), RE)], dst_ref=xin.at[l, pl.ds(r * RE, RE)],
                send_sem=dis_s.at[l, r], recv_sem=dis_r.at[l, r],
                device_id={"pool": p, "ep": dst}, device_id_type=MESH)

        def ring_dev(way):
            return {"pool": pool_of(1 if way == 0 else NP - 1), "ep": e}

        def relay_send(g, way):
            return pltpu.make_async_remote_copy(
                src_ref=ys.at[l, g, 2, pl.ds(way * RH, RH)], dst_ref=rlr.at[l, g, way], send_sem=rl_s.at[l, g, way],
                recv_sem=rl_r.at[l, g, way], device_id=ring_dev(way), device_id_type=MESH)

        def direct_send(g, way):
            return pltpu.make_async_remote_copy(
                src_ref=ys.at[l, g, 1 if way == 0 else 3, pl.ds((1 - way) * RH, RH)], dst_ref=drr.at[l, g, way],
                send_sem=dr_s.at[l, g, way], recv_sem=dr_r.at[l, g, way], device_id=ring_dev(way),
                device_id_type=MESH)

        def sum_send(g, way):
            return pltpu.make_async_remote_copy(
                src_ref=ysum.at[l, g, way], dst_ref=srr.at[l, g, way], send_sem=sr_s.at[l, g, way],
                recv_sem=sr_r.at[l, g, way], device_id=ring_dev(way), device_id_type=MESH)

        def ret_send(dp_, r):
            dst = ep_sender(r)
            return pltpu.make_async_remote_copy(
                src_ref=ybf.at[l, pl.ds(r * RE, RE)],
                dst_ref=yret.at[l, p, pl.ds(pl.multiple_of(e * RE, RE), RE)],
                send_sem=ret_s.at[l, dp_, r], recv_sem=ret_r.at[l, dp_, r],
                device_id={"pool": pool_of(dp_), "ep": dst}, device_id_type=MESH)

        with jax.named_scope("qkv"):
            hn = rms_norm(xs[...]).astype(BF)
            cps = qkv_copies(l)
            for b in range(len(cps)):
                cps[b].wait()
                r = dot(hn, wqkv[b]).astype(BF).astype(F32)
                if b * BW < QW:
                    for j in range(2):
                        qrows[pl.ds(2 * b + j, T, stride=NH), :] = r[:, j * HD:(j + 1) * HD]
                else:
                    kvs[:, b * BW - QW:(b + 1) * BW - QW] = r

            @pl.when(first)
            def _():
                for n in range(2, 4):
                    start(kv_copies(l, n))

            for half in range(2):
                for h in range(NH):
                    g = h // QG
                    kx[pl.ds(half * UR + h, TU, stride=NH), :] = kvs[own_tok(half), g * HD:(g + 1) * HD]
                    vx[pl.ds(half * UR + h, TU, stride=NH), :] = kvs[own_tok(half), KW + g * HD:KW + (g + 1) * HD]

        def combine(half):
            with jax.named_scope("combine"):
                orows = pl.ds(pl.multiple_of((half * TH + p * TU) * NH, UR), UR)
                hrows = pl.ds(pl.multiple_of(half * UR, UR), UR)
                s_new = jnp.sum(qrows[orows, :] * kx[hrows, :], axis=1, keepdims=True) * scale
                for i in range(NP - 1):
                    att_send(half, i).wait_recv()
                    zst[8 * i:8 * i + 8, :] = arx[l, half, i, UR:UR + 8, :]
                zst[8 * (NP - 1):8 * NP, :] = msg[l, half, NP - 1, UR:UR + 8, :]
                zc = zst[...].T
                cut = [zc[(i % 2) * UR:(i % 2) * UR + UR] for i in range(NP)]
                ms = [cut[i][:, 8 * i:8 * i + 1] for i in range(NP)]
                top = s_new
                for m in ms:
                    top = jnp.maximum(top, m)
                p_new = jnp.exp(s_new - top)
                den = p_new
                num = p_new * vx[hrows, :]
                for i in range(NP):
                    w = jnp.exp(ms[i] - top)
                    den = den + w * cut[i][:, 8 * i + 1:8 * i + 2]
                    num = num + w * (arx[l, half, i, 0:UR, :] if i < NP - 1 else msg[l, half, i, 0:UR, :])
                orow[...] = num / den
                for h in range(NH):
                    oag[l, own_tok(half), h * HD:(h + 1) * HD] = orow[pl.ds(h, TU, stride=NH), :].astype(BF)
                for d in (2, 1, 3):
                    og_send(half, d).start()

        def chunk(it, c2):
            half = lax.div(it, NP // 2)
            i0 = lax.rem(it, NP // 2) * 2
            for un in range(2):
                n = 2 * it + un
                wait(kv_copies(l, n))
                nxt = n + 4

                @pl.when(jnp.logical_and(first, nxt < NU))
                def _():
                    start(kv_copies(l, nxt))

            @pl.when(jnp.logical_and(first, it == 2))
            def _():
                start(wo_copies(l))
                start(up_copies(l))
                start(down_copies(l))

            for un in range(2):
                i = i0 + un
                n = 2 * it + un
                sc = []
                for j in range(TU):
                    t = half * TH + lax.rem(p + i + 1, NP) * TU + j
                    qt = qrows[pl.ds(pl.multiple_of(t * NH, NH), NH), :].astype(BF)
                    s = lax.dot_general(qt, kbuf[n, j], NT, preferred_element_type=F32) * scale
                    sc.append(jnp.where(posm < len_ref[t] - p * S, s, NEG))
                mx = [jnp.max(s, axis=1, keepdims=True) for s in sc]
                pr = [jnp.exp(s - m) for s, m in zip(sc, mx)]
                ls = [jnp.sum(q, axis=1, keepdims=True) for q in pr]
                for j in range(TU):
                    msg[l, half, i, j * NH:(j + 1) * NH, :] = dot(pr[j].astype(BF), vbuf[n, j])
                    zst[un * UR + j * NH:un * UR + (j + 1) * NH, :] = jnp.where(lane == 0, mx[j], ls[j])
            zt = zst[...].T[0:8, :]
            for un in range(2):
                msg[l, half, i0 + un, UR:UR + 8, :] = zt

            @pl.when(jnp.logical_and(first, it == 0))
            def _():
                pl.semaphore_wait(barrier, NP * NE - 1)

            att_send(half, i0).start()

            @pl.when(i0 == 0)
            def _():
                att_send(half, i0 + 1).start()

            @pl.when(it == 2)
            def _():
                combine(0)

            return c2

        with jax.named_scope("attn"):
            lax.fori_loop(0, NP, chunk, 0)

        @pl.when(more)
        def _():
            start(qkv_copies(l + 1))
            for n in range(NU):
                start(kv_copies(l + 1, n))

        combine(1)

        with jax.named_scope("tables"):
            slot_col = lax.broadcasted_iota(jnp.int32, (SLOTS, SLOTS), 0)
            pair_row = lax.broadcasted_iota(jnp.int32, (SLOTS, SLOTS), 1)
            upper = (slot_col < pair_row).astype(F32).astype(BF)
            want_rank = lax.rem(slot_col, RE).astype(F32)
            idrow = jnp.concatenate([idb[l, k:k + 1, :] for k in range(K)], axis=1)
            same = (jnp.broadcast_to(idrow, (SLOTS, SLOTS)) == lax.div(slot_col, RE))
            rank = dot(same.astype(F32).astype(BF), upper)
            pick = jnp.where(jnp.logical_and(same, rank == want_rank), 1.0, 0.0).astype(F32)
            rmat = pick.T.astype(BF)
            dmat = pick[:, 0:T]
            for k in range(1, K):
                dmat = dmat + pick[:, k * T:(k + 1) * T]
            dmat = dmat.astype(BF)
            wr = wrb[l]
            hi = wr.astype(BF).astype(F32)
            mid = (wr - hi).astype(BF).astype(F32)
            lo = wr - hi - mid
            wr3 = jnp.concatenate([hi, mid, lo, jnp.zeros_like(lo)], axis=0).astype(BF)

        with jax.named_scope("agwait"):
            wait(wo_copies(l))
            for half in range(2):
                for d in range(1, NP):
                    og_send(half, d).wait_recv()

        with jax.named_scope("oproj"):
            for b in range(NP):
                cols = slice(b * CB, (b + 1) * CB)
                a_s[:, cols] = (xs[:, cols] + dot(oag[l], wob[:, cols])).astype(BF).astype(F32)

            @pl.when(more)
            def _():
                start(wo_copies(l + 1))

            u = rms_norm(a_s[...]).astype(BF)
            for b in range(NP):
                cols = slice(b * CB, (b + 1) * CB)
                uperm[l, :, cols] = dot(dmat, u[:, cols]).astype(BF)
            for r in range(1, NR):
                dis_send(r).start()
            xin[l, 0:RE, :] = uperm[l, pl.ds(pl.multiple_of(e * RE, RE), RE), :]

        with jax.named_scope("gates"):
            lg3 = lax.dot_general(wr3, u, NT, preferred_element_type=F32)
            lg = lg3[0:NEX] + lg3[NEX:2 * NEX] + lg3[2 * NEX:3 * NEX]
            picked = [jnp.sum(jnp.where(ecol == idb[l, k:k + 1, :], lg, 0.0), axis=0, keepdims=True)
                      for k in range(K)]
            gtop = picked[0]
            for k in range(1, K):
                gtop = jnp.maximum(gtop, picked[k])
            ex = [jnp.exp(v - gtop) for v in picked]
            tot = ex[0]
            for k in range(1, K):
                tot = tot + ex[k]
            grow = jnp.concatenate([v / tot for v in ex], axis=1)
            gcol = jnp.broadcast_to(grow, (SLOTS, SLOTS)).T[:, 0:1]
            wait(up_copies(l))

        def up(g):
            for r in range(g * NR // 2, (g + 1) * NR // 2):
                if r:
                    dis_send(r).wait_recv()
            xe = xin[l, g * RG:(g + 1) * RG]
            f0 = 0
            while f0 < FF:
                fw = min(BW, FF - f0)
                h1 = dot(xe, w1b[:, f0:f0 + fw])
                h3 = dot(xe, w3b[:, f0:f0 + fw])
                act[g, :, f0:f0 + fw] = (h1 * jax.nn.sigmoid(h1) * h3).astype(BF)
                f0 += fw

        def down(g, d):
            ys[l, g, d] = dot(act[g], w2b[pool_of(d)])

        def relay_add(g):
            for way in range(2):
                relay_send(g, way).wait_recv()
                ysum[l, g, way] = ys[l, g, 1 if way == 0 else 3, way * RH:(way + 1) * RH] + rlr[l, g, way]
                sum_send(g, way).start()

        def finish(g):
            for way in range(2):
                direct_send(g, 1 - way).wait_recv()
                sum_send(g, way).wait_recv()
                rows = slice(way * RH, (way + 1) * RH)
                tot = ys[l, g, 0, rows] + drr[l, g, 1 - way] + srr[l, g, way]
                ybf[l, g * RG + way * RH:g * RG + (way + 1) * RH] = tot.astype(BF)
            for dp_ in (2, 1, 3, 0):
                for r in range((g + 1) * NR // 2 - 1, g * NR // 2 - 1, -1):
                    if dp_ or r:
                        ret_send(dp_, r).start()
            if g == 0:
                yret[l, p, pl.ds(pl.multiple_of(e * RE, RE), RE), :] = ybf[l, 0:RE, :]

        with jax.named_scope("up0"):
            up(0)
        with jax.named_scope("down0"):
            wait(down_copies(l))
            down(0, 2)
            for way in range(2):
                relay_send(0, way).start()
            down(0, 1)
            direct_send(0, 0).start()
            down(0, 3)
            direct_send(0, 1).start()
            down(0, 0)
        with jax.named_scope("up1"):
            up(1)

            @pl.when(more)
            def _():
                start(up_copies(l + 1))

        with jax.named_scope("down1"):
            down(1, 2)
            for way in range(2):
                relay_send(1, way).start()
            relay_add(0)
            down(1, 1)
            direct_send(1, 0).start()
            down(1, 3)
            direct_send(1, 1).start()
            down(1, 0)

            @pl.when(more)
            def _():
                start(down_copies(l + 1))

        with jax.named_scope("relay1"):
            relay_add(1)
        with jax.named_scope("finish0"):
            finish(0)
        with jax.named_scope("finish1"):
            finish(1)
        with jax.named_scope("retwait"):
            for dp_ in range(NP):
                for r in range(NR):
                    if dp_ or r:
                        ret_send(dp_, r).wait_recv()

        with jax.named_scope("gsum"):
            for b in range(NP):
                cols = slice(b * CB, (b + 1) * CB)
                yp = dot(rmat, yret[l, b]) * gcol
                mixed = yp[0:T]
                for k in range(1, K):
                    mixed = mixed + yp[k * T:(k + 1) * T]
                xs[:, cols] = (a_s[:, cols] + mixed).astype(BF).astype(F32)

        for half in range(2):
            for i in range(NP - 1):
                att_send(half, i).wait_send()
                og_send(half, i + 1).wait_send()
        for r in range(1, NR):
            dis_send(r).wait_send()
        for g in range(2):
            for way in range(2):
                relay_send(g, way).wait_send()
                direct_send(g, way).wait_send()
                sum_send(g, way).wait_send()
        for dp_ in range(NP):
            for r in range(NR):
                if dp_ or r:
                    ret_send(dp_, r).wait_send()
        return carry

    lax.fori_loop(0, L, layer, 0)
    out_ref[...] = xs[...].astype(BF)


def solution(mesh):
    tok_spec = P(("dp", "ep"), None)
    cache_spec = P(None, ("dp", "ep"), "pool", None, None)
    up_spec = P(None, "ep", None, "pool")
    down_spec = P(None, "ep", "pool", None)
    in_specs = (tok_spec, cache_spec, cache_spec, P(("dp", "ep")), P(), P(), P(), P(), P(),
                P(None, ("dp", "ep"), None), up_spec, up_spec, down_spec)
    NP, NE = mesh.shape["pool"], mesh.shape["ep"]

    def body(hidden, k_cache, v_cache, cache_len, w_q, w_k, w_v, w_o, w_router, ids, w_one, w_three, w_two):
        L = w_q.shape[0]
        T, D = hidden.shape
        S, G, HD = k_cache.shape[2:]
        NH = w_q.shape[2] // HD
        K = ids.shape[2]
        FF = w_one.shape[3]
        TC = T // NP
        SLOTS, CB, ROWS, SG, UR = T * K, D // NP, TC * NH, S * G, TC // 2 * NH
        assert w_one.shape[1] == 1 and SLOTS == HD and ROWS == HD and w_router.shape[2] == 8 and NP == 4 and G == 2
        dims = (L, T, D, S, G, HD, NH, NP, NE, TC, K, FF)
        kc = k_cache.reshape(L, T, SG, HD)
        vc = v_cache.reshape(L, T, SG, HD)
        wr_t = jnp.swapaxes(w_router, 1, 2)
        ids_t = jnp.swapaxes(ids, 1, 2)
        V = pltpu.VMEM
        dma = pltpu.SemaphoreType.DMA
        anyspec = pl.BlockSpec(memory_space=pl.ANY)
        vspec = pl.BlockSpec(memory_space=pltpu.VMEM)
        scratch = [
            V((T, D), BF), V((T, D), F32), V(ids_t.shape, jnp.int32), V(wr_t.shape, F32),
            V((NH // 2 + G, D, 2 * HD), BF),
            V((2 * NP, TC // 2, SG, HD), BF), V((2 * NP, TC // 2, SG, HD), BF), V((D, D), BF),
            V((D, FF), BF), V((D, FF), BF), V((NP, FF, CB), BF),
            V((T * NH, HD), F32), V((T, 2 * G * HD), F32), V((ROWS, HD), F32), V((ROWS, HD), F32),
            V((ROWS, HD), F32), V((L, 2, NP, UR + 8, HD), F32), V((L, 2, NP - 1, UR + 8, HD), F32),
            V((UR, HD), F32), V((L, T, NH * HD), BF),
            V((T, D), F32), V((L, SLOTS, D), BF), V((L, SLOTS, D), BF), V((2, SLOTS // 2, FF), BF),
            V((L, 2, NP, SLOTS // 2, CB), F32), V((L, 2, 2, SLOTS // 4, CB), F32),
            V((L, 2, 2, SLOTS // 4, CB), F32), V((L, 2, 2, SLOTS // 4, CB), F32), V((L, 2, 2, SLOTS // 4, CB), F32),
            V((L, SLOTS, CB), BF), V((L, NP, SLOTS, CB), BF),
            dma((NH // 2 + G + 6 + NP,)), dma((2, 2 * NP)),
            dma((L, 2, NP - 1)), dma((L, 2, NP - 1)), dma((L, 2, NP - 1)), dma((L, 2, NP - 1)),
            dma((L, NE)), dma((L, NE)),
            dma((L, 2, 2)), dma((L, 2, 2)), dma((L, 2, 2)), dma((L, 2, 2)), dma((L, 2, 2)), dma((L, 2, 2)),
            dma((L, NP, NE)), dma((L, NP, NE)),
        ]
        return pl.pallas_call(
            functools.partial(layers_kernel, dims),
            out_shape=jax.ShapeDtypeStruct((T, D), BF),
            in_specs=[pl.BlockSpec(memory_space=pltpu.SMEM), anyspec, anyspec, anyspec, anyspec, anyspec, anyspec,
                      anyspec, anyspec, anyspec, anyspec, anyspec, anyspec],
            out_specs=vspec,
            scratch_shapes=scratch,
            name="moe_layers",
            compiler_params=pltpu.CompilerParams(collective_id=0, has_side_effects=True,
                                                 vmem_limit_bytes=60 * 1024 * 1024),
        )(cache_len, hidden, ids_t, kc, vc, w_q, w_k, w_v, w_o, wr_t, w_one, w_three, w_two)

    return jax.shard_map(body, mesh=mesh, in_specs=in_specs, out_specs=tok_spec, check_vma=False)
```

```python
import functools

import jax
import jax.numpy as jnp
from jax import lax
from jax.experimental import pallas as pl
from jax.experimental.pallas import tpu as pltpu
from jax.sharding import PartitionSpec as P

MESH = pl.DeviceIdType.MESH
NORM_EPS = 1e-6
NEG = -1e30
BF = jnp.bfloat16
F32 = jnp.float32
NT = (((1,), (1,)), ((), ()))


def rms_norm(v):
    return v * lax.rsqrt(jnp.mean(v * v, axis=-1, keepdims=True) + NORM_EPS)


def dot(a, b):
    return jnp.dot(a, b, preferred_element_type=F32)


def layers_kernel(dims, len_ref, x_hbm, ids_hbm, k_hbm, v_hbm, wq_hbm, wk_hbm, wv_hbm, wo_hbm, wr_hbm,
                  w1_hbm, w3_hbm, w2_hbm, out_ref,
                  xb, xs, idb, wrb, wqb, wkvb, kvbuf, wob, w1b, w3b, w2b, qrows, kvs, kx, vx, zst, msg, arx, orow, oag,
                  a_s, uperm, xin, act, ys, yrecv, ybf, yret,
                  ld_sem, kv_sem, att_s, att_r, og_s, og_r, dis_s, dis_r, ys_s, ys_r, ret_s, ret_r):
    L, T, D, S, G, HD, NH, NP, NE, TC, K, FF = dims
    QG = NH // G
    SLOTS = T * K
    RE = SLOTS // NE
    CB = D // NP
    SG = S * G
    QW = NH * HD
    KW = G * HD
    TU = TC // 2
    TH = T // 2
    UR = TU * NH
    NU = 2 * NP
    NM = 2 * (NP - 1)
    NX = NE // 2
    RG = SLOTS // 2
    BW = 2 * HD
    scale = HD ** -0.5
    p = lax.axis_index("pool")
    e = lax.axis_index("ep")
    chip = lax.div(e, 2)
    core = lax.rem(e, 2)

    def pool_of(d):
        return lax.rem(p + d, NP)

    rel = [(0, 0), (0, 1), (1, 0), (NX - 1, 0), (1, 1), (NX - 1, 1)]
    rel += [(dx, dc) for dx in range(2, NX - 1) for dc in range(2)]
    NR = len(rel)

    def ep_sender(r):
        return lax.rem(chip + rel[r][0], NX) * 2 + lax.rem(core + rel[r][1], 2)

    def ep_receiver(r):
        return lax.rem(chip + NX - rel[r][0], NX) * 2 + lax.rem(core + rel[r][1], 2)

    def qkv_load(l):
        for b in range(2):
            rows = pl.ds(b * (D // 2), D // 2)
            pltpu.make_async_copy(wq_hbm.at[l, rows], wqb.at[rows], ld_sem.at[0]).start()
        pltpu.make_async_copy(wk_hbm.at[l], wkvb.at[0], ld_sem.at[1]).start()
        pltpu.make_async_copy(wv_hbm.at[l], wkvb.at[1], ld_sem.at[1]).start()

    def drain(ref, sem):
        pltpu.make_async_copy(ref, ref, sem).wait()

    def unit(n):
        z = n // NM
        half = (1 - z) * (n // (NP - 1)) + z * (n - NM)
        away = (1 - z) * (n % (NP - 1) + 1)
        return half, away

    def unit_tok(n):
        half, away = unit(n)
        return half * TH + lax.rem(p + away, NP) * TU

    def kv_load(l, n):
        tok = pl.ds(pl.multiple_of(unit_tok(n), TU), TU)
        pltpu.make_async_copy(k_hbm.at[l, tok], kvbuf.at[n, 0], kv_sem.at[n]).start()
        pltpu.make_async_copy(v_hbm.at[l, tok], kvbuf.at[n, 1], kv_sem.at[n]).start()

    def wo_copy(l):
        return pltpu.make_async_copy(wo_hbm.at[l], wob, ld_sem.at[2])

    def up_load(l):
        pltpu.make_async_copy(w1_hbm.at[l, 0], w1b, ld_sem.at[3]).start()
        pltpu.make_async_copy(w3_hbm.at[l, 0], w3b, ld_sem.at[4]).start()

    def down_load(l):
        for q in range(NP):
            pltpu.make_async_copy(w2_hbm.at[l, 0, :, pl.ds(q * CB, CB)], w2b.at[q], ld_sem.at[5]).start()

    small = [pltpu.make_async_copy(x_hbm, xb, ld_sem.at[6]),
             pltpu.make_async_copy(ids_hbm, idb, ld_sem.at[7]),
             pltpu.make_async_copy(wr_hbm, wrb, ld_sem.at[8])]
    small[0].start()
    qkv_load(0)
    for n in range(2):
        kv_load(0, n)
    small[1].start()
    small[2].start()

    barrier = pltpu.get_barrier_semaphore()
    for dp_ in range(NP):
        for de in range(NE):
            if dp_ or de:
                pl.semaphore_signal(barrier, inc=1,
                                    device_id={"pool": pool_of(dp_), "ep": lax.rem(e + de, NE)},
                                    device_id_type=MESH)

    hrow = lax.broadcasted_iota(jnp.int32, (NH, SG), 0)
    pcol = lax.broadcasted_iota(jnp.int32, (NH, SG), 1)
    posm = jnp.where(lax.rem(pcol, G) == lax.div(hrow, QG), lax.div(pcol, G), jnp.int32(1 << 30))
    lane = lax.broadcasted_iota(jnp.int32, (NH, HD), 1)
    NEX = wrb.shape[1]
    ecol = lax.broadcasted_iota(jnp.int32, (NEX, T), 0)

    small[0].wait()
    xs[...] = xb[...].astype(F32)

    def layer(l, carry):
        more = l + 1 < L
        first = l == 0

        def att_send(n, away):
            return pltpu.make_async_remote_copy(
                src_ref=msg.at[l, n], dst_ref=arx.at[l, n], send_sem=att_s, recv_sem=att_r.at[n // (NP - 1)],
                device_id={"pool": pool_of(away), "ep": e}, device_id_type=MESH)

        def own_tok(half):
            return pl.ds(pl.multiple_of(half * TH + p * TU, TU), TU)

        def og_send(half, d):
            return pltpu.make_async_remote_copy(
                src_ref=oag.at[l, own_tok(half)], dst_ref=oag.at[l, own_tok(half)], send_sem=og_s, recv_sem=og_r,
                device_id={"pool": pool_of(d), "ep": e}, device_id_type=MESH)

        def dis_send(r):
            dst = ep_receiver(r)
            return pltpu.make_async_remote_copy(
                src_ref=uperm.at[l, pl.ds(pl.multiple_of(dst * RE, RE), RE)], dst_ref=xin.at[l, pl.ds(r * RE, RE)],
                send_sem=dis_s, recv_sem=dis_r.at[r // (NR // 2)],
                device_id={"pool": p, "ep": dst}, device_id_type=MESH)

        def ys_send(g, d):
            return pltpu.make_async_remote_copy(
                src_ref=ys.at[l, g, d - 1], dst_ref=yrecv.at[l, g, d - 1], send_sem=ys_s.at[g],
                recv_sem=ys_r.at[g], device_id={"pool": pool_of(d), "ep": e}, device_id_type=MESH)

        def ret_send(dp_, r):
            dst = ep_sender(r)
            return pltpu.make_async_remote_copy(
                src_ref=ybf.at[l, pl.ds(r * RE, RE)],
                dst_ref=yret.at[l, pl.ds(pl.multiple_of(p * SLOTS + e * RE, RE), RE)], send_sem=ret_s, recv_sem=ret_r,
                device_id={"pool": pool_of(dp_), "ep": dst}, device_id_type=MESH)

        with jax.named_scope("qkv"):
            hn = rms_norm(xs[...]).astype(BF)
            drain(wqb, ld_sem.at[0])
            for b in range(QW // BW):
                r = dot(hn, wqb[:, b * BW:(b + 1) * BW]).astype(BF).astype(F32)
                for j in range(2):
                    qrows[pl.ds(2 * b + j, T, stride=NH), :] = r[:, j * HD:(j + 1) * HD]
            drain(wkvb, ld_sem.at[1])
            for b in range(2):
                kvs[:, b * KW:(b + 1) * KW] = dot(hn, wkvb[b]).astype(BF).astype(F32)

            @pl.when(first)
            def _():
                for n in range(2, 4):
                    kv_load(l, n)

            for half in range(2):
                for h in range(NH):
                    g = h // QG
                    kx[pl.ds(half * UR + h, TU, stride=NH), :] = kvs[own_tok(half), g * HD:(g + 1) * HD]
                    vx[pl.ds(half * UR + h, TU, stride=NH), :] = kvs[own_tok(half), KW + g * HD:KW + (g + 1) * HD]

        def merge(qrow, krow, stats, parts):
            s_new = jnp.sum(qrow * kx[krow, :], axis=1, keepdims=True) * scale
            ms = [c[:, 0:1] for c in stats]
            top = s_new
            for m in ms:
                top = jnp.maximum(top, m)
            p_new = jnp.exp(s_new - top)
            den = p_new
            num = p_new * vx[krow, :]
            for i in range(NP):
                w = jnp.exp(ms[i] - top)
                den = den + w * stats[i][:, 1:2]
                num = num + w * parts[i]
            return num / den

        def combine(half):
            m0 = half * (NP - 1)
            drain(arx.at[l, pl.ds(m0, NP - 1)], att_r.at[half])
            for i in range(NP - 1):
                zst[8 * i:8 * i + 8, :] = arx[l, m0 + i, UR:UR + 8, :]
            zst[8 * (NP - 1):8 * NP, :] = msg[l, NM + half, UR:UR + 8, :]
            zc = zst[...].T
            odd = [(m0 + i) % 2 for i in range(NP - 1)] + [(NM + half) % 2]
            stats = [zc[odd[i] * UR:(odd[i] + 1) * UR, 8 * i:8 * i + 8] for i in range(NP)]
            parts = [arx[l, m0 + i, 0:UR, :] for i in range(NP - 1)] + [msg[l, NM + half, 0:UR, :]]
            q0 = pl.multiple_of((half * TH + p * TU) * NH, UR)
            orow[...] = merge(qrows[pl.ds(q0, UR), :], pl.ds(half * UR, UR), stats, parts)
            for h in range(NH):
                oag[l, own_tok(half), h * HD:(h + 1) * HD] = orow[pl.ds(h, TU, stride=NH), :].astype(BF)
            for d in (2, 1, 3):
                og_send(half, d).start()

        def chunk(it, c2):
            for un in range(2):
                n = 2 * it + un
                drain(kvbuf.at[n], kv_sem.at[n])

            @pl.when(jnp.logical_and(first, it < 2))
            def _():
                for un in range(2):
                    kv_load(l, 2 * it + 4 + un)

            @pl.when(jnp.logical_and(first, it == 2))
            def _():
                wo_copy(l).start()
                up_load(l)
                down_load(l)

            for un in range(2):
                n = 2 * it + un
                t0 = unit_tok(n)
                sc = []
                for j in range(TU):
                    t = t0 + j
                    qt = qrows[pl.ds(pl.multiple_of(t * NH, NH), NH), :].astype(BF)
                    s = lax.dot_general(qt, kvbuf[n, 0, j], NT, preferred_element_type=F32) * scale
                    sc.append(jnp.where(posm < len_ref[t] - p * S, s, NEG))
                mx = [jnp.max(s, axis=1, keepdims=True) for s in sc]
                pr = [jnp.exp(s - m) for s, m in zip(sc, mx)]
                ls = [jnp.sum(q, axis=1, keepdims=True) for q in pr]
                for j in range(TU):
                    msg[l, n, j * NH:(j + 1) * NH, :] = dot(pr[j].astype(BF), kvbuf[n, 1, j])
                    zst[un * UR + j * NH:un * UR + (j + 1) * NH, :] = jnp.where(lane == 0, mx[j], ls[j])
            zt = zst[...].T[0:8, :]
            for un in range(2):
                msg[l, 2 * it + un, UR:UR + 8, :] = zt

            @pl.when(jnp.logical_and(first, it == 0))
            def _():
                pl.semaphore_wait(barrier, NP * NE - 1)

            @pl.when(it < NP - 1)
            def _():
                for un in range(2):
                    n = 2 * it + un
                    att_send(n, unit(n)[1]).start()

            return c2

        with jax.named_scope("attn"):
            lax.fori_loop(0, NP, chunk, 0)

        @pl.when(more)
        def _():
            qkv_load(l + 1)
            for n in range(NU):
                kv_load(l + 1, n)

        @pl.when(first)
        def _():
            small[1].wait()
            small[2].wait()

        with jax.named_scope("tables"):
            slot_col = lax.broadcasted_iota(jnp.int32, (SLOTS, SLOTS), 0)
            pair_row = lax.broadcasted_iota(jnp.int32, (SLOTS, SLOTS), 1)
            upper = (slot_col < pair_row).astype(F32).astype(BF)
            want_rank = lax.rem(slot_col, RE).astype(F32)
            idrow = jnp.concatenate([idb[l, k:k + 1, :] for k in range(K)], axis=1)
            same = (jnp.broadcast_to(idrow, (SLOTS, SLOTS)) == lax.div(slot_col, RE))
            rank = dot(same.astype(F32).astype(BF), upper)
            pick = jnp.where(jnp.logical_and(same, rank == want_rank), 1.0, 0.0).astype(F32)
            rmat = pick.T.astype(BF)
            dmat = pick[:, 0:T]
            for k in range(1, K):
                dmat = dmat + pick[:, k * T:(k + 1) * T]
            dmat = dmat.astype(BF)
            wr = wrb[l]
            hi = wr.astype(BF).astype(F32)
            mid = (wr - hi).astype(BF).astype(F32)
            lo = wr - hi - mid
            wr3 = jnp.concatenate([hi, mid, lo, jnp.zeros_like(lo)], axis=0).astype(BF)

        with jax.named_scope("comb0"):
            combine(0)
        with jax.named_scope("comb1"):
            combine(1)
        with jax.named_scope("agwait"):
            wo_copy(l).wait()
            drain(oag.at[l, pl.ds(0, NM * TU)], og_r)

        with jax.named_scope("oproj"):
            for b in range(NP):
                cols = slice(b * CB, (b + 1) * CB)
                a_s[:, cols] = (xs[:, cols] + dot(oag[l], wob[:, cols])).astype(BF).astype(F32)

            @pl.when(more)
            def _():
                wo_copy(l + 1).start()

            u = rms_norm(a_s[...]).astype(BF)
            for b in range(NP):
                cols = slice(b * CB, (b + 1) * CB)
                uperm[l, :, cols] = dot(dmat, u[:, cols]).astype(BF)
            for r in range(1, NR):
                dis_send(r).start()
            xin[l, 0:RE, :] = uperm[l, pl.ds(pl.multiple_of(e * RE, RE), RE), :]

        with jax.named_scope("gates"):
            lg3 = lax.dot_general(wr3, u, NT, preferred_element_type=F32)
            lg = lg3[0:NEX] + lg3[NEX:2 * NEX] + lg3[2 * NEX:3 * NEX]
            picked = [jnp.sum(jnp.where(ecol == idb[l, k:k + 1, :], lg, 0.0), axis=0, keepdims=True)
                      for k in range(K)]
            gtop = picked[0]
            for k in range(1, K):
                gtop = jnp.maximum(gtop, picked[k])
            ex = [jnp.exp(v - gtop) for v in picked]
            tot = ex[0]
            for k in range(1, K):
                tot = tot + ex[k]
            grow = jnp.concatenate([v / tot for v in ex], axis=1)
            gcol = jnp.broadcast_to(grow, (SLOTS, SLOTS)).T[:, 0:1]
            drain(w1b, ld_sem.at[3])
            drain(w3b, ld_sem.at[4])

        def up(g):
            r0 = 1 if g == 0 else NR // 2
            drain(xin.at[l, pl.ds(r0 * RE, (NR // 2 - (g == 0)) * RE)], dis_r.at[g])
            xe = xin[l, g * RG:(g + 1) * RG]
            f0 = 0
            while f0 < FF:
                fw = min(BW, FF - f0)
                h1 = dot(xe, w1b[:, f0:f0 + fw])
                h3 = dot(xe, w3b[:, f0:f0 + fw])
                act[g, :, f0:f0 + fw] = (h1 * jax.nn.sigmoid(h1) * h3).astype(BF)
                f0 += fw

        def down(g, d):
            ys[l, g, (d + NP - 1) % NP] = dot(act[g], w2b[pool_of(d)])

        def finish(g):
            drain(yrecv.at[l, g], ys_r.at[g])
            tot = ys[l, g, NP - 1]
            for d in range(1, NP):
                tot = tot + yrecv[l, g, d - 1]
            ybf[l, g * RG:(g + 1) * RG] = tot.astype(BF)
            for dp_ in (2, 1, 3, 0):
                for r in range((g + 1) * NR // 2 - 1, g * NR // 2 - 1, -1):
                    if dp_ or r:
                        ret_send(dp_, r).start()
            if g == 0:
                yret[l, pl.ds(pl.multiple_of(p * SLOTS + e * RE, RE), RE), :] = ybf[l, 0:RE, :]

        def down_all(g):
            for d in (2, 1, 3, 0):
                down(g, d)
                if d:
                    ys_send(g, d).start()

        with jax.named_scope("up0"):
            up(0)
        with jax.named_scope("down0"):
            drain(w2b, ld_sem.at[5])
            down_all(0)
        with jax.named_scope("up1"):
            up(1)

            @pl.when(more)
            def _():
                up_load(l + 1)

        with jax.named_scope("down1"):
            down_all(1)

            @pl.when(more)
            def _():
                down_load(l + 1)

        with jax.named_scope("finish0"):
            finish(0)
        with jax.named_scope("finish1"):
            finish(1)
        all_ret = yret.at[l, pl.ds(0, (NP * NE - 1) * RE)]
        with jax.named_scope("retwait"):
            drain(all_ret, ret_r)

        with jax.named_scope("gsum"):
            for b in range(NP):
                cols = slice(b * CB, (b + 1) * CB)
                yp = dot(rmat, yret[l, b * SLOTS:(b + 1) * SLOTS]) * gcol
                mixed = yp[0:T]
                for k in range(1, K):
                    mixed = mixed + yp[k * T:(k + 1) * T]
                xs[:, cols] = (a_s[:, cols] + mixed).astype(BF).astype(F32)

        drain(msg.at[l, pl.ds(0, NM)], att_s)
        drain(oag.at[l, pl.ds(0, NM * TU)], og_s)
        drain(uperm.at[l, pl.ds(0, (NR - 1) * RE)], dis_s)
        for g in range(2):
            drain(ys.at[l, g, pl.ds(0, NP - 1)], ys_s.at[g])
        drain(all_ret, ret_s)
        return carry

    lax.fori_loop(0, L, layer, 0)
    out_ref[...] = xs[...].astype(BF)


def solution(mesh):
    tok_spec = P(("dp", "ep"), None)
    cache_spec = P(None, ("dp", "ep"), "pool", None, None)
    up_spec = P(None, "ep", None, "pool")
    down_spec = P(None, "ep", "pool", None)
    in_specs = (tok_spec, cache_spec, cache_spec, P(("dp", "ep")), P(), P(), P(), P(), P(),
                P(None, ("dp", "ep"), None), up_spec, up_spec, down_spec)
    NP, NE = mesh.shape["pool"], mesh.shape["ep"]

    def body(hidden, k_cache, v_cache, cache_len, w_q, w_k, w_v, w_o, w_router, ids, w_one, w_three, w_two):
        L = w_q.shape[0]
        T, D = hidden.shape
        S, G, HD = k_cache.shape[2:]
        NH = w_q.shape[2] // HD
        K = ids.shape[2]
        FF = w_one.shape[3]
        TC = T // NP
        SLOTS, CB, ROWS, SG, UR = T * K, D // NP, TC * NH, S * G, TC // 2 * NH
        assert w_one.shape[1] == 1 and SLOTS == HD and ROWS == HD and w_router.shape[2] == 8 and NP == 4 and G == 2
        dims = (L, T, D, S, G, HD, NH, NP, NE, TC, K, FF)
        kc = k_cache.reshape(L, T, SG, HD)
        vc = v_cache.reshape(L, T, SG, HD)
        wr_t = jnp.swapaxes(w_router, 1, 2)
        ids_t = jnp.swapaxes(ids, 1, 2)
        V = pltpu.VMEM
        dma = pltpu.SemaphoreType.DMA
        anyspec = pl.BlockSpec(memory_space=pl.ANY)
        vspec = pl.BlockSpec(memory_space=pltpu.VMEM)
        scratch = [
            V((T, D), BF), V((T, D), F32), V(ids_t.shape, jnp.int32), V(wr_t.shape, F32),
            V((D, NH * HD), BF), V((2, D, G * HD), BF), V((2 * NP, 2, TC // 2, SG, HD), BF), V((D, D), BF),
            V((D, FF), BF), V((D, FF), BF), V((NP, FF, CB), BF),
            V((T * NH, HD), F32), V((T, 2 * G * HD), F32), V((ROWS, HD), F32), V((ROWS, HD), F32),
            V((ROWS, HD), F32), V((L, 2 * NP, UR + 8, HD), F32), V((L, 2 * NP - 2, UR + 8, HD), F32),
            V((UR, HD), F32), V((L, T, NH * HD), BF),
            V((T, D), F32), V((L, SLOTS, D), BF), V((L, SLOTS, D), BF), V((2, SLOTS // 2, FF), BF),
            V((L, 2, NP, SLOTS // 2, CB), F32), V((L, 2, NP - 1, SLOTS // 2, CB), F32),
            V((L, SLOTS, CB), BF), V((L, NP * SLOTS, CB), BF),
            dma((9,)), dma((2 * NP,)), dma, dma((2,)), dma, dma, dma, dma((2,)), dma((2,)), dma((2,)), dma, dma,
        ]
        return pl.pallas_call(
            functools.partial(layers_kernel, dims),
            out_shape=jax.ShapeDtypeStruct((T, D), BF),
            in_specs=[pl.BlockSpec(memory_space=pltpu.SMEM), anyspec, anyspec, anyspec, anyspec, anyspec, anyspec,
                      anyspec, anyspec, anyspec, anyspec, anyspec, anyspec],
            out_specs=vspec,
            scratch_shapes=scratch,
            name="moe_layers",
            compiler_params=pltpu.CompilerParams(collective_id=0, has_side_effects=True,
                                                 vmem_limit_bytes=60 * 1024 * 1024),
        )(cache_len, hidden, ids_t, kc, vc, w_q, w_k, w_v, w_o, wr_t, w_one, w_three, w_two)

    return jax.shard_map(body, mesh=mesh, in_specs=in_specs, out_specs=tok_spec, check_vma=False)
```

```python
import functools

import jax
import jax.numpy as jnp
from jax import lax
from jax.experimental import pallas as pl
from jax.experimental.pallas import tpu as pltpu
from jax.sharding import PartitionSpec as P

MESH = pl.DeviceIdType.MESH
NORM_EPS = 1e-6
NEG = -1e30
BF = jnp.bfloat16
F32 = jnp.float32
NT = (((1,), (1,)), ((), ()))


def rms_norm(v):
    return v * lax.rsqrt(jnp.mean(v * v, axis=-1, keepdims=True) + NORM_EPS)


def dot(a, b):
    return jnp.dot(a, b, preferred_element_type=F32)


def layers_kernel(dims, len_ref, x_hbm, ids_hbm, k_hbm, v_hbm, wq_hbm, wk_hbm, wv_hbm, wo_hbm, wr_hbm,
                  w1_hbm, w3_hbm, w2_hbm, out_ref,
                  xb, xs, idb, wrb, wqb, wkvb, kvbuf, wob, w1b, w3b, w2b, qrows, kvs, kx, vx, zst, msg, arx, orow, oag,
                  a_s, uperm, xin, act, ys, yrecv, ybf, yret,
                  ld_sem, kv_sem, att_s, att_r, og_s, og_r, dis_s, dis_r, ys_s, ys_r, ret_s, ret_r):
    L, T, D, S, G, HD, NH, NP, NE, TC, K, FF = dims
    QG = NH // G
    SLOTS = T * K
    RE = SLOTS // NE
    CB = D // NP
    SG = S * G
    QW = NH * HD
    KW = G * HD
    TU = TC // 2
    TH = T // 2
    UR = TU * NH
    NU = 2 * NP
    NM = 2 * (NP - 1)
    NX = NE // 2
    BW = 2 * HD
    scale = HD ** -0.5
    p = lax.axis_index("pool")
    e = lax.axis_index("ep")
    chip = lax.div(e, 2)
    core = lax.rem(e, 2)

    def pool_of(d):
        return lax.rem(p + d, NP)

    rel = [(0, 0), (0, 1)] + [(dx, dc) for dx in range(2, NX - 1) for dc in range(2)]
    rel += [(1, 0), (NX - 1, 0), (1, 1), (NX - 1, 1)]
    NR = len(rel)
    groups = [(0, 2), (2, 4), (4, NR)]
    NG = len(groups)
    group_of = [next(g for g in range(NG) if r < groups[g][1]) for r in range(NR)]

    def ep_sender(r):
        return lax.rem(chip + rel[r][0], NX) * 2 + lax.rem(core + rel[r][1], 2)

    def ep_receiver(r):
        return lax.rem(chip + NX - rel[r][0], NX) * 2 + lax.rem(core + rel[r][1], 2)

    def qkv_load(l):
        for b in range(2):
            rows = pl.ds(b * (D // 2), D // 2)
            pltpu.make_async_copy(wq_hbm.at[l, rows], wqb.at[rows], ld_sem.at[0]).start()
        pltpu.make_async_copy(wk_hbm.at[l], wkvb.at[0], ld_sem.at[1]).start()
        pltpu.make_async_copy(wv_hbm.at[l], wkvb.at[1], ld_sem.at[1]).start()

    def drain(ref, sem):
        pltpu.make_async_copy(ref, ref, sem).wait()

    def unit(it, un):
        z = (it + 1) // 2 % 2
        half = z * (it - 1) + (1 - z) * un
        away = z * (1 + 2 * un) + (1 - z) * (2 - 2 * (it // 3))
        return half, away

    def unit_tok(it, un):
        half, away = unit(it, un)
        return half * TH + lax.rem(p + away, NP) * TU

    def kv_load(l, it, un):
        n = 2 * it + un
        tok = pl.ds(pl.multiple_of(unit_tok(it, un), TU), TU)
        pltpu.make_async_copy(k_hbm.at[l, tok], kvbuf.at[n, 0], kv_sem.at[n]).start()
        pltpu.make_async_copy(v_hbm.at[l, tok], kvbuf.at[n, 1], kv_sem.at[n]).start()

    def wo_copy(l):
        return pltpu.make_async_copy(wo_hbm.at[l], wob, ld_sem.at[2])

    def up_load(l):
        pltpu.make_async_copy(w1_hbm.at[l, 0], w1b, ld_sem.at[3]).start()
        pltpu.make_async_copy(w3_hbm.at[l, 0], w3b, ld_sem.at[4]).start()

    def down_load(l):
        for q in range(NP):
            pltpu.make_async_copy(w2_hbm.at[l, 0, :, pl.ds(q * CB, CB)], w2b.at[q], ld_sem.at[5]).start()

    small = [pltpu.make_async_copy(x_hbm, xb, ld_sem.at[6]),
             pltpu.make_async_copy(ids_hbm, idb, ld_sem.at[7]),
             pltpu.make_async_copy(wr_hbm, wrb, ld_sem.at[8])]
    small[0].start()
    qkv_load(0)
    for un in range(2):
        kv_load(0, 0, un)
    small[1].start()
    small[2].start()

    barrier = pltpu.get_barrier_semaphore()
    for dp_ in range(NP):
        for de in range(NE):
            if dp_ or de:
                pl.semaphore_signal(barrier, inc=1,
                                    device_id={"pool": pool_of(dp_), "ep": lax.rem(e + de, NE)},
                                    device_id_type=MESH)

    hrow = lax.broadcasted_iota(jnp.int32, (NH, SG), 0)
    pcol = lax.broadcasted_iota(jnp.int32, (NH, SG), 1)
    posm = jnp.where(lax.rem(pcol, G) == lax.div(hrow, QG), lax.div(pcol, G), jnp.int32(1 << 30))
    lane = lax.broadcasted_iota(jnp.int32, (NH, HD), 1)
    hsub = lax.broadcasted_iota(jnp.int32, (NH, HD), 0)
    NEX = wrb.shape[1]
    ecol = lax.broadcasted_iota(jnp.int32, (NEX, T), 0)

    small[0].wait()
    xs[...] = xb[...].astype(F32)

    def layer(l, carry):
        more = l + 1 < L
        first = l == 0

        def att_send(it, un):
            half, away = unit(it, un)
            return pltpu.make_async_remote_copy(
                src_ref=msg.at[l, 2 * it + un], dst_ref=arx.at[l, half * (NP - 1) + away - 1], send_sem=att_s,
                recv_sem=att_r.at[half],
                device_id={"pool": pool_of(away), "ep": e}, device_id_type=MESH)

        def own_tok(half):
            return pl.ds(pl.multiple_of(half * TH + p * TU, TU), TU)

        def og_send(half, d):
            return pltpu.make_async_remote_copy(
                src_ref=oag.at[l, own_tok(half)], dst_ref=oag.at[l, own_tok(half)], send_sem=og_s, recv_sem=og_r,
                device_id={"pool": pool_of(d), "ep": e}, device_id_type=MESH)

        def dis_send(r):
            dst = ep_receiver(r)
            return pltpu.make_async_remote_copy(
                src_ref=uperm.at[l, pl.ds(pl.multiple_of(dst * RE, RE), RE)], dst_ref=xin.at[l, pl.ds(r * RE, RE)],
                send_sem=dis_s, recv_sem=dis_r.at[group_of[r]],
                device_id={"pool": p, "ep": dst}, device_id_type=MESH)

        def grows(g):
            return pl.ds(groups[g][0] * RE, (groups[g][1] - groups[g][0]) * RE)

        def ys_send(g, d):
            return pltpu.make_async_remote_copy(
                src_ref=ys.at[l, d - 1, grows(g)], dst_ref=yrecv.at[l, d - 1, grows(g)], send_sem=ys_s.at[g],
                recv_sem=ys_r.at[g], device_id={"pool": pool_of(d), "ep": e}, device_id_type=MESH)

        def ret_send(dp_, r):
            dst = ep_sender(r)
            return pltpu.make_async_remote_copy(
                src_ref=ybf.at[l, pl.ds(r * RE, RE)],
                dst_ref=yret.at[l, pl.ds(pl.multiple_of(p * SLOTS + e * RE, RE), RE)], send_sem=ret_s, recv_sem=ret_r,
                device_id={"pool": pool_of(dp_), "ep": dst}, device_id_type=MESH)

        with jax.named_scope("qkv"):
            hn = rms_norm(xs[...]).astype(BF)
            drain(wqb, ld_sem.at[0])
            for b in range(QW // BW):
                r = dot(hn, wqb[:, b * BW:(b + 1) * BW]).astype(BF).astype(F32)
                for j in range(2):
                    qrows[pl.ds(2 * b + j, T, stride=NH), :] = r[:, j * HD:(j + 1) * HD]
            drain(wkvb, ld_sem.at[1])
            for b in range(2):
                kvs[:, b * KW:(b + 1) * KW] = dot(hn, wkvb[b]).astype(BF).astype(F32)

            @pl.when(first)
            def _():
                for un in range(2):
                    kv_load(l, 1, un)

            for half in range(2):
                for h in range(NH):
                    g = h // QG
                    kx[pl.ds(half * UR + h, TU, stride=NH), :] = kvs[own_tok(half), g * HD:(g + 1) * HD]
                    vx[pl.ds(half * UR + h, TU, stride=NH), :] = kvs[own_tok(half), KW + g * HD:KW + (g + 1) * HD]

        def merge(qrow, krow, stats, parts):
            s_new = jnp.sum(qrow * kx[krow, :], axis=1, keepdims=True) * scale
            ms = [c[:, 0:1] for c in stats]
            top = s_new
            for m in ms:
                top = jnp.maximum(top, m)
            p_new = jnp.exp(s_new - top)
            den = p_new
            num = p_new * vx[krow, :]
            for i in range(NP):
                w = jnp.exp(ms[i] - top)
                den = den + w * stats[i][:, 1:2]
                num = num + w * parts[i]
            return num / den

        def combine(half):
            m0 = half * (NP - 1)
            drain(arx.at[l, pl.ds(m0, NP - 1)], att_r.at[half])
            for i in range(NP - 1):
                zst[8 * i:8 * i + 8, :] = arx[l, m0 + i, UR:UR + 8, :]
            zst[8 * (NP - 1):8 * NP, :] = msg[l, NM + half, UR:UR + 8, :]
            zc = zst[...].T
            odd = [0, half, 1, half]
            stats = [zc[odd[i] * UR:(odd[i] + 1) * UR, 8 * i:8 * i + 8] for i in range(NP)]
            parts = [arx[l, m0 + i, 0:UR, :] for i in range(NP - 1)] + [msg[l, NM + half, 0:UR, :]]
            q0 = pl.multiple_of((half * TH + p * TU) * NH, UR)
            orow[...] = merge(qrows[pl.ds(q0, UR), :], pl.ds(half * UR, UR), stats, parts)
            for h in range(NH):
                oag[l, own_tok(half), h * HD:(h + 1) * HD] = orow[pl.ds(h, TU, stride=NH), :].astype(BF)
            for d in (2, 1, 3):
                og_send(half, d).start()

        def chunk(it, c2):
            for un in range(2):
                n = 2 * it + un
                drain(kvbuf.at[n], kv_sem.at[n])

            @pl.when(jnp.logical_and(first, it < 2))
            def _():
                for un in range(2):
                    kv_load(l, it + 2, un)

            @pl.when(jnp.logical_and(first, it == 2))
            def _():
                wo_copy(l).start()
                up_load(l)
                down_load(l)

            mrow = jnp.zeros((NH, HD), F32)
            lrow = jnp.zeros((NH, HD), F32)
            for un in range(2):
                n = 2 * it + un
                t0 = unit_tok(it, un)
                sc = []
                for j in range(TU):
                    t = t0 + j
                    qt = qrows[pl.ds(pl.multiple_of(t * NH, NH), NH), :].astype(BF)
                    s = lax.dot_general(qt, kvbuf[n, 0, j], NT, preferred_element_type=F32) * scale
                    sc.append(jnp.where(posm < len_ref[t] - p * S, s, NEG))
                mx = [jnp.max(s, axis=1, keepdims=True) for s in sc]
                pr = [jnp.exp(s - m) for s, m in zip(sc, mx)]
                ls = [jnp.sum(q, axis=1, keepdims=True) for q in pr]
                for j in range(TU):
                    msg[l, n, j * NH:(j + 1) * NH, :] = dot(pr[j].astype(BF), kvbuf[n, 1, j])
                    here = lane == hsub + (un * UR + j * NH)
                    mrow = jnp.where(here, mx[j], mrow)
                    lrow = jnp.where(here, ls[j], lrow)
            stat = jnp.where(hsub == 0, jnp.sum(mrow, axis=0, keepdims=True), jnp.sum(lrow, axis=0, keepdims=True))
            for un in range(2):
                msg[l, 2 * it + un, UR:UR + NH, :] = stat

            @pl.when(jnp.logical_and(first, it == 0))
            def _():
                pl.semaphore_wait(barrier, NP * NE - 1)

            @pl.when(it < NP - 1)
            def _():
                for un in range(2):
                    att_send(it, un).start()

            return c2

        with jax.named_scope("attn"):
            lax.fori_loop(0, NP, chunk, 0)

        @pl.when(more)
        def _():
            qkv_load(l + 1)
            for n in range(NU):
                kv_load(l + 1, n // 2, n % 2)

        @pl.when(first)
        def _():
            small[1].wait()
            small[2].wait()

        with jax.named_scope("tables"):
            slot_col = lax.broadcasted_iota(jnp.int32, (SLOTS, SLOTS), 0)
            pair_row = lax.broadcasted_iota(jnp.int32, (SLOTS, SLOTS), 1)
            upper = (slot_col < pair_row).astype(F32).astype(BF)
            want_rank = lax.rem(slot_col, RE).astype(F32)
            idrow = jnp.concatenate([idb[l, k:k + 1, :] for k in range(K)], axis=1)
            same = (jnp.broadcast_to(idrow, (SLOTS, SLOTS)) == lax.div(slot_col, RE))
            rank = dot(same.astype(F32).astype(BF), upper)
            pick = jnp.where(jnp.logical_and(same, rank == want_rank), 1.0, 0.0).astype(F32)
            rmat = pick.T.astype(BF)
            dmat = pick[:, 0:T]
            for k in range(1, K):
                dmat = dmat + pick[:, k * T:(k + 1) * T]
            dmat = dmat.astype(BF)
            wr = wrb[l]
            hi = wr.astype(BF).astype(F32)
            mid = (wr - hi).astype(BF).astype(F32)
            lo = wr - hi - mid
            wr3 = jnp.concatenate([hi, mid, lo, jnp.zeros_like(lo)], axis=0).astype(BF)

        with jax.named_scope("comb0"):
            combine(0)
        with jax.named_scope("comb1"):
            combine(1)
        with jax.named_scope("agwait"):
            wo_copy(l).wait()
            drain(oag.at[l, pl.ds(0, NM * TU)], og_r)

        with jax.named_scope("oproj"):
            for b in range(NP):
                cols = slice(b * CB, (b + 1) * CB)
                a_s[:, cols] = (xs[:, cols] + dot(oag[l], wob[:, cols])).astype(BF).astype(F32)

            @pl.when(more)
            def _():
                wo_copy(l + 1).start()

            u = rms_norm(a_s[...]).astype(BF)
            for b in range(NP):
                cols = slice(b * CB, (b + 1) * CB)
                uperm[l, :, cols] = dot(dmat, u[:, cols]).astype(BF)
            for r in range(1, NR):
                dis_send(r).start()
            xin[l, 0:RE, :] = uperm[l, pl.ds(pl.multiple_of(e * RE, RE), RE), :]

        with jax.named_scope("gates"):
            lg3 = lax.dot_general(wr3, u, NT, preferred_element_type=F32)
            lg = lg3[0:NEX] + lg3[NEX:2 * NEX] + lg3[2 * NEX:3 * NEX]
            picked = [jnp.sum(jnp.where(ecol == idb[l, k:k + 1, :], lg, 0.0), axis=0, keepdims=True)
                      for k in range(K)]
            gtop = picked[0]
            for k in range(1, K):
                gtop = jnp.maximum(gtop, picked[k])
            ex = [jnp.exp(v - gtop) for v in picked]
            tot = ex[0]
            for k in range(1, K):
                tot = tot + ex[k]
            grow = jnp.concatenate([v / tot for v in ex], axis=1)
            gcol = jnp.broadcast_to(grow, (SLOTS, SLOTS)).T[:, 0:1]
            drain(w1b, ld_sem.at[3])
            drain(w3b, ld_sem.at[4])

        def up(g):
            r0 = max(1, groups[g][0])
            drain(xin.at[l, pl.ds(r0 * RE, (groups[g][1] - r0) * RE)], dis_r.at[g])
            xe = xin[l, grows(g)]
            f0 = 0
            while f0 < FF:
                fw = min(BW, FF - f0)
                h1 = dot(xe, w1b[:, f0:f0 + fw])
                h3 = dot(xe, w3b[:, f0:f0 + fw])
                act[grows(g), f0:f0 + fw] = (h1 * jax.nn.sigmoid(h1) * h3).astype(BF)
                f0 += fw

        def down(g):
            for d in (2, 1, 3, 0):
                ys[l, (d + NP - 1) % NP, grows(g)] = dot(act[grows(g)], w2b[pool_of(d)])
            for d in (2, 1, 3):
                ys_send(g, d).start()

        def finish(g):
            drain(yrecv.at[l, :, grows(g)], ys_r.at[g])
            tot = ys[l, NP - 1, grows(g)]
            for d in range(1, NP):
                tot = tot + yrecv[l, d - 1, grows(g)]
            ybf[l, grows(g)] = tot.astype(BF)
            for dp_ in (2, 1, 3, 0):
                for r in range(groups[g][1] - 1, groups[g][0] - 1, -1):
                    if dp_ or r:
                        ret_send(dp_, r).start()
            if g == 0:
                yret[l, pl.ds(pl.multiple_of(p * SLOTS + e * RE, RE), RE), :] = ybf[l, 0:RE, :]

        for g in range(NG):
            with jax.named_scope(f"up{g}"):
                up(g)
            if g == 0:
                drain(w2b, ld_sem.at[5])
            with jax.named_scope(f"down{g}"):
                down(g)

        @pl.when(more)
        def _():
            up_load(l + 1)
            down_load(l + 1)

        for g in range(NG):
            with jax.named_scope(f"finish{g}"):
                finish(g)

        all_ret = yret.at[l, pl.ds(0, (NP * NE - 1) * RE)]
        with jax.named_scope("retwait"):
            drain(all_ret, ret_r)

        with jax.named_scope("gsum"):
            for b in range(NP):
                cols = slice(b * CB, (b + 1) * CB)
                yp = dot(rmat, yret[l, b * SLOTS:(b + 1) * SLOTS]) * gcol
                mixed = yp[0:T]
                for k in range(1, K):
                    mixed = mixed + yp[k * T:(k + 1) * T]
                xs[:, cols] = (a_s[:, cols] + mixed).astype(BF).astype(F32)

        drain(msg.at[l, pl.ds(0, NM)], att_s)
        drain(oag.at[l, pl.ds(0, NM * TU)], og_s)
        drain(uperm.at[l, pl.ds(0, (NR - 1) * RE)], dis_s)
        for g in range(NG):
            drain(ys.at[l, pl.ds(0, NP - 1), grows(g)], ys_s.at[g])
        drain(all_ret, ret_s)
        return carry

    lax.fori_loop(0, L, layer, 0)
    out_ref[...] = xs[...].astype(BF)


def solution(mesh):
    tok_spec = P(("dp", "ep"), None)
    cache_spec = P(None, ("dp", "ep"), "pool", None, None)
    up_spec = P(None, "ep", None, "pool")
    down_spec = P(None, "ep", "pool", None)
    in_specs = (tok_spec, cache_spec, cache_spec, P(("dp", "ep")), P(), P(), P(), P(), P(),
                P(None, ("dp", "ep"), None), up_spec, up_spec, down_spec)
    NP, NE = mesh.shape["pool"], mesh.shape["ep"]

    def body(hidden, k_cache, v_cache, cache_len, w_q, w_k, w_v, w_o, w_router, ids, w_one, w_three, w_two):
        L = w_q.shape[0]
        T, D = hidden.shape
        S, G, HD = k_cache.shape[2:]
        NH = w_q.shape[2] // HD
        K = ids.shape[2]
        FF = w_one.shape[3]
        TC = T // NP
        SLOTS, CB, ROWS, SG, UR = T * K, D // NP, TC * NH, S * G, TC // 2 * NH
        assert w_one.shape[1] == 1 and SLOTS == HD and ROWS == HD and w_router.shape[2] == 8 and NP == 4 and G == 2
        dims = (L, T, D, S, G, HD, NH, NP, NE, TC, K, FF)
        kc = k_cache.reshape(L, T, SG, HD)
        vc = v_cache.reshape(L, T, SG, HD)
        wr_t = jnp.swapaxes(w_router, 1, 2)
        ids_t = jnp.swapaxes(ids, 1, 2)
        NG = 3
        V = pltpu.VMEM
        dma = pltpu.SemaphoreType.DMA
        anyspec = pl.BlockSpec(memory_space=pl.ANY)
        vspec = pl.BlockSpec(memory_space=pltpu.VMEM)
        scratch = [
            V((T, D), BF), V((T, D), F32), V(ids_t.shape, jnp.int32), V(wr_t.shape, F32),
            V((D, NH * HD), BF), V((2, D, G * HD), BF), V((2 * NP, 2, TC // 2, SG, HD), BF), V((D, D), BF),
            V((D, FF), BF), V((D, FF), BF), V((NP, FF, CB), BF),
            V((T * NH, HD), F32), V((T, 2 * G * HD), F32), V((ROWS, HD), F32), V((ROWS, HD), F32),
            V((ROWS, HD), F32), V((L, 2 * NP, UR + 8, HD), F32), V((L, 2 * NP - 2, UR + 8, HD), F32),
            V((UR, HD), F32), V((L, T, NH * HD), BF),
            V((T, D), F32), V((L, SLOTS, D), BF), V((L, SLOTS, D), BF), V((SLOTS, FF), BF),
            V((L, NP, SLOTS, CB), F32), V((L, NP - 1, SLOTS, CB), F32),
            V((L, SLOTS, CB), BF), V((L, NP * SLOTS, CB), BF),
            dma((9,)), dma((2 * NP,)), dma, dma((2,)), dma, dma, dma, dma((NG,)), dma((NG,)), dma((NG,)), dma, dma,
        ]
        return pl.pallas_call(
            functools.partial(layers_kernel, dims),
            out_shape=pltpu.VMEM((T, D), BF),
            in_specs=[pl.BlockSpec(memory_space=pltpu.SMEM), anyspec, anyspec, anyspec, anyspec, anyspec, anyspec,
                      anyspec, anyspec, anyspec, anyspec, anyspec, anyspec],
            out_specs=vspec,
            scratch_shapes=scratch,
            name="moe_layers",
            compiler_params=pltpu.CompilerParams(collective_id=0, has_side_effects=True,
                                                 vmem_limit_bytes=60 * 1024 * 1024),
        )(cache_len, hidden, ids_t, kc, vc, w_q, w_k, w_v, w_o, wr_t, w_one, w_three, w_two)

    return jax.shard_map(body, mesh=mesh, in_specs=in_specs, out_specs=tok_spec, check_vma=False)
```

```python
import functools

import jax
import jax.numpy as jnp
from jax import lax
from jax.experimental import pallas as pl
from jax.experimental.pallas import tpu as pltpu
from jax.sharding import PartitionSpec as P

MESH = pl.DeviceIdType.MESH
NORM_EPS = 1e-6
NEG = -1e30
BF = jnp.bfloat16
F32 = jnp.float32
NT = (((1,), (1,)), ((), ()))


def rms_norm(v):
    return v * lax.rsqrt(jnp.mean(v * v, axis=-1, keepdims=True) + NORM_EPS)


def dot(a, b):
    return jnp.dot(a, b, preferred_element_type=F32)


def layers_kernel(dims, len_ref, x_hbm, ids_hbm, k_hbm, v_hbm, wq_hbm, wk_hbm, wv_hbm, wo_hbm, wr_hbm,
                  w1_hbm, w3_hbm, w2_hbm, out_ref,
                  xb, xs, hb, idb, wrb, wqb, wkvb, kvbuf, wob, w1b, w3b, w2b, qrows, kvs, kx, vx, zst, msg, arx, orow, oag,
                  a_s, uperm, xin, act, ys, yrecv, ybf, yret,
                  ld_sem, kv_sem, att_s, att_r, og_s, og_r, dis_s, dis_r, ys_s, ys_r, ret_s, ret_r):
    L, T, D, S, G, HD, NH, NP, NE, TC, K, FF = dims
    QG = NH // G
    SLOTS = T * K
    RE = SLOTS // NE
    CB = D // NP
    SG = S * G
    QW = NH * HD
    KW = G * HD
    TU = TC // 2
    TH = T // 2
    UR = TU * NH
    NU = 2 * NP
    NM = 2 * (NP - 1)
    NX = NE // 2
    BW = 2 * HD
    scale = HD ** -0.5
    p = lax.axis_index("pool")
    e = lax.axis_index("ep")
    chip = lax.div(e, 2)
    core = lax.rem(e, 2)

    def pool_of(d):
        return lax.rem(p + d, NP)

    rel = [(0, 0), (0, 1)] + [(dx, dc) for dx in range(2, NX - 1) for dc in range(2)]
    rel += [(1, 0), (NX - 1, 0), (1, 1), (NX - 1, 1)]
    NR = len(rel)
    groups = [(0, 2), (2, 4), (4, 6), (6, NR)]
    NG = len(groups)
    group_of = [next(g for g in range(NG) if groups[g][0] <= r < groups[g][1]) for r in range(NR)]

    def ep_sender(r):
        return lax.rem(chip + rel[r][0], NX) * 2 + lax.rem(core + rel[r][1], 2)

    def ep_receiver(r):
        return lax.rem(chip + NX - rel[r][0], NX) * 2 + lax.rem(core + rel[r][1], 2)

    def wq_load(l):
        for b in range(2):
            rows = pl.ds(b * (D // 2), D // 2)
            pltpu.make_async_copy(wq_hbm.at[l, rows], wqb.at[rows], ld_sem.at[0]).start()

    def wkv_load(l):
        pltpu.make_async_copy(wk_hbm.at[l], wkvb.at[0], ld_sem.at[1]).start()
        pltpu.make_async_copy(wv_hbm.at[l], wkvb.at[1], ld_sem.at[1]).start()

    def drain(ref, sem):
        pltpu.make_async_copy(ref, ref, sem).wait()

    def unit(it, un):
        z = (it + 1) // 2 % 2
        half = z * (it - 1) + (1 - z) * un
        away = z * (1 + 2 * un) + (1 - z) * (2 - 2 * (it // 3))
        return half, away

    def unit_tok(it, un):
        half, away = unit(it, un)
        return half * TH + lax.rem(p + away, NP) * TU

    def kv_load(l, it, un):
        n = 2 * it + un
        tok = pl.ds(pl.multiple_of(unit_tok(it, un), TU), TU)
        pltpu.make_async_copy(k_hbm.at[l, tok], kvbuf.at[n, 0], kv_sem.at[n]).start()
        pltpu.make_async_copy(v_hbm.at[l, tok], kvbuf.at[n, 1], kv_sem.at[n]).start()

    def wo_copy(l):
        return pltpu.make_async_copy(wo_hbm.at[l], wob, ld_sem.at[2])

    def up_load(l):
        pltpu.make_async_copy(w1_hbm.at[l, 0], w1b, ld_sem.at[3]).start()
        pltpu.make_async_copy(w3_hbm.at[l, 0], w3b, ld_sem.at[4]).start()

    def down_load(l):
        for q in range(NP):
            pltpu.make_async_copy(w2_hbm.at[l, 0, :, pl.ds(q * CB, CB)], w2b.at[q], ld_sem.at[5]).start()

    small = [pltpu.make_async_copy(x_hbm, xb, ld_sem.at[6]),
             pltpu.make_async_copy(ids_hbm, idb, ld_sem.at[7]),
             pltpu.make_async_copy(wr_hbm, wrb, ld_sem.at[8])]
    small[0].start()
    wq_load(0)
    for un in range(2):
        kv_load(0, 0, un)
    small[1].start()
    small[2].start()

    barrier = pltpu.get_barrier_semaphore()
    for dp_ in range(NP):
        for de in range(NE):
            if dp_ or de:
                pl.semaphore_signal(barrier, inc=1,
                                    device_id={"pool": pool_of(dp_), "ep": lax.rem(e + de, NE)},
                                    device_id_type=MESH)

    hrow = lax.broadcasted_iota(jnp.int32, (NH, SG), 0)
    pcol = lax.broadcasted_iota(jnp.int32, (NH, SG), 1)
    posm = jnp.where(lax.rem(pcol, G) == lax.div(hrow, QG), lax.div(pcol, G), jnp.int32(1 << 30))
    lane = lax.broadcasted_iota(jnp.int32, (NH, HD), 1)
    hsub = lax.broadcasted_iota(jnp.int32, (NH, HD), 0)
    NEX = wrb.shape[1]
    ecol = lax.broadcasted_iota(jnp.int32, (NEX, T), 0)

    small[0].wait()
    xs[...] = xb[...].astype(F32)

    def layer(l, carry):
        more = l + 1 < L
        first = l == 0

        def att_send(it, un):
            half, away = unit(it, un)
            return pltpu.make_async_remote_copy(
                src_ref=msg.at[l, 2 * it + un], dst_ref=arx.at[l, half * (NP - 1) + away - 1], send_sem=att_s,
                recv_sem=att_r.at[half],
                device_id={"pool": pool_of(away), "ep": e}, device_id_type=MESH)

        def own_tok(half):
            return pl.ds(pl.multiple_of(half * TH + p * TU, TU), TU)

        def og_send(half, d):
            return pltpu.make_async_remote_copy(
                src_ref=oag.at[l, own_tok(half)], dst_ref=oag.at[l, own_tok(half)], send_sem=og_s, recv_sem=og_r,
                device_id={"pool": pool_of(d), "ep": e}, device_id_type=MESH)

        def dis_send(r):
            dst = ep_receiver(r)
            return pltpu.make_async_remote_copy(
                src_ref=uperm.at[l, pl.ds(pl.multiple_of(dst * RE, RE), RE)], dst_ref=xin.at[l, pl.ds(r * RE, RE)],
                send_sem=dis_s, recv_sem=dis_r.at[group_of[r]],
                device_id={"pool": p, "ep": dst}, device_id_type=MESH)

        def grows(g):
            return pl.ds(groups[g][0] * RE, (groups[g][1] - groups[g][0]) * RE)

        def ys_send(g, d):
            return pltpu.make_async_remote_copy(
                src_ref=ys.at[l, d - 1, grows(g)], dst_ref=yrecv.at[l, d - 1, grows(g)], send_sem=ys_s.at[g],
                recv_sem=ys_r.at[g], device_id={"pool": pool_of(d), "ep": e}, device_id_type=MESH)

        def ret_send(dp_, r):
            dst = ep_sender(r)
            return pltpu.make_async_remote_copy(
                src_ref=ybf.at[l, pl.ds(r * RE, RE)],
                dst_ref=yret.at[l, pl.ds(pl.multiple_of(p * SLOTS + e * RE, RE), RE)], send_sem=ret_s, recv_sem=ret_r,
                device_id={"pool": pool_of(dp_), "ep": dst}, device_id_type=MESH)

        with jax.named_scope("qkv"):
            hn = rms_norm(xs[...]).astype(BF)
            drain(wqb, ld_sem.at[0])
            for b in range(QW // BW):
                r = dot(hn, wqb[:, b * BW:(b + 1) * BW]).astype(BF).astype(F32)
                for j in range(2):
                    qrows[pl.ds(2 * b + j, T, stride=NH), :] = r[:, j * HD:(j + 1) * HD]
            hb[...] = hn

            @pl.when(first)
            def _():
                for un in range(2):
                    kv_load(l, 1, un)
                wkv_load(l)

        def merge(qrow, krow, stats, parts):
            s_new = jnp.sum(qrow * kx[krow, :], axis=1, keepdims=True) * scale
            ms = [c[:, 0:1] for c in stats]
            top = s_new
            for m in ms:
                top = jnp.maximum(top, m)
            p_new = jnp.exp(s_new - top)
            den = p_new
            num = p_new * vx[krow, :]
            for i in range(NP):
                w = jnp.exp(ms[i] - top)
                den = den + w * stats[i][:, 1:2]
                num = num + w * parts[i]
            return num / den

        def combine(half):
            m0 = half * (NP - 1)
            drain(arx.at[l, pl.ds(m0, NP - 1)], att_r.at[half])
            for i in range(NP - 1):
                zst[8 * i:8 * i + 8, :] = arx[l, m0 + i, UR:UR + 8, :]
            zst[8 * (NP - 1):8 * NP, :] = msg[l, NM + half, UR:UR + 8, :]
            zc = zst[...].T
            odd = [0, half, 1, half]
            stats = [zc[odd[i] * UR:(odd[i] + 1) * UR, 8 * i:8 * i + 8] for i in range(NP)]
            parts = [arx[l, m0 + i, 0:UR, :] for i in range(NP - 1)] + [msg[l, NM + half, 0:UR, :]]
            q0 = pl.multiple_of((half * TH + p * TU) * NH, UR)
            orow[...] = merge(qrows[pl.ds(q0, UR), :], pl.ds(half * UR, UR), stats, parts)
            for h in range(NH):
                oag[l, own_tok(half), h * HD:(h + 1) * HD] = orow[pl.ds(h, TU, stride=NH), :].astype(BF)
            for d in (2, 1, 3):
                og_send(half, d).start()

        def chunk(it, c2):
            for un in range(2):
                n = 2 * it + un
                drain(kvbuf.at[n], kv_sem.at[n])

            @pl.when(jnp.logical_and(first, it < 2))
            def _():
                for un in range(2):
                    kv_load(l, it + 2, un)

            @pl.when(jnp.logical_and(first, it == 2))
            def _():
                wo_copy(l).start()
                up_load(l)
                down_load(l)

            mrow = jnp.zeros((NH, HD), F32)
            lrow = jnp.zeros((NH, HD), F32)
            for un in range(2):
                n = 2 * it + un
                t0 = unit_tok(it, un)
                sc = []
                for j in range(TU):
                    t = t0 + j
                    qt = qrows[pl.ds(pl.multiple_of(t * NH, NH), NH), :].astype(BF)
                    s = lax.dot_general(qt, kvbuf[n, 0, j], NT, preferred_element_type=F32) * scale
                    sc.append(jnp.where(posm < len_ref[t] - p * S, s, NEG))
                mx = [jnp.max(s, axis=1, keepdims=True) for s in sc]
                pr = [jnp.exp(s - m) for s, m in zip(sc, mx)]
                ls = [jnp.sum(q, axis=1, keepdims=True) for q in pr]
                for j in range(TU):
                    msg[l, n, j * NH:(j + 1) * NH, :] = dot(pr[j].astype(BF), kvbuf[n, 1, j])
                    here = lane == hsub + (un * UR + j * NH)
                    mrow = jnp.where(here, mx[j], mrow)
                    lrow = jnp.where(here, ls[j], lrow)
            stat = jnp.where(hsub == 0, jnp.sum(mrow, axis=0, keepdims=True), jnp.sum(lrow, axis=0, keepdims=True))
            for un in range(2):
                msg[l, 2 * it + un, UR:UR + NH, :] = stat

            @pl.when(jnp.logical_and(first, it == 0))
            def _():
                pl.semaphore_wait(barrier, NP * NE - 1)

            @pl.when(it < NP - 1)
            def _():
                for un in range(2):
                    att_send(it, un).start()

            return c2

        with jax.named_scope("attn"):
            lax.fori_loop(0, NP, chunk, 0)

        with jax.named_scope("kvproj"):
            drain(wkvb, ld_sem.at[1])
            for b in range(2):
                kvs[:, b * KW:(b + 1) * KW] = dot(hb[...], wkvb[b]).astype(BF).astype(F32)

            for half in range(2):
                for h in range(NH):
                    g = h // QG
                    kx[pl.ds(half * UR + h, TU, stride=NH), :] = kvs[own_tok(half), g * HD:(g + 1) * HD]
                    vx[pl.ds(half * UR + h, TU, stride=NH), :] = kvs[own_tok(half), KW + g * HD:KW + (g + 1) * HD]

        @pl.when(more)
        def _():
            wq_load(l + 1)
            wkv_load(l + 1)
            for n in range(NU):
                kv_load(l + 1, n // 2, n % 2)

        @pl.when(first)
        def _():
            small[1].wait()
            small[2].wait()

        with jax.named_scope("tables"):
            slot_col = lax.broadcasted_iota(jnp.int32, (SLOTS, SLOTS), 0)
            pair_row = lax.broadcasted_iota(jnp.int32, (SLOTS, SLOTS), 1)
            upper = (slot_col < pair_row).astype(F32).astype(BF)
            want_rank = lax.rem(slot_col, RE).astype(F32)
            idrow = jnp.concatenate([idb[l, k:k + 1, :] for k in range(K)], axis=1)
            same = (jnp.broadcast_to(idrow, (SLOTS, SLOTS)) == lax.div(slot_col, RE))
            rank = dot(same.astype(F32).astype(BF), upper)
            pick = jnp.where(jnp.logical_and(same, rank == want_rank), 1.0, 0.0).astype(F32)
            rmat = pick.T.astype(BF)
            dmat = pick[:, 0:T]
            for k in range(1, K):
                dmat = dmat + pick[:, k * T:(k + 1) * T]
            dmat = dmat.astype(BF)
            wr = wrb[l]
            hi = wr.astype(BF).astype(F32)
            mid = (wr - hi).astype(BF).astype(F32)
            lo = wr - hi - mid
            wr3 = jnp.concatenate([hi, mid, lo, jnp.zeros_like(lo)], axis=0).astype(BF)

        with jax.named_scope("comb0"):
            combine(0)
        with jax.named_scope("comb1"):
            combine(1)
        with jax.named_scope("agwait"):
            wo_copy(l).wait()
            drain(oag.at[l, pl.ds(0, NM * TU)], og_r)

        with jax.named_scope("oproj"):
            for b in range(NP):
                cols = slice(b * CB, (b + 1) * CB)
                a_s[:, cols] = (xs[:, cols] + dot(oag[l], wob[:, cols])).astype(BF).astype(F32)

            @pl.when(more)
            def _():
                wo_copy(l + 1).start()

            u = rms_norm(a_s[...]).astype(BF)
            for b in range(NP):
                cols = slice(b * CB, (b + 1) * CB)
                uperm[l, :, cols] = dot(dmat, u[:, cols]).astype(BF)
            for r in range(1, NR):
                dis_send(r).start()
            xin[l, 0:RE, :] = uperm[l, pl.ds(pl.multiple_of(e * RE, RE), RE), :]

        with jax.named_scope("gates"):
            lg3 = lax.dot_general(wr3, u, NT, preferred_element_type=F32)
            lg = lg3[0:NEX] + lg3[NEX:2 * NEX] + lg3[2 * NEX:3 * NEX]
            picked = [jnp.sum(jnp.where(ecol == idb[l, k:k + 1, :], lg, 0.0), axis=0, keepdims=True)
                      for k in range(K)]
            gtop = picked[0]
            for k in range(1, K):
                gtop = jnp.maximum(gtop, picked[k])
            ex = [jnp.exp(v - gtop) for v in picked]
            tot = ex[0]
            for k in range(1, K):
                tot = tot + ex[k]
            grow = jnp.concatenate([v / tot for v in ex], axis=1)
            gcol = jnp.broadcast_to(grow, (SLOTS, SLOTS)).T[:, 0:1]
            drain(w1b, ld_sem.at[3])
            drain(w3b, ld_sem.at[4])

        def up(g):
            r0 = max(1, groups[g][0])
            drain(xin.at[l, pl.ds(r0 * RE, (groups[g][1] - r0) * RE)], dis_r.at[g])
            xe = xin[l, grows(g)]
            f0 = 0
            while f0 < FF:
                fw = min(BW, FF - f0)
                h1 = dot(xe, w1b[:, f0:f0 + fw])
                h3 = dot(xe, w3b[:, f0:f0 + fw])
                act[grows(g), f0:f0 + fw] = (h1 * jax.nn.sigmoid(h1) * h3).astype(BF)
                f0 += fw

        def down(g):
            for d in (2, 1, 3, 0):
                ys[l, (d + NP - 1) % NP, grows(g)] = dot(act[grows(g)], w2b[pool_of(d)])
            for d in (2, 1, 3):
                ys_send(g, d).start()

        def finish(g):
            drain(yrecv.at[l, :, grows(g)], ys_r.at[g])
            tot = ys[l, NP - 1, grows(g)]
            for d in range(1, NP):
                tot = tot + yrecv[l, d - 1, grows(g)]
            ybf[l, grows(g)] = tot.astype(BF)
            for dp_ in (2, 1, 3, 0):
                for r in range(groups[g][1] - 1, groups[g][0] - 1, -1):
                    if dp_ or r:
                        ret_send(dp_, r).start()
            if g == 0:
                yret[l, pl.ds(pl.multiple_of(p * SLOTS + e * RE, RE), RE), :] = ybf[l, 0:RE, :]

        for g in range(NG):
            with jax.named_scope(f"up{g}"):
                up(g)
            if g == 0:
                drain(w2b, ld_sem.at[5])
            with jax.named_scope(f"down{g}"):
                down(g)

        @pl.when(more)
        def _():
            up_load(l + 1)
            down_load(l + 1)

        for g in range(NG):
            with jax.named_scope(f"finish{g}"):
                finish(g)

        all_ret = yret.at[l, pl.ds(0, (NP * NE - 1) * RE)]
        with jax.named_scope("retwait"):
            drain(all_ret, ret_r)

        with jax.named_scope("gsum"):
            for b in range(NP):
                cols = slice(b * CB, (b + 1) * CB)
                yp = dot(rmat, yret[l, b * SLOTS:(b + 1) * SLOTS]) * gcol
                mixed = yp[0:T]
                for k in range(1, K):
                    mixed = mixed + yp[k * T:(k + 1) * T]
                xs[:, cols] = (a_s[:, cols] + mixed).astype(BF).astype(F32)

        drain(msg.at[l, pl.ds(0, NM)], att_s)
        drain(oag.at[l, pl.ds(0, NM * TU)], og_s)
        drain(uperm.at[l, pl.ds(0, (NR - 1) * RE)], dis_s)
        for g in range(NG):
            drain(ys.at[l, pl.ds(0, NP - 1), grows(g)], ys_s.at[g])
        drain(all_ret, ret_s)
        return carry

    lax.fori_loop(0, L, layer, 0)
    out_ref[...] = xs[...].astype(BF)


def solution(mesh):
    tok_spec = P(("dp", "ep"), None)
    cache_spec = P(None, ("dp", "ep"), "pool", None, None)
    up_spec = P(None, "ep", None, "pool")
    down_spec = P(None, "ep", "pool", None)
    in_specs = (tok_spec, cache_spec, cache_spec, P(("dp", "ep")), P(), P(), P(), P(), P(),
                P(None, ("dp", "ep"), None), up_spec, up_spec, down_spec)
    NP, NE = mesh.shape["pool"], mesh.shape["ep"]

    def body(hidden, k_cache, v_cache, cache_len, w_q, w_k, w_v, w_o, w_router, ids, w_one, w_three, w_two):
        L = w_q.shape[0]
        T, D = hidden.shape
        S, G, HD = k_cache.shape[2:]
        NH = w_q.shape[2] // HD
        K = ids.shape[2]
        FF = w_one.shape[3]
        TC = T // NP
        SLOTS, CB, ROWS, SG, UR = T * K, D // NP, TC * NH, S * G, TC // 2 * NH
        assert w_one.shape[1] == 1 and SLOTS == HD and ROWS == HD and w_router.shape[2] == 8 and NP == 4 and G == 2
        dims = (L, T, D, S, G, HD, NH, NP, NE, TC, K, FF)
        kc = k_cache.reshape(L, T, SG, HD)
        vc = v_cache.reshape(L, T, SG, HD)
        wr_t = jnp.swapaxes(w_router, 1, 2)
        ids_t = jnp.swapaxes(ids, 1, 2)
        NG = 4
        V = pltpu.VMEM
        dma = pltpu.SemaphoreType.DMA
        anyspec = pl.BlockSpec(memory_space=pl.ANY)
        vspec = pl.BlockSpec(memory_space=pltpu.VMEM)
        scratch = [
            V((T, D), BF), V((T, D), F32), V((T, D), BF), V(ids_t.shape, jnp.int32), V(wr_t.shape, F32),
            V((D, NH * HD), BF), V((2, D, G * HD), BF), V((2 * NP, 2, TC // 2, SG, HD), BF), V((D, D), BF),
            V((D, FF), BF), V((D, FF), BF), V((NP, FF, CB), BF),
            V((T * NH, HD), F32), V((T, 2 * G * HD), F32), V((ROWS, HD), F32), V((ROWS, HD), F32),
            V((ROWS, HD), F32), V((L, 2 * NP, UR + 8, HD), F32), V((L, 2 * NP - 2, UR + 8, HD), F32),
            V((UR, HD), F32), V((L, T, NH * HD), BF),
            V((T, D), F32), V((L, SLOTS, D), BF), V((L, SLOTS, D), BF), V((SLOTS, FF), BF),
            V((L, NP, SLOTS, CB), F32), V((L, NP - 1, SLOTS, CB), F32),
            V((L, SLOTS, CB), BF), V((L, NP * SLOTS, CB), BF),
            dma((9,)), dma((2 * NP,)), dma, dma((2,)), dma, dma, dma, dma((NG,)), dma((NG,)), dma((NG,)), dma, dma,
        ]
        return pl.pallas_call(
            functools.partial(layers_kernel, dims),
            out_shape=pltpu.VMEM((T, D), BF),
            in_specs=[pl.BlockSpec(memory_space=pltpu.SMEM), anyspec, anyspec, anyspec, anyspec, anyspec, anyspec,
                      anyspec, anyspec, anyspec, anyspec, anyspec, anyspec],
            out_specs=vspec,
            scratch_shapes=scratch,
            name="moe_layers",
            compiler_params=pltpu.CompilerParams(collective_id=0, has_side_effects=True,
                                                 vmem_limit_bytes=60 * 1024 * 1024),
        )(cache_len, hidden, ids_t, kc, vc, w_q, w_k, w_v, w_o, wr_t, w_one, w_three, w_two)

    return jax.shard_map(body, mesh=mesh, in_specs=in_specs, out_specs=tok_spec, check_vma=False)
```

```python
import functools

import jax
import jax.numpy as jnp
from jax import lax
from jax.experimental import pallas as pl
from jax.experimental.pallas import tpu as pltpu
from jax.sharding import PartitionSpec as P

MESH = pl.DeviceIdType.MESH
NORM_EPS = 1e-6
NEG = -1e30
BF = jnp.bfloat16
F32 = jnp.float32
NT = (((1,), (1,)), ((), ()))


def rms_norm(v):
    return v * lax.rsqrt(jnp.mean(v * v, axis=-1, keepdims=True) + NORM_EPS)


def dot(a, b):
    return jnp.dot(a, b, preferred_element_type=F32)


def layers_kernel(dims, len_hbm, x_hbm, ids_hbm, k_hbm, v_hbm, wq_hbm, wk_hbm, wv_hbm, wo_hbm, wr_hbm,
                  w1_hbm, w3_hbm, w2_hbm, out_ref,
                  len_ref, xb, xs, hb, idb, wrb, wqb, wkvb, kvbuf, wob, w1b, w3b, w2b, qrows, kvs, kx, vx, zst, msg, arx, orow, oag,
                  a_s, uperm, xin, act, ys, yrecv, ybf, yret,
                  ld_sem, kv_sem, att_s, att_r, og_s, og_r, dis_s, dis_r, ys_s, ys_r, ret_s, ret_r):
    L, T, D, S, G, HD, NH, NP, NE, TC, K, FF = dims
    QG = NH // G
    SLOTS = T * K
    RE = SLOTS // NE
    CB = D // NP
    SG = S * G
    QW = NH * HD
    KW = G * HD
    TU = TC // 2
    TH = T // 2
    UR = TU * NH
    NU = 2 * NP
    NM = 2 * (NP - 1)
    NX = NE // 2
    BW = 2 * HD
    scale = HD ** -0.5
    p = lax.axis_index("pool")
    e = lax.axis_index("ep")
    chip = lax.div(e, 2)
    core = lax.rem(e, 2)

    def pool_of(d):
        return lax.rem(p + d, NP)

    rel = [(0, 0), (0, 1)] + [(dx, dc) for dx in range(2, NX - 1) for dc in range(2)]
    rel += [(1, 0), (NX - 1, 0), (1, 1), (NX - 1, 1)]
    NR = len(rel)
    groups = [(0, 2), (2, 4), (4, 6), (6, NR)]
    NG = len(groups)
    group_of = [next(g for g in range(NG) if groups[g][0] <= r < groups[g][1]) for r in range(NR)]

    def ep_sender(r):
        return lax.rem(chip + rel[r][0], NX) * 2 + lax.rem(core + rel[r][1], 2)

    def ep_receiver(r):
        return lax.rem(chip + NX - rel[r][0], NX) * 2 + lax.rem(core + rel[r][1], 2)

    def wq_load(l):
        for b in range(2):
            rows = pl.ds(b * (D // 2), D // 2)
            pltpu.make_async_copy(wq_hbm.at[l, rows], wqb.at[rows], ld_sem.at[0]).start()

    def wkv_load(l):
        pltpu.make_async_copy(wk_hbm.at[l], wkvb.at[0], ld_sem.at[1]).start()
        pltpu.make_async_copy(wv_hbm.at[l], wkvb.at[1], ld_sem.at[1]).start()

    def drain(ref, sem):
        pltpu.make_async_copy(ref, ref, sem).wait()

    def unit(it, un):
        z = (it + 1) // 2 % 2
        half = z * (it - 1) + (1 - z) * un
        away = z * (1 + 2 * un) + (1 - z) * (2 - 2 * (it // 3))
        return half, away

    def unit_tok(it, un):
        half, away = unit(it, un)
        return half * TH + lax.rem(p + away, NP) * TU

    def kv_load(l, it, un):
        n = 2 * it + un
        tok = pl.ds(pl.multiple_of(unit_tok(it, un), TU), TU)
        pltpu.make_async_copy(k_hbm.at[l, tok], kvbuf.at[n, 0], kv_sem.at[n]).start()
        pltpu.make_async_copy(v_hbm.at[l, tok], kvbuf.at[n, 1], kv_sem.at[n]).start()

    def wo_copy(l):
        return pltpu.make_async_copy(wo_hbm.at[l], wob, ld_sem.at[2])

    def up_load(l):
        pltpu.make_async_copy(w1_hbm.at[l, 0], w1b, ld_sem.at[3]).start()
        pltpu.make_async_copy(w3_hbm.at[l, 0], w3b, ld_sem.at[4]).start()

    def down_load(l):
        for q in range(NP):
            pltpu.make_async_copy(w2_hbm.at[l, 0, :, pl.ds(q * CB, CB)], w2b.at[q], ld_sem.at[5]).start()

    small = [pltpu.make_async_copy(x_hbm, xb, ld_sem.at[6]),
             pltpu.make_async_copy(ids_hbm, idb, ld_sem.at[7]),
             pltpu.make_async_copy(wr_hbm, wrb, ld_sem.at[8]),
             pltpu.make_async_copy(len_hbm, len_ref, ld_sem.at[9])]
    small[0].start()
    small[3].start()
    wq_load(0)
    for un in range(2):
        kv_load(0, 0, un)
    small[1].start()
    small[2].start()

    barrier = pltpu.get_barrier_semaphore()
    for dp_ in range(NP):
        for de in range(NE):
            if dp_ or de:
                pl.semaphore_signal(barrier, inc=1,
                                    device_id={"pool": pool_of(dp_), "ep": lax.rem(e + de, NE)},
                                    device_id_type=MESH)

    hrow = lax.broadcasted_iota(jnp.int32, (NH, SG), 0)
    pcol = lax.broadcasted_iota(jnp.int32, (NH, SG), 1)
    posm = jnp.where(lax.rem(pcol, G) == lax.div(hrow, QG), lax.div(pcol, G), jnp.int32(1 << 30))
    lane = lax.broadcasted_iota(jnp.int32, (NH, HD), 1)
    hsub = lax.broadcasted_iota(jnp.int32, (NH, HD), 0)
    NEX = wrb.shape[1]
    ecol = lax.broadcasted_iota(jnp.int32, (NEX, T), 0)

    small[0].wait()
    xs[...] = xb[...].astype(F32)

    def layer(l, carry):
        more = l + 1 < L
        first = l == 0

        def att_send(it, un):
            half, away = unit(it, un)
            return pltpu.make_async_remote_copy(
                src_ref=msg.at[l, 2 * it + un], dst_ref=arx.at[l, half * (NP - 1) + away - 1], send_sem=att_s,
                recv_sem=att_r.at[half],
                device_id={"pool": pool_of(away), "ep": e}, device_id_type=MESH)

        def own_tok(half):
            return pl.ds(pl.multiple_of(half * TH + p * TU, TU), TU)

        def og_send(half, d):
            return pltpu.make_async_remote_copy(
                src_ref=oag.at[l, own_tok(half)], dst_ref=oag.at[l, own_tok(half)], send_sem=og_s, recv_sem=og_r,
                device_id={"pool": pool_of(d), "ep": e}, device_id_type=MESH)

        def dis_send(r):
            dst = ep_receiver(r)
            return pltpu.make_async_remote_copy(
                src_ref=uperm.at[l, pl.ds(pl.multiple_of(dst * RE, RE), RE)], dst_ref=xin.at[l, pl.ds(r * RE, RE)],
                send_sem=dis_s, recv_sem=dis_r.at[group_of[r]],
                device_id={"pool": p, "ep": dst}, device_id_type=MESH)

        def grows(g):
            return pl.ds(groups[g][0] * RE, (groups[g][1] - groups[g][0]) * RE)

        def ys_send(g, d):
            return pltpu.make_async_remote_copy(
                src_ref=ys.at[l, d - 1, grows(g)], dst_ref=yrecv.at[l, d - 1, grows(g)], send_sem=ys_s.at[g],
                recv_sem=ys_r.at[g], device_id={"pool": pool_of(d), "ep": e}, device_id_type=MESH)

        def ret_send(dp_, r):
            dst = ep_sender(r)
            return pltpu.make_async_remote_copy(
                src_ref=ybf.at[l, pl.ds(r * RE, RE)],
                dst_ref=yret.at[l, pl.ds(pl.multiple_of(p * SLOTS + e * RE, RE), RE)], send_sem=ret_s, recv_sem=ret_r,
                device_id={"pool": pool_of(dp_), "ep": dst}, device_id_type=MESH)

        with jax.named_scope("qkv"):
            hn = rms_norm(xs[...]).astype(BF)
            drain(wqb, ld_sem.at[0])

            @pl.when(first)
            def _():
                small[3].wait()

            for b in range(QW // BW):
                r = dot(hn, wqb[:, b * BW:(b + 1) * BW]).astype(BF).astype(F32)
                for j in range(2):
                    qrows[pl.ds(2 * b + j, T, stride=NH), :] = r[:, j * HD:(j + 1) * HD]
            hb[...] = hn

            @pl.when(first)
            def _():
                for un in range(2):
                    kv_load(l, 1, un)
                for un in range(2):
                    kv_load(l, 2, un)

        def merge(qrow, krow, stats, parts):
            s_new = jnp.sum(qrow * kx[krow, :], axis=1, keepdims=True) * scale
            ms = [c[:, 0:1] for c in stats]
            top = s_new
            for m in ms:
                top = jnp.maximum(top, m)
            p_new = jnp.exp(s_new - top)
            den = p_new
            num = p_new * vx[krow, :]
            for i in range(NP):
                w = jnp.exp(ms[i] - top)
                den = den + w * stats[i][:, 1:2]
                num = num + w * parts[i]
            return num / den

        def combine(half):
            m0 = half * (NP - 1)
            drain(arx.at[l, pl.ds(m0, NP - 1)], att_r.at[half])
            for i in range(NP - 1):
                zst[8 * i:8 * i + 8, :] = arx[l, m0 + i, UR:UR + 8, :]
            zst[8 * (NP - 1):8 * NP, :] = msg[l, NM + half, UR:UR + 8, :]
            zc = zst[...].T
            odd = [0, half, 1, half]
            stats = [zc[odd[i] * UR:(odd[i] + 1) * UR, 8 * i:8 * i + 8] for i in range(NP)]
            parts = [arx[l, m0 + i, 0:UR, :] for i in range(NP - 1)] + [msg[l, NM + half, 0:UR, :]]
            q0 = pl.multiple_of((half * TH + p * TU) * NH, UR)
            orow[...] = merge(qrows[pl.ds(q0, UR), :], pl.ds(half * UR, UR), stats, parts)
            for h in range(NH):
                oag[l, own_tok(half), h * HD:(h + 1) * HD] = orow[pl.ds(h, TU, stride=NH), :].astype(BF)
            for d in (2, 1, 3):
                og_send(half, d).start()

        def chunk(it, c2):
            for un in range(2):
                n = 2 * it + un
                drain(kvbuf.at[n], kv_sem.at[n])

            @pl.when(jnp.logical_and(first, it == 0))
            def _():
                for un in range(2):
                    kv_load(l, 3, un)

            @pl.when(jnp.logical_and(first, it == 2))
            def _():
                wkv_load(l)
                wo_copy(l).start()
                up_load(l)
                down_load(l)

            mrow = jnp.zeros((NH, HD), F32)
            lrow = jnp.zeros((NH, HD), F32)
            for un in range(2):
                n = 2 * it + un
                t0 = unit_tok(it, un)
                sc = []
                for j in range(TU):
                    t = t0 + j
                    qt = qrows[pl.ds(pl.multiple_of(t * NH, NH), NH), :].astype(BF)
                    s = lax.dot_general(qt, kvbuf[n, 0, j], NT, preferred_element_type=F32) * scale
                    sc.append(jnp.where(posm < len_ref[t] - p * S, s, NEG))
                mx = [jnp.max(s, axis=1, keepdims=True) for s in sc]
                pr = [jnp.exp(s - m) for s, m in zip(sc, mx)]
                ls = [jnp.sum(q, axis=1, keepdims=True) for q in pr]
                for j in range(TU):
                    msg[l, n, j * NH:(j + 1) * NH, :] = dot(pr[j].astype(BF), kvbuf[n, 1, j])
                    here = lane == hsub + (un * UR + j * NH)
                    mrow = jnp.where(here, mx[j], mrow)
                    lrow = jnp.where(here, ls[j], lrow)
            stat = jnp.where(hsub == 0, jnp.sum(mrow, axis=0, keepdims=True), jnp.sum(lrow, axis=0, keepdims=True))
            for un in range(2):
                msg[l, 2 * it + un, UR:UR + NH, :] = stat

            @pl.when(jnp.logical_and(first, it == 0))
            def _():
                pl.semaphore_wait(barrier, NP * NE - 1)

            @pl.when(it < NP - 1)
            def _():
                for un in range(2):
                    att_send(it, un).start()

            return c2

        with jax.named_scope("attn"):
            lax.fori_loop(0, NP, chunk, 0)

        with jax.named_scope("kvproj"):
            drain(wkvb, ld_sem.at[1])
            for b in range(2):
                kvs[:, b * KW:(b + 1) * KW] = dot(hb[...], wkvb[b]).astype(BF).astype(F32)

            for half in range(2):
                for h in range(NH):
                    g = h // QG
                    kx[pl.ds(half * UR + h, TU, stride=NH), :] = kvs[own_tok(half), g * HD:(g + 1) * HD]
                    vx[pl.ds(half * UR + h, TU, stride=NH), :] = kvs[own_tok(half), KW + g * HD:KW + (g + 1) * HD]

        @pl.when(more)
        def _():
            wq_load(l + 1)
            wkv_load(l + 1)
            for n in range(NU):
                kv_load(l + 1, n // 2, n % 2)

        @pl.when(first)
        def _():
            small[1].wait()
            small[2].wait()

        with jax.named_scope("tables"):
            slot_col = lax.broadcasted_iota(jnp.int32, (SLOTS, SLOTS), 0)
            pair_row = lax.broadcasted_iota(jnp.int32, (SLOTS, SLOTS), 1)
            upper = (slot_col < pair_row).astype(F32).astype(BF)
            want_rank = lax.rem(slot_col, RE).astype(F32)
            idrow = jnp.concatenate([idb[l, k:k + 1, :] for k in range(K)], axis=1)
            same = (jnp.broadcast_to(idrow, (SLOTS, SLOTS)) == lax.div(slot_col, RE))
            rank = dot(same.astype(F32).astype(BF), upper)
            pick = jnp.where(jnp.logical_and(same, rank == want_rank), 1.0, 0.0).astype(F32)
            rmat = pick.T.astype(BF)
            dmat = pick[:, 0:T]
            for k in range(1, K):
                dmat = dmat + pick[:, k * T:(k + 1) * T]
            dmat = dmat.astype(BF)
            wr = wrb[l]
            hi = wr.astype(BF).astype(F32)
            mid = (wr - hi).astype(BF).astype(F32)
            lo = wr - hi - mid
            wr3 = jnp.concatenate([hi, mid, lo, jnp.zeros_like(lo)], axis=0).astype(BF)

        with jax.named_scope("comb0"):
            combine(0)
        with jax.named_scope("comb1"):
            combine(1)
        with jax.named_scope("agwait"):
            wo_copy(l).wait()
            drain(oag.at[l, pl.ds(0, NM * TU)], og_r)

        with jax.named_scope("oproj"):
            for b in range(NP):
                cols = slice(b * CB, (b + 1) * CB)
                a_s[:, cols] = (xs[:, cols] + dot(oag[l], wob[:, cols])).astype(BF).astype(F32)

            @pl.when(more)
            def _():
                wo_copy(l + 1).start()

            u = rms_norm(a_s[...]).astype(BF)
            for b in range(NP):
                cols = slice(b * CB, (b + 1) * CB)
                uperm[l, :, cols] = dot(dmat, u[:, cols]).astype(BF)
            for r in range(1, NR):
                dis_send(r).start()
            xin[l, 0:RE, :] = uperm[l, pl.ds(pl.multiple_of(e * RE, RE), RE), :]

        with jax.named_scope("gates"):
            lg3 = lax.dot_general(wr3, u, NT, preferred_element_type=F32)
            lg = lg3[0:NEX] + lg3[NEX:2 * NEX] + lg3[2 * NEX:3 * NEX]
            picked = [jnp.sum(jnp.where(ecol == idb[l, k:k + 1, :], lg, 0.0), axis=0, keepdims=True)
                      for k in range(K)]
            gtop = picked[0]
            for k in range(1, K):
                gtop = jnp.maximum(gtop, picked[k])
            ex = [jnp.exp(v - gtop) for v in picked]
            tot = ex[0]
            for k in range(1, K):
                tot = tot + ex[k]
            grow = jnp.concatenate([v / tot for v in ex], axis=1)
            gcol = jnp.broadcast_to(grow, (SLOTS, SLOTS)).T[:, 0:1]
            drain(w1b, ld_sem.at[3])
            drain(w3b, ld_sem.at[4])

        def up(g):
            r0 = max(1, groups[g][0])
            drain(xin.at[l, pl.ds(r0 * RE, (groups[g][1] - r0) * RE)], dis_r.at[g])
            xe = xin[l, grows(g)]
            f0 = 0
            while f0 < FF:
                fw = min(BW, FF - f0)
                h1 = dot(xe, w1b[:, f0:f0 + fw])
                h3 = dot(xe, w3b[:, f0:f0 + fw])
                act[grows(g), f0:f0 + fw] = (h1 * jax.nn.sigmoid(h1) * h3).astype(BF)
                f0 += fw

        def down(g):
            for d in (2, 1, 3, 0):
                ys[l, (d + NP - 1) % NP, grows(g)] = dot(act[grows(g)], w2b[pool_of(d)])
            for d in (2, 1, 3):
                ys_send(g, d).start()

        def finish(g):
            drain(yrecv.at[l, :, grows(g)], ys_r.at[g])
            tot = ys[l, NP - 1, grows(g)]
            for d in range(1, NP):
                tot = tot + yrecv[l, d - 1, grows(g)]
            ybf[l, grows(g)] = tot.astype(BF)
            for dp_ in (2, 1, 3, 0):
                for r in range(groups[g][1] - 1, groups[g][0] - 1, -1):
                    if dp_ or r:
                        ret_send(dp_, r).start()
            if g == 0:
                yret[l, pl.ds(pl.multiple_of(p * SLOTS + e * RE, RE), RE), :] = ybf[l, 0:RE, :]

        for g in range(NG):
            with jax.named_scope(f"up{g}"):
                up(g)
            if g == 0:
                drain(w2b, ld_sem.at[5])
            with jax.named_scope(f"down{g}"):
                down(g)

        @pl.when(more)
        def _():
            up_load(l + 1)
            down_load(l + 1)

        for g in range(NG):
            with jax.named_scope(f"finish{g}"):
                finish(g)

        all_ret = yret.at[l, pl.ds(0, (NP * NE - 1) * RE)]
        with jax.named_scope("retwait"):
            drain(all_ret, ret_r)

        with jax.named_scope("gsum"):
            for b in range(NP):
                cols = slice(b * CB, (b + 1) * CB)
                yp = dot(rmat, yret[l, b * SLOTS:(b + 1) * SLOTS]) * gcol
                mixed = yp[0:T]
                for k in range(1, K):
                    mixed = mixed + yp[k * T:(k + 1) * T]
                xs[:, cols] = (a_s[:, cols] + mixed).astype(BF).astype(F32)

        drain(msg.at[l, pl.ds(0, NM)], att_s)
        drain(oag.at[l, pl.ds(0, NM * TU)], og_s)
        drain(uperm.at[l, pl.ds(0, (NR - 1) * RE)], dis_s)
        for g in range(NG):
            drain(ys.at[l, pl.ds(0, NP - 1), grows(g)], ys_s.at[g])
        drain(all_ret, ret_s)
        return carry

    lax.fori_loop(0, L, layer, 0)
    out_ref[...] = xs[...].astype(BF)


def solution(mesh):
    tok_spec = P(("dp", "ep"), None)
    cache_spec = P(None, ("dp", "ep"), "pool", None, None)
    up_spec = P(None, "ep", None, "pool")
    down_spec = P(None, "ep", "pool", None)
    in_specs = (tok_spec, cache_spec, cache_spec, P(("dp", "ep")), P(), P(), P(), P(), P(),
                P(None, ("dp", "ep"), None), up_spec, up_spec, down_spec)
    NP, NE = mesh.shape["pool"], mesh.shape["ep"]

    def body(hidden, k_cache, v_cache, cache_len, w_q, w_k, w_v, w_o, w_router, ids, w_one, w_three, w_two):
        L = w_q.shape[0]
        T, D = hidden.shape
        S, G, HD = k_cache.shape[2:]
        NH = w_q.shape[2] // HD
        K = ids.shape[2]
        FF = w_one.shape[3]
        TC = T // NP
        SLOTS, CB, ROWS, SG, UR = T * K, D // NP, TC * NH, S * G, TC // 2 * NH
        assert w_one.shape[1] == 1 and SLOTS == HD and ROWS == HD and w_router.shape[2] == 8 and NP == 4 and G == 2
        dims = (L, T, D, S, G, HD, NH, NP, NE, TC, K, FF)
        kc = k_cache.reshape(L, T, SG, HD)
        vc = v_cache.reshape(L, T, SG, HD)
        wr_t = jnp.swapaxes(w_router, 1, 2)
        ids_t = jnp.swapaxes(ids, 1, 2)
        NG = 4
        V = pltpu.VMEM
        dma = pltpu.SemaphoreType.DMA
        anyspec = pl.BlockSpec(memory_space=pl.ANY)
        vspec = pl.BlockSpec(memory_space=pltpu.VMEM)
        scratch = [
            pltpu.SMEM((T,), jnp.int32),
            V((T, D), BF), V((T, D), F32), V((T, D), BF), V(ids_t.shape, jnp.int32), V(wr_t.shape, F32),
            V((D, NH * HD), BF), V((2, D, G * HD), BF), V((2 * NP, 2, TC // 2, SG, HD), BF), V((D, D), BF),
            V((D, FF), BF), V((D, FF), BF), V((NP, FF, CB), BF),
            V((T * NH, HD), F32), V((T, 2 * G * HD), F32), V((ROWS, HD), F32), V((ROWS, HD), F32),
            V((ROWS, HD), F32), V((L, 2 * NP, UR + 8, HD), F32), V((L, 2 * NP - 2, UR + 8, HD), F32),
            V((UR, HD), F32), V((L, T, NH * HD), BF),
            V((T, D), F32), V((L, SLOTS, D), BF), V((L, SLOTS, D), BF), V((SLOTS, FF), BF),
            V((L, NP, SLOTS, CB), F32), V((L, NP - 1, SLOTS, CB), F32),
            V((L, SLOTS, CB), BF), V((L, NP * SLOTS, CB), BF),
            dma((10,)), dma((2 * NP,)), dma, dma((2,)), dma, dma, dma, dma((NG,)), dma((NG,)), dma((NG,)), dma, dma,
        ]
        return pl.pallas_call(
            functools.partial(layers_kernel, dims),
            out_shape=pltpu.VMEM((T, D), BF),
            in_specs=[anyspec, anyspec, anyspec, anyspec, anyspec, anyspec, anyspec,
                      anyspec, anyspec, anyspec, anyspec, anyspec, anyspec],
            out_specs=vspec,
            scratch_shapes=scratch,
            name="moe_layers",
            compiler_params=pltpu.CompilerParams(collective_id=0, has_side_effects=True,
                                                 vmem_limit_bytes=60 * 1024 * 1024),
        )(cache_len, hidden, ids_t, kc, vc, w_q, w_k, w_v, w_o, wr_t, w_one, w_three, w_two)

    return jax.shard_map(body, mesh=mesh, in_specs=in_specs, out_specs=tok_spec, check_vma=False)
```

```python
import functools

import jax
import jax.numpy as jnp
from jax import lax
from jax.experimental import pallas as pl
from jax.experimental.pallas import tpu as pltpu
from jax.sharding import PartitionSpec as P

MESH = pl.DeviceIdType.MESH
NORM_EPS = 1e-6
NEG = -1e30
BF = jnp.bfloat16
F32 = jnp.float32
NT = (((1,), (1,)), ((), ()))


def rms_norm(v):
    return v * lax.rsqrt(jnp.mean(v * v, axis=-1, keepdims=True) + NORM_EPS)


def dot(a, b):
    return jnp.dot(a, b, preferred_element_type=F32)


def layers_kernel(dims, len_hbm, x_hbm, ids_hbm, k_hbm, v_hbm, wq_hbm, wk_hbm, wv_hbm, wo_hbm, wr_hbm,
                  w1_hbm, w3_hbm, w2_hbm, out_ref,
                  len_ref, xb, xs, hb, idb, wrb, wqb, wkvb, kvbuf, wob, w1b, w3b, w2b, qrows, kvs, kx, vx, zst, msg, arx, orow, oag,
                  a_s, uperm, xin, act, ys, yrecv, ybf, yret,
                  ld_sem, kv_sem, att_s, att_r, og_s, og_r, dis_s, dis_r, ys_s, ys_r, ret_s, ret_r):
    L, T, D, S, G, HD, NH, NP, NE, TC, K, FF = dims
    QG = NH // G
    SLOTS = T * K
    RE = SLOTS // NE
    CB = D // NP
    SG = S * G
    QW = NH * HD
    KW = G * HD
    TU = TC // 2
    TH = T // 2
    UR = TU * NH
    NU = 2 * NP
    NM = 2 * (NP - 1)
    NX = NE // 2
    BW = 2 * HD
    scale = HD ** -0.5
    p = lax.axis_index("pool")
    e = lax.axis_index("ep")
    chip = lax.div(e, 2)
    core = lax.rem(e, 2)

    def pool_of(d):
        return lax.rem(p + d, NP)

    rel = [(0, 0), (0, 1)] + [(dx, dc) for dx in range(2, NX - 1) for dc in range(2)]
    rel += [(1, 0), (NX - 1, 0), (1, 1), (NX - 1, 1)]
    NR = len(rel)
    groups = [(0, 2), (2, 4), (4, 6), (6, NR)]
    NG = len(groups)
    group_of = [next(g for g in range(NG) if groups[g][0] <= r < groups[g][1]) for r in range(NR)]

    def ep_sender(r):
        return lax.rem(chip + rel[r][0], NX) * 2 + lax.rem(core + rel[r][1], 2)

    def ep_receiver(r):
        return lax.rem(chip + NX - rel[r][0], NX) * 2 + lax.rem(core + rel[r][1], 2)

    def wq_load(l):
        for b in range(2):
            rows = pl.ds(b * (D // 2), D // 2)
            pltpu.make_async_copy(wq_hbm.at[l, rows], wqb.at[rows], ld_sem.at[0]).start()

    def wkv_load(l):
        pltpu.make_async_copy(wk_hbm.at[l], wkvb.at[0], ld_sem.at[1]).start()
        pltpu.make_async_copy(wv_hbm.at[l], wkvb.at[1], ld_sem.at[1]).start()

    def drain(ref, sem):
        pltpu.make_async_copy(ref, ref, sem).wait()

    def unit(it, un):
        z = (it + 1) // 2 % 2
        half = z * (it - 1) + (1 - z) * un
        away = z * (1 + 2 * un) + (1 - z) * (2 - 2 * (it // 3))
        return half, away

    def unit_tok(it, un):
        half, away = unit(it, un)
        return half * TH + lax.rem(p + away, NP) * TU

    def kv_load(l, it, un):
        n = 2 * it + un
        tok = pl.ds(pl.multiple_of(unit_tok(it, un), TU), TU)
        pltpu.make_async_copy(k_hbm.at[l, tok], kvbuf.at[n, 0], kv_sem.at[n]).start()
        pltpu.make_async_copy(v_hbm.at[l, tok], kvbuf.at[n, 1], kv_sem.at[n]).start()

    def wo_copy(l):
        return pltpu.make_async_copy(wo_hbm.at[l], wob, ld_sem.at[2])

    def up_load(l):
        pltpu.make_async_copy(w1_hbm.at[l, 0], w1b, ld_sem.at[3]).start()
        pltpu.make_async_copy(w3_hbm.at[l, 0], w3b, ld_sem.at[4]).start()

    def down_load(l):
        for q in range(NP):
            pltpu.make_async_copy(w2_hbm.at[l, 0, :, pl.ds(q * CB, CB)], w2b.at[q], ld_sem.at[5]).start()

    small = [pltpu.make_async_copy(x_hbm, xb, ld_sem.at[6]),
             pltpu.make_async_copy(ids_hbm, idb, ld_sem.at[7]),
             pltpu.make_async_copy(wr_hbm, wrb, ld_sem.at[8]),
             pltpu.make_async_copy(len_hbm, len_ref, ld_sem.at[9])]
    small[0].start()
    small[3].start()
    wq_load(0)
    for un in range(2):
        kv_load(0, 0, un)
    small[1].start()
    small[2].start()

    barrier = pltpu.get_barrier_semaphore()
    for dp_ in range(NP):
        for de in range(NE):
            if dp_ or de:
                pl.semaphore_signal(barrier, inc=1,
                                    device_id={"pool": pool_of(dp_), "ep": lax.rem(e + de, NE)},
                                    device_id_type=MESH)

    hrow = lax.broadcasted_iota(jnp.int32, (NH, SG), 0)
    pcol = lax.broadcasted_iota(jnp.int32, (NH, SG), 1)
    posm = jnp.where(lax.rem(pcol, G) == lax.div(hrow, QG), lax.div(pcol, G), jnp.int32(1 << 30))
    lane = lax.broadcasted_iota(jnp.int32, (NH, HD), 1)
    hsub = lax.broadcasted_iota(jnp.int32, (NH, HD), 0)
    NEX = wrb.shape[1]
    hlane = lax.rem(lane, UR)
    row_lane = lax.rem(lax.broadcasted_iota(jnp.int32, (UR, HD), 1), UR)
    row_id = lax.broadcasted_iota(jnp.int32, (UR, HD), 0)
    ecol = lax.broadcasted_iota(jnp.int32, (NEX, T), 0)

    zst[...] = jnp.zeros_like(zst)
    small[0].wait()
    xs[...] = xb[...].astype(F32)

    def layer(l, carry):
        more = l + 1 < L
        first = l == 0

        def att_send(it, un):
            half, away = unit(it, un)
            return pltpu.make_async_remote_copy(
                src_ref=msg.at[l, 2 * it + un], dst_ref=arx.at[l, half * (NP - 1) + away - 1], send_sem=att_s,
                recv_sem=att_r.at[half],
                device_id={"pool": pool_of(away), "ep": e}, device_id_type=MESH)

        def own_tok(half):
            return pl.ds(pl.multiple_of(half * TH + p * TU, TU), TU)

        def og_send(half, d):
            return pltpu.make_async_remote_copy(
                src_ref=oag.at[l, own_tok(half)], dst_ref=oag.at[l, own_tok(half)], send_sem=og_s, recv_sem=og_r,
                device_id={"pool": pool_of(d), "ep": e}, device_id_type=MESH)

        def dis_send(r):
            dst = ep_receiver(r)
            return pltpu.make_async_remote_copy(
                src_ref=uperm.at[l, pl.ds(pl.multiple_of(dst * RE, RE), RE)], dst_ref=xin.at[l, pl.ds(r * RE, RE)],
                send_sem=dis_s, recv_sem=dis_r.at[group_of[r]],
                device_id={"pool": p, "ep": dst}, device_id_type=MESH)

        def grows(g):
            return pl.ds(groups[g][0] * RE, (groups[g][1] - groups[g][0]) * RE)

        def ys_send(g, d):
            return pltpu.make_async_remote_copy(
                src_ref=ys.at[l, d - 1, grows(g)], dst_ref=yrecv.at[l, d - 1, grows(g)], send_sem=ys_s.at[g],
                recv_sem=ys_r.at[g], device_id={"pool": pool_of(d), "ep": e}, device_id_type=MESH)

        def ret_send(dp_, r):
            dst = ep_sender(r)
            return pltpu.make_async_remote_copy(
                src_ref=ybf.at[l, pl.ds(r * RE, RE)],
                dst_ref=yret.at[l, pl.ds(pl.multiple_of(p * SLOTS + e * RE, RE), RE)], send_sem=ret_s, recv_sem=ret_r,
                device_id={"pool": pool_of(dp_), "ep": dst}, device_id_type=MESH)

        with jax.named_scope("qkv"):
            hn = rms_norm(xs[...]).astype(BF)
            drain(wqb, ld_sem.at[0])

            @pl.when(first)
            def _():
                small[3].wait()

            for b in range(QW // BW):
                r = dot(hn, wqb[:, b * BW:(b + 1) * BW]).astype(BF).astype(F32)
                for j in range(2):
                    qrows[pl.ds(2 * b + j, T, stride=NH), :] = r[:, j * HD:(j + 1) * HD]
            hb[...] = hn

            @pl.when(first)
            def _():
                for un in range(2):
                    kv_load(l, 1, un)
                for un in range(2):
                    kv_load(l, 2, un)

        def new_scores(half):
            q0 = pl.multiple_of((half * TH + p * TU) * NH, UR)
            krow = pl.ds(half * UR, UR)
            s_new = jnp.sum(qrows[pl.ds(q0, UR), :] * kx[krow, :], axis=1, keepdims=True) * scale
            return jnp.sum(jnp.where(row_lane == row_id, s_new, 0.0), axis=0, keepdims=True)

        def combine(half, s_new):
            m0 = half * (NP - 1)
            drain(arx.at[l, pl.ds(m0, NP - 1)], att_r.at[half])
            parts = [arx.at[l, m0 + i] for i in range(NP - 1)] + [msg.at[l, 2 * (NP - 1) + half]]
            ms = [ref[UR:UR + 1, :] for ref in parts]
            top = s_new
            for m in ms:
                top = jnp.maximum(top, m)
            w = [jnp.exp(m - top) for m in ms] + [jnp.exp(s_new - top)]
            den = w[NP]
            for i in range(NP):
                den = den + w[i] * parts[i][UR + 1:UR + 2, :]
            inv = 1.0 / den
            for i in range(NP + 1):
                zst[i:i + 1, :] = w[i] * inv
            zc = zst[...].T
            out = zc[0:UR, NP:NP + 1] * vx[pl.ds(half * UR, UR), :]
            for i in range(NP):
                out = out + zc[0:UR, i:i + 1] * parts[i][0:UR, :]
            orow[...] = out
            for h in range(NH):
                oag[l, own_tok(half), h * HD:(h + 1) * HD] = orow[pl.ds(h, TU, stride=NH), :].astype(BF)
            for d in (2, 1, 3):
                og_send(half, d).start()

        def attend(it, send):
            for un in range(2):
                n = 2 * it + un
                drain(kvbuf.at[n], kv_sem.at[n])

            @pl.when(jnp.logical_and(first, it == 0))
            def _():
                for un in range(2):
                    kv_load(l, 3, un)

            @pl.when(jnp.logical_and(first, it == 2))
            def _():
                wkv_load(l)
                wo_copy(l).start()
                up_load(l)
                down_load(l)

            for un in range(2):
                n = 2 * it + un
                t0 = unit_tok(it, un)
                sc = []
                for j in range(TU):
                    t = t0 + j
                    qt = qrows[pl.ds(pl.multiple_of(t * NH, NH), NH), :].astype(BF)
                    s = lax.dot_general(qt, kvbuf[n, 0, j], NT, preferred_element_type=F32) * scale
                    sc.append(jnp.where(posm < len_ref[t] - p * S, s, NEG))
                mx = [jnp.max(s, axis=1, keepdims=True) for s in sc]
                pr = [jnp.exp(s - m) for s, m in zip(sc, mx)]
                ls = [jnp.sum(q, axis=1, keepdims=True) for q in pr]
                mrow = jnp.zeros((NH, HD), F32)
                lrow = jnp.zeros((NH, HD), F32)
                for j in range(TU):
                    msg[l, n, j * NH:(j + 1) * NH, :] = dot(pr[j].astype(BF), kvbuf[n, 1, j])
                    here = hlane == hsub + j * NH
                    mrow = jnp.where(here, mx[j], mrow)
                    lrow = jnp.where(here, ls[j], lrow)
                msg[l, n, UR:UR + 1, :] = jnp.sum(mrow, axis=0, keepdims=True)
                msg[l, n, UR + 1:UR + 2, :] = jnp.sum(lrow, axis=0, keepdims=True)
                if send and un == 0:
                    @pl.when(jnp.logical_and(first, it == 0))
                    def _():
                        pl.semaphore_wait(barrier, NP * NE - 1)

                if send:
                    att_send(it, un).start()

        def chunk(it, c2):
            attend(it, True)
            return c2

        with jax.named_scope("attn"):
            lax.fori_loop(0, NP - 1, chunk, 0)
            attend(NP - 1, False)

        with jax.named_scope("kvproj"):
            drain(wkvb, ld_sem.at[1])
            for b in range(2):
                kvs[:, b * KW:(b + 1) * KW] = dot(hb[...], wkvb[b]).astype(BF).astype(F32)

            for half in range(2):
                for h in range(NH):
                    g = h // QG
                    kx[pl.ds(half * UR + h, TU, stride=NH), :] = kvs[own_tok(half), g * HD:(g + 1) * HD]
                    vx[pl.ds(half * UR + h, TU, stride=NH), :] = kvs[own_tok(half), KW + g * HD:KW + (g + 1) * HD]

        @pl.when(more)
        def _():
            wq_load(l + 1)
            wkv_load(l + 1)
            for n in range(NU):
                kv_load(l + 1, n // 2, n % 2)

        new_row = [new_scores(half) for half in range(2)]

        @pl.when(first)
        def _():
            small[1].wait()
            small[2].wait()

        with jax.named_scope("tables"):
            slot_col = lax.broadcasted_iota(jnp.int32, (SLOTS, SLOTS), 0)
            pair_row = lax.broadcasted_iota(jnp.int32, (SLOTS, SLOTS), 1)
            upper = (slot_col < pair_row).astype(F32).astype(BF)
            want_rank = lax.rem(slot_col, RE).astype(F32)
            idrow = jnp.concatenate([idb[l, k:k + 1, :] for k in range(K)], axis=1)
            same = (jnp.broadcast_to(idrow, (SLOTS, SLOTS)) == lax.div(slot_col, RE))
            rank = dot(same.astype(F32).astype(BF), upper)
            pick = jnp.where(jnp.logical_and(same, rank == want_rank), 1.0, 0.0).astype(F32)
            rmat = pick.T.astype(BF)
            dmat = pick[:, 0:T]
            for k in range(1, K):
                dmat = dmat + pick[:, k * T:(k + 1) * T]
            dmat = dmat.astype(BF)
            wr = wrb[l]
            hi = wr.astype(BF).astype(F32)
            mid = (wr - hi).astype(BF).astype(F32)
            lo = wr - hi - mid
            wr3 = jnp.concatenate([hi, mid, lo, jnp.zeros_like(lo)], axis=0).astype(BF)

        with jax.named_scope("comb0"):
            combine(0, new_row[0])
        with jax.named_scope("comb1"):
            combine(1, new_row[1])
        with jax.named_scope("agwait"):
            wo_copy(l).wait()
            drain(oag.at[l, pl.ds(0, NM * TU)], og_r)

        with jax.named_scope("oproj"):
            for b in range(NP):
                cols = slice(b * CB, (b + 1) * CB)
                a_s[:, cols] = (xs[:, cols] + dot(oag[l], wob[:, cols])).astype(BF).astype(F32)

            @pl.when(more)
            def _():
                wo_copy(l + 1).start()

            u = rms_norm(a_s[...]).astype(BF)
            for b in range(NP):
                cols = slice(b * CB, (b + 1) * CB)
                uperm[l, :, cols] = dot(dmat, u[:, cols]).astype(BF)
            for r in range(1, NR):
                dis_send(r).start()
            xin[l, 0:RE, :] = uperm[l, pl.ds(pl.multiple_of(e * RE, RE), RE), :]

        with jax.named_scope("gates"):
            lg3 = lax.dot_general(wr3, u, NT, preferred_element_type=F32)
            lg = lg3[0:NEX] + lg3[NEX:2 * NEX] + lg3[2 * NEX:3 * NEX]
            picked = [jnp.sum(jnp.where(ecol == idb[l, k:k + 1, :], lg, 0.0), axis=0, keepdims=True)
                      for k in range(K)]
            gtop = picked[0]
            for k in range(1, K):
                gtop = jnp.maximum(gtop, picked[k])
            ex = [jnp.exp(v - gtop) for v in picked]
            tot = ex[0]
            for k in range(1, K):
                tot = tot + ex[k]
            grow = jnp.concatenate([v / tot for v in ex], axis=1)
            gcol = jnp.broadcast_to(grow, (SLOTS, SLOTS)).T[:, 0:1]
            drain(w1b, ld_sem.at[3])
            drain(w3b, ld_sem.at[4])

        def up(g):
            r0 = max(1, groups[g][0])
            drain(xin.at[l, pl.ds(r0 * RE, (groups[g][1] - r0) * RE)], dis_r.at[g])
            xe = xin[l, grows(g)]
            f0 = 0
            while f0 < FF:
                fw = min(BW, FF - f0)
                h1 = dot(xe, w1b[:, f0:f0 + fw])
                h3 = dot(xe, w3b[:, f0:f0 + fw])
                act[grows(g), f0:f0 + fw] = (h1 * jax.nn.sigmoid(h1) * h3).astype(BF)
                f0 += fw

        def down(g):
            for d in (2, 1, 3, 0):
                ys[l, (d + NP - 1) % NP, grows(g)] = dot(act[grows(g)], w2b[pool_of(d)])
            for d in (2, 1, 3):
                ys_send(g, d).start()

        def finish(g):
            drain(yrecv.at[l, :, grows(g)], ys_r.at[g])
            tot = ys[l, NP - 1, grows(g)]
            for d in range(1, NP):
                tot = tot + yrecv[l, d - 1, grows(g)]
            ybf[l, grows(g)] = tot.astype(BF)
            for dp_ in (2, 1, 3, 0):
                for r in range(groups[g][1] - 1, groups[g][0] - 1, -1):
                    if dp_ or r:
                        ret_send(dp_, r).start()
            if g == 0:
                yret[l, pl.ds(pl.multiple_of(p * SLOTS + e * RE, RE), RE), :] = ybf[l, 0:RE, :]

        for g in range(NG):
            with jax.named_scope(f"up{g}"):
                up(g)
            if g == 0:
                drain(w2b, ld_sem.at[5])
            with jax.named_scope(f"down{g}"):
                down(g)

        @pl.when(more)
        def _():
            up_load(l + 1)
            down_load(l + 1)

        for g in range(NG):
            with jax.named_scope(f"finish{g}"):
                finish(g)

        all_ret = yret.at[l, pl.ds(0, (NP * NE - 1) * RE)]
        with jax.named_scope("retwait"):
            drain(all_ret, ret_r)

        with jax.named_scope("gsum"):
            for b in range(NP):
                cols = slice(b * CB, (b + 1) * CB)
                yp = dot(rmat, yret[l, b * SLOTS:(b + 1) * SLOTS]) * gcol
                mixed = yp[0:T]
                for k in range(1, K):
                    mixed = mixed + yp[k * T:(k + 1) * T]
                xs[:, cols] = (a_s[:, cols] + mixed).astype(BF).astype(F32)

        drain(msg.at[l, pl.ds(0, NM)], att_s)
        drain(oag.at[l, pl.ds(0, NM * TU)], og_s)
        drain(uperm.at[l, pl.ds(0, (NR - 1) * RE)], dis_s)
        for g in range(NG):
            drain(ys.at[l, pl.ds(0, NP - 1), grows(g)], ys_s.at[g])
        drain(all_ret, ret_s)
        return carry

    lax.fori_loop(0, L, layer, 0)
    out_ref[...] = xs[...].astype(BF)


def solution(mesh):
    tok_spec = P(("dp", "ep"), None)
    cache_spec = P(None, ("dp", "ep"), "pool", None, None)
    up_spec = P(None, "ep", None, "pool")
    down_spec = P(None, "ep", "pool", None)
    in_specs = (tok_spec, cache_spec, cache_spec, P(("dp", "ep")), P(), P(), P(), P(), P(),
                P(None, ("dp", "ep"), None), up_spec, up_spec, down_spec)
    NP, NE = mesh.shape["pool"], mesh.shape["ep"]

    def body(hidden, k_cache, v_cache, cache_len, w_q, w_k, w_v, w_o, w_router, ids, w_one, w_three, w_two):
        L = w_q.shape[0]
        T, D = hidden.shape
        S, G, HD = k_cache.shape[2:]
        NH = w_q.shape[2] // HD
        K = ids.shape[2]
        FF = w_one.shape[3]
        TC = T // NP
        SLOTS, CB, ROWS, SG, UR = T * K, D // NP, TC * NH, S * G, TC // 2 * NH
        assert w_one.shape[1] == 1 and SLOTS == HD and ROWS == HD and w_router.shape[2] == 8 and NP == 4 and G == 2
        dims = (L, T, D, S, G, HD, NH, NP, NE, TC, K, FF)
        kc = k_cache.reshape(L, T, SG, HD)
        vc = v_cache.reshape(L, T, SG, HD)
        wr_t = jnp.swapaxes(w_router, 1, 2)
        ids_t = jnp.swapaxes(ids, 1, 2)
        NG = 4
        V = pltpu.VMEM
        dma = pltpu.SemaphoreType.DMA
        anyspec = pl.BlockSpec(memory_space=pl.ANY)
        vspec = pl.BlockSpec(memory_space=pltpu.VMEM)
        scratch = [
            pltpu.SMEM((T,), jnp.int32),
            V((T, D), BF), V((T, D), F32), V((T, D), BF), V(ids_t.shape, jnp.int32), V(wr_t.shape, F32),
            V((D, NH * HD), BF), V((2, D, G * HD), BF), V((2 * NP, 2, TC // 2, SG, HD), BF), V((D, D), BF),
            V((D, FF), BF), V((D, FF), BF), V((NP, FF, CB), BF),
            V((T * NH, HD), F32), V((T, 2 * G * HD), F32), V((ROWS, HD), F32), V((ROWS, HD), F32),
            V((ROWS, HD), F32), V((L, 2 * NP, UR + 2, HD), F32), V((L, 2 * NP - 2, UR + 2, HD), F32),
            V((UR, HD), F32), V((L, T, NH * HD), BF),
            V((T, D), F32), V((L, SLOTS, D), BF), V((L, SLOTS, D), BF), V((SLOTS, FF), BF),
            V((L, NP, SLOTS, CB), F32), V((L, NP - 1, SLOTS, CB), F32),
            V((L, SLOTS, CB), BF), V((L, NP * SLOTS, CB), BF),
            dma((10,)), dma((2 * NP,)), dma, dma((2,)), dma, dma, dma, dma((NG,)), dma((NG,)), dma((NG,)), dma, dma,
        ]
        return pl.pallas_call(
            functools.partial(layers_kernel, dims),
            out_shape=pltpu.VMEM((T, D), BF),
            in_specs=[anyspec, anyspec, anyspec, anyspec, anyspec, anyspec, anyspec,
                      anyspec, anyspec, anyspec, anyspec, anyspec, anyspec],
            out_specs=vspec,
            scratch_shapes=scratch,
            name="moe_layers",
            compiler_params=pltpu.CompilerParams(collective_id=0, has_side_effects=True,
                                                 vmem_limit_bytes=60 * 1024 * 1024),
        )(cache_len, hidden, ids_t, kc, vc, w_q, w_k, w_v, w_o, wr_t, w_one, w_three, w_two)

    return jax.shard_map(body, mesh=mesh, in_specs=in_specs, out_specs=tok_spec, check_vma=False)
```

```python
import functools

import jax
import jax.numpy as jnp
from jax import lax
from jax.experimental import pallas as pl
from jax.experimental.pallas import tpu as pltpu
from jax.sharding import PartitionSpec as P

MESH = pl.DeviceIdType.MESH
NORM_EPS = 1e-6
NEG = -1e30
BF = jnp.bfloat16
F32 = jnp.float32
NT = (((1,), (1,)), ((), ()))


def rms_norm(v):
    return v * lax.rsqrt(jnp.mean(v * v, axis=-1, keepdims=True) + NORM_EPS)


def dot(a, b):
    return jnp.dot(a, b, preferred_element_type=F32)


def layers_kernel(dims, len_hbm, x_hbm, ids_hbm, k_hbm, v_hbm, wq_hbm, wk_hbm, wv_hbm, wo_hbm, wr_hbm,
                  w1_hbm, w3_hbm, w2_hbm, out_ref,
                  len_ref, xb, xs, hb, idb, wrb, wqb, wkvb, kvbuf, wob, w1b, w3b, w2b, qrows, kvs, kx, vx, zst, msg, arx, orow, oag,
                  a_s, uperm, xin, act, ys, yrecv, ybf, yret,
                  ld_sem, kv_sem, att_s, att_r, og_s, og_r, dis_s, dis_r, ys_s, ys_r, ret_s, ret_r):
    L, T, D, S, G, HD, NH, NP, NE, TC, K, FF = dims
    QG = NH // G
    SLOTS = T * K
    RE = SLOTS // NE
    CB = D // NP
    SG = S * G
    QW = NH * HD
    KW = G * HD
    TU = TC // 2
    TH = T // 2
    UR = TU * NH
    NU = 2 * NP
    NM = 2 * (NP - 1)
    NX = NE // 2
    BW = 2 * HD
    scale = HD ** -0.5
    p = lax.axis_index("pool")
    e = lax.axis_index("ep")
    chip = lax.div(e, 2)
    core = lax.rem(e, 2)

    def pool_of(d):
        return lax.rem(p + d, NP)

    rel = [(0, 0), (0, 1), (1, 0), (NX - 1, 0)] + [(dx, dc) for dx in range(2, NX - 1) for dc in range(2)] + [(1, 1), (NX - 1, 1)]
    NR = len(rel)
    ups = [(0, 2), (2, 4), (4, NR)]
    groups = [(0, 2), (2, 4), (4, 6), (6, NR)]
    NG = len(groups)
    group_of = [next(g for g in range(len(ups)) if ups[g][0] <= r < ups[g][1]) for r in range(NR)]

    def ep_sender(r):
        return lax.rem(chip + rel[r][0], NX) * 2 + lax.rem(core + rel[r][1], 2)

    def ep_receiver(r):
        return lax.rem(chip + NX - rel[r][0], NX) * 2 + lax.rem(core + rel[r][1], 2)

    def wq_load(l):
        for b in range(2):
            rows = pl.ds(b * (D // 2), D // 2)
            pltpu.make_async_copy(wq_hbm.at[l, rows], wqb.at[rows], ld_sem.at[0]).start()

    def wkv_load(l):
        pltpu.make_async_copy(wk_hbm.at[l], wkvb.at[0], ld_sem.at[1]).start()
        pltpu.make_async_copy(wv_hbm.at[l], wkvb.at[1], ld_sem.at[1]).start()

    def drain(ref, sem):
        pltpu.make_async_copy(ref, ref, sem).wait()

    def unit(it, un):
        z = (it + 1) // 2 % 2
        half = z * (it - 1) + (1 - z) * un
        away = z * (1 + 2 * un) + (1 - z) * (2 - 2 * (it // 3))
        return half, away

    def unit_tok(it, un):
        half, away = unit(it, un)
        return half * TH + lax.rem(p + away, NP) * TU

    def kv_load(l, it, un):
        n = 2 * it + un
        tok = pl.ds(pl.multiple_of(unit_tok(it, un), TU), TU)
        pltpu.make_async_copy(k_hbm.at[l, tok], kvbuf.at[n, 0], kv_sem.at[n]).start()
        pltpu.make_async_copy(v_hbm.at[l, tok], kvbuf.at[n, 1], kv_sem.at[n]).start()

    def wo_copy(l):
        return pltpu.make_async_copy(wo_hbm.at[l], wob, ld_sem.at[2])

    def up_load(l):
        pltpu.make_async_copy(w1_hbm.at[l, 0], w1b, ld_sem.at[3]).start()
        pltpu.make_async_copy(w3_hbm.at[l, 0], w3b, ld_sem.at[4]).start()

    def down_load(l):
        for q in range(NP):
            pltpu.make_async_copy(w2_hbm.at[l, 0, :, pl.ds(q * CB, CB)], w2b.at[q], ld_sem.at[5]).start()

    small = [pltpu.make_async_copy(x_hbm, xb, ld_sem.at[6]),
             pltpu.make_async_copy(ids_hbm, idb, ld_sem.at[7]),
             pltpu.make_async_copy(wr_hbm, wrb, ld_sem.at[8]),
             pltpu.make_async_copy(len_hbm, len_ref, ld_sem.at[9])]
    small[0].start()
    small[3].start()
    wq_load(0)
    for un in range(2):
        kv_load(0, 0, un)
    small[1].start()
    small[2].start()

    barrier = pltpu.get_barrier_semaphore()
    for dp_ in range(NP):
        for de in range(NE):
            if dp_ or de:
                pl.semaphore_signal(barrier, inc=1,
                                    device_id={"pool": pool_of(dp_), "ep": lax.rem(e + de, NE)},
                                    device_id_type=MESH)

    hrow = lax.broadcasted_iota(jnp.int32, (NH, SG), 0)
    pcol = lax.broadcasted_iota(jnp.int32, (NH, SG), 1)
    posm = jnp.where(lax.rem(pcol, G) == lax.div(hrow, QG), lax.div(pcol, G), jnp.int32(1 << 30))
    lane = lax.broadcasted_iota(jnp.int32, (NH, HD), 1)
    hsub = lax.broadcasted_iota(jnp.int32, (NH, HD), 0)
    NEX = wrb.shape[1]
    hlane = lax.rem(lane, UR)
    row_lane = lax.rem(lax.broadcasted_iota(jnp.int32, (UR, HD), 1), UR)
    row_id = lax.broadcasted_iota(jnp.int32, (UR, HD), 0)
    ecol = lax.broadcasted_iota(jnp.int32, (NEX, T), 0)

    zst[...] = jnp.zeros_like(zst)
    small[0].wait()
    xs[...] = xb[...].astype(F32)

    def layer(l, carry):
        more = l + 1 < L
        first = l == 0

        def att_send(it, un):
            half, away = unit(it, un)
            return pltpu.make_async_remote_copy(
                src_ref=msg.at[l, 2 * it + un], dst_ref=arx.at[l, half * (NP - 1) + away - 1], send_sem=att_s,
                recv_sem=att_r.at[half],
                device_id={"pool": pool_of(away), "ep": e}, device_id_type=MESH)

        def own_tok(half):
            return pl.ds(pl.multiple_of(half * TH + p * TU, TU), TU)

        def og_send(half, d):
            return pltpu.make_async_remote_copy(
                src_ref=oag.at[l, own_tok(half)], dst_ref=oag.at[l, own_tok(half)], send_sem=og_s, recv_sem=og_r,
                device_id={"pool": pool_of(d), "ep": e}, device_id_type=MESH)

        def dis_send(r):
            dst = ep_receiver(r)
            return pltpu.make_async_remote_copy(
                src_ref=uperm.at[l, pl.ds(pl.multiple_of(dst * RE, RE), RE)], dst_ref=xin.at[l, pl.ds(r * RE, RE)],
                send_sem=dis_s, recv_sem=dis_r.at[group_of[r]],
                device_id={"pool": p, "ep": dst}, device_id_type=MESH)

        def grows(g):
            return pl.ds(groups[g][0] * RE, (groups[g][1] - groups[g][0]) * RE)

        def ys_send(g, d):
            return pltpu.make_async_remote_copy(
                src_ref=ys.at[l, d - 1, grows(g)], dst_ref=yrecv.at[l, d - 1, grows(g)], send_sem=ys_s.at[g],
                recv_sem=ys_r.at[g], device_id={"pool": pool_of(d), "ep": e}, device_id_type=MESH)

        def ret_send(dp_, r):
            dst = ep_sender(r)
            return pltpu.make_async_remote_copy(
                src_ref=ybf.at[l, pl.ds(r * RE, RE)],
                dst_ref=yret.at[l, pl.ds(pl.multiple_of(p * SLOTS + e * RE, RE), RE)], send_sem=ret_s, recv_sem=ret_r,
                device_id={"pool": pool_of(dp_), "ep": dst}, device_id_type=MESH)

        with jax.named_scope("qkv"):
            hn = rms_norm(xs[...]).astype(BF)
            drain(wqb, ld_sem.at[0])

            @pl.when(first)
            def _():
                small[3].wait()

            for b in range(QW // BW):
                r = dot(hn, wqb[:, b * BW:(b + 1) * BW]).astype(BF).astype(F32)
                for j in range(2):
                    qrows[pl.ds(2 * b + j, T, stride=NH), :] = r[:, j * HD:(j + 1) * HD]
            hb[...] = hn

            @pl.when(first)
            def _():
                for un in range(2):
                    kv_load(l, 1, un)
                for un in range(2):
                    kv_load(l, 2, un)

        def new_scores(half):
            q0 = pl.multiple_of((half * TH + p * TU) * NH, UR)
            krow = pl.ds(half * UR, UR)
            s_new = jnp.sum(qrows[pl.ds(q0, UR), :] * kx[krow, :], axis=1, keepdims=True) * scale
            return jnp.sum(jnp.where(row_lane == row_id, s_new, 0.0), axis=0, keepdims=True)

        def combine(half, s_new):
            m0 = half * (NP - 1)
            drain(arx.at[l, pl.ds(m0, NP - 1)], att_r.at[half])
            parts = [arx.at[l, m0 + i] for i in range(NP - 1)] + [msg.at[l, 2 * (NP - 1) + half]]
            ms = [ref[UR:UR + 1, :] for ref in parts]
            top = s_new
            for m in ms:
                top = jnp.maximum(top, m)
            w = [jnp.exp(m - top) for m in ms] + [jnp.exp(s_new - top)]
            den = w[NP]
            for i in range(NP):
                den = den + w[i] * parts[i][UR + 1:UR + 2, :]
            inv = 1.0 / den
            for i in range(NP + 1):
                zst[i:i + 1, :] = w[i] * inv
            zc = zst[...].T
            out = zc[0:UR, NP:NP + 1] * vx[pl.ds(half * UR, UR), :]
            for i in range(NP):
                out = out + zc[0:UR, i:i + 1] * parts[i][0:UR, :]
            orow[...] = out
            for h in range(NH):
                oag[l, own_tok(half), h * HD:(h + 1) * HD] = orow[pl.ds(h, TU, stride=NH), :].astype(BF)
            for d in (2, 1, 3):
                og_send(half, d).start()

        def attend(it, send):
            for un in range(2):
                n = 2 * it + un
                drain(kvbuf.at[n], kv_sem.at[n])

            @pl.when(jnp.logical_and(first, it == 0))
            def _():
                for un in range(2):
                    kv_load(l, 3, un)

            @pl.when(jnp.logical_and(first, it == 2))
            def _():
                wkv_load(l)
                wo_copy(l).start()
                up_load(l)
                down_load(l)

            for un in range(2):
                n = 2 * it + un
                t0 = unit_tok(it, un)
                sc = []
                for j in range(TU):
                    t = t0 + j
                    qt = qrows[pl.ds(pl.multiple_of(t * NH, NH), NH), :].astype(BF)
                    s = lax.dot_general(qt, kvbuf[n, 0, j], NT, preferred_element_type=F32) * scale
                    sc.append(jnp.where(posm < len_ref[t] - p * S, s, NEG))
                mx = [jnp.max(s, axis=1, keepdims=True) for s in sc]
                pr = [jnp.exp(s - m) for s, m in zip(sc, mx)]
                ls = [jnp.sum(q, axis=1, keepdims=True) for q in pr]
                mrow = jnp.zeros((NH, HD), F32)
                lrow = jnp.zeros((NH, HD), F32)
                for j in range(TU):
                    msg[l, n, j * NH:(j + 1) * NH, :] = dot(pr[j].astype(BF), kvbuf[n, 1, j])
                    here = hlane == hsub + j * NH
                    mrow = jnp.where(here, mx[j], mrow)
                    lrow = jnp.where(here, ls[j], lrow)
                msg[l, n, UR:UR + 1, :] = jnp.sum(mrow, axis=0, keepdims=True)
                msg[l, n, UR + 1:UR + 2, :] = jnp.sum(lrow, axis=0, keepdims=True)
                if send and un == 0:
                    @pl.when(jnp.logical_and(first, it == 0))
                    def _():
                        pl.semaphore_wait(barrier, NP * NE - 1)

                if send:
                    att_send(it, un).start()

        def chunk(it, c2):
            attend(it, True)
            return c2

        with jax.named_scope("attn"):
            lax.fori_loop(0, NP - 1, chunk, 0)
            attend(NP - 1, False)

        with jax.named_scope("kvproj"):
            drain(wkvb, ld_sem.at[1])
            for b in range(2):
                kvs[:, b * KW:(b + 1) * KW] = dot(hb[...], wkvb[b]).astype(BF).astype(F32)

            for half in range(2):
                for h in range(NH):
                    g = h // QG
                    kx[pl.ds(half * UR + h, TU, stride=NH), :] = kvs[own_tok(half), g * HD:(g + 1) * HD]
                    vx[pl.ds(half * UR + h, TU, stride=NH), :] = kvs[own_tok(half), KW + g * HD:KW + (g + 1) * HD]

        @pl.when(more)
        def _():
            wq_load(l + 1)
            wkv_load(l + 1)
            for n in range(NU):
                kv_load(l + 1, n // 2, n % 2)

        new_row = [new_scores(half) for half in range(2)]

        @pl.when(first)
        def _():
            small[1].wait()
            small[2].wait()

        with jax.named_scope("tables"):
            slot_col = lax.broadcasted_iota(jnp.int32, (SLOTS, SLOTS), 0)
            pair_row = lax.broadcasted_iota(jnp.int32, (SLOTS, SLOTS), 1)
            upper = (slot_col < pair_row).astype(F32).astype(BF)
            want_rank = lax.rem(slot_col, RE).astype(F32)
            idrow = jnp.concatenate([idb[l, k:k + 1, :] for k in range(K)], axis=1)
            same = (jnp.broadcast_to(idrow, (SLOTS, SLOTS)) == lax.div(slot_col, RE))
            rank = dot(same.astype(F32).astype(BF), upper)
            pick = jnp.where(jnp.logical_and(same, rank == want_rank), 1.0, 0.0).astype(F32)
            rmat = pick.T.astype(BF)
            dmat = pick[:, 0:T]
            for k in range(1, K):
                dmat = dmat + pick[:, k * T:(k + 1) * T]
            dmat = dmat.astype(BF)
            wr = wrb[l]
            hi = wr.astype(BF).astype(F32)
            mid = (wr - hi).astype(BF).astype(F32)
            lo = wr - hi - mid
            wr3 = jnp.concatenate([hi, mid, lo, jnp.zeros_like(lo)], axis=0).astype(BF)

        with jax.named_scope("comb0"):
            combine(0, new_row[0])
        with jax.named_scope("comb1"):
            combine(1, new_row[1])
        with jax.named_scope("agwait"):
            wo_copy(l).wait()
            drain(oag.at[l, pl.ds(0, NM * TU)], og_r)

        with jax.named_scope("oproj"):
            for b in range(NP):
                cols = slice(b * CB, (b + 1) * CB)
                a_s[:, cols] = (xs[:, cols] + dot(oag[l], wob[:, cols])).astype(BF).astype(F32)

            @pl.when(more)
            def _():
                wo_copy(l + 1).start()

            u = rms_norm(a_s[...]).astype(BF)
            for b in range(NP):
                cols = slice(b * CB, (b + 1) * CB)
                uperm[l, :, cols] = dot(dmat, u[:, cols]).astype(BF)
            for r in range(1, NR):
                dis_send(r).start()
            xin[l, 0:RE, :] = uperm[l, pl.ds(pl.multiple_of(e * RE, RE), RE), :]

        with jax.named_scope("gates"):
            lg3 = lax.dot_general(wr3, u, NT, preferred_element_type=F32)
            lg = lg3[0:NEX] + lg3[NEX:2 * NEX] + lg3[2 * NEX:3 * NEX]
            picked = [jnp.sum(jnp.where(ecol == idb[l, k:k + 1, :], lg, 0.0), axis=0, keepdims=True)
                      for k in range(K)]
            gtop = picked[0]
            for k in range(1, K):
                gtop = jnp.maximum(gtop, picked[k])
            ex = [jnp.exp(v - gtop) for v in picked]
            tot = ex[0]
            for k in range(1, K):
                tot = tot + ex[k]
            grow = jnp.concatenate([v / tot for v in ex], axis=1)
            gcol = jnp.broadcast_to(grow, (SLOTS, SLOTS)).T[:, 0:1]
            drain(w1b, ld_sem.at[3])
            drain(w3b, ld_sem.at[4])

        def up(g):
            r0, r1 = max(1, ups[g][0]), ups[g][1]
            drain(xin.at[l, pl.ds(r0 * RE, (r1 - r0) * RE)], dis_r.at[g])
            rows = pl.ds(ups[g][0] * RE, (r1 - ups[g][0]) * RE)
            xe = xin[l, rows]
            f0 = 0
            while f0 < FF:
                fw = min(BW, FF - f0)
                h1 = dot(xe, w1b[:, f0:f0 + fw])
                h3 = dot(xe, w3b[:, f0:f0 + fw])
                act[rows, f0:f0 + fw] = (h1 * jax.nn.sigmoid(h1) * h3).astype(BF)
                f0 += fw

        def down(g):
            for d in (2, 1, 3, 0):
                ys[l, (d + NP - 1) % NP, grows(g)] = dot(act[grows(g)], w2b[pool_of(d)])
            for d in (2, 1, 3):
                ys_send(g, d).start()

        def finish(g):
            drain(yrecv.at[l, :, grows(g)], ys_r.at[g])
            tot = ys[l, NP - 1, grows(g)]
            for d in range(1, NP):
                tot = tot + yrecv[l, d - 1, grows(g)]
            ybf[l, grows(g)] = tot.astype(BF)
            for dp_ in (2, 1, 3, 0):
                for r in range(groups[g][1] - 1, groups[g][0] - 1, -1):
                    if dp_ or r:
                        ret_send(dp_, r).start()
            if g == 0:
                yret[l, pl.ds(pl.multiple_of(p * SLOTS + e * RE, RE), RE), :] = ybf[l, 0:RE, :]

        for g in range(NG):
            if g < len(ups):
                with jax.named_scope(f"up{g}"):
                    up(g)
            if g == 0:
                drain(w2b, ld_sem.at[5])
            with jax.named_scope(f"down{g}"):
                down(g)

        @pl.when(more)
        def _():
            up_load(l + 1)
            down_load(l + 1)

        for g in range(NG):
            with jax.named_scope(f"finish{g}"):
                finish(g)

        all_ret = yret.at[l, pl.ds(0, (NP * NE - 1) * RE)]
        with jax.named_scope("retwait"):
            drain(all_ret, ret_r)

        with jax.named_scope("gsum"):
            for b in range(NP):
                cols = slice(b * CB, (b + 1) * CB)
                yp = dot(rmat, yret[l, b * SLOTS:(b + 1) * SLOTS]) * gcol
                mixed = yp[0:T]
                for k in range(1, K):
                    mixed = mixed + yp[k * T:(k + 1) * T]
                xs[:, cols] = (a_s[:, cols] + mixed).astype(BF).astype(F32)

        drain(msg.at[l, pl.ds(0, NM)], att_s)
        drain(oag.at[l, pl.ds(0, NM * TU)], og_s)
        drain(uperm.at[l, pl.ds(0, (NR - 1) * RE)], dis_s)
        for g in range(NG):
            drain(ys.at[l, pl.ds(0, NP - 1), grows(g)], ys_s.at[g])
        drain(all_ret, ret_s)
        return carry

    lax.fori_loop(0, L, layer, 0)
    out_ref[...] = xs[...].astype(BF)


def solution(mesh):
    tok_spec = P(("dp", "ep"), None)
    cache_spec = P(None, ("dp", "ep"), "pool", None, None)
    up_spec = P(None, "ep", None, "pool")
    down_spec = P(None, "ep", "pool", None)
    in_specs = (tok_spec, cache_spec, cache_spec, P(("dp", "ep")), P(), P(), P(), P(), P(),
                P(None, ("dp", "ep"), None), up_spec, up_spec, down_spec)
    NP, NE = mesh.shape["pool"], mesh.shape["ep"]

    def body(hidden, k_cache, v_cache, cache_len, w_q, w_k, w_v, w_o, w_router, ids, w_one, w_three, w_two):
        L = w_q.shape[0]
        T, D = hidden.shape
        S, G, HD = k_cache.shape[2:]
        NH = w_q.shape[2] // HD
        K = ids.shape[2]
        FF = w_one.shape[3]
        TC = T // NP
        SLOTS, CB, ROWS, SG, UR = T * K, D // NP, TC * NH, S * G, TC // 2 * NH
        assert w_one.shape[1] == 1 and SLOTS == HD and ROWS == HD and w_router.shape[2] == 8 and NP == 4 and G == 2
        dims = (L, T, D, S, G, HD, NH, NP, NE, TC, K, FF)
        kc = k_cache.reshape(L, T, SG, HD)
        vc = v_cache.reshape(L, T, SG, HD)
        wr_t = jnp.swapaxes(w_router, 1, 2)
        ids_t = jnp.swapaxes(ids, 1, 2)
        NG = 4
        V = pltpu.VMEM
        dma = pltpu.SemaphoreType.DMA
        anyspec = pl.BlockSpec(memory_space=pl.ANY)
        vspec = pl.BlockSpec(memory_space=pltpu.VMEM)
        scratch = [
            pltpu.SMEM((T,), jnp.int32),
            V((T, D), BF), V((T, D), F32), V((T, D), BF), V(ids_t.shape, jnp.int32), V(wr_t.shape, F32),
            V((D, NH * HD), BF), V((2, D, G * HD), BF), V((2 * NP, 2, TC // 2, SG, HD), BF), V((D, D), BF),
            V((D, FF), BF), V((D, FF), BF), V((NP, FF, CB), BF),
            V((T * NH, HD), F32), V((T, 2 * G * HD), F32), V((ROWS, HD), F32), V((ROWS, HD), F32),
            V((ROWS, HD), F32), V((L, 2 * NP, UR + 2, HD), F32), V((L, 2 * NP - 2, UR + 2, HD), F32),
            V((UR, HD), F32), V((L, T, NH * HD), BF),
            V((T, D), F32), V((L, SLOTS, D), BF), V((L, SLOTS, D), BF), V((SLOTS, FF), BF),
            V((L, NP, SLOTS, CB), F32), V((L, NP - 1, SLOTS, CB), F32),
            V((L, SLOTS, CB), BF), V((L, NP * SLOTS, CB), BF),
            dma((10,)), dma((2 * NP,)), dma, dma((2,)), dma, dma, dma, dma((NG,)), dma((NG,)), dma((NG,)), dma, dma,
        ]
        return pl.pallas_call(
            functools.partial(layers_kernel, dims),
            out_shape=pltpu.VMEM((T, D), BF),
            in_specs=[anyspec, anyspec, anyspec, anyspec, anyspec, anyspec, anyspec,
                      anyspec, anyspec, anyspec, anyspec, anyspec, anyspec],
            out_specs=vspec,
            scratch_shapes=scratch,
            name="moe_layers",
            compiler_params=pltpu.CompilerParams(collective_id=0, has_side_effects=True,
                                                 vmem_limit_bytes=60 * 1024 * 1024),
        )(cache_len, hidden, ids_t, kc, vc, w_q, w_k, w_v, w_o, wr_t, w_one, w_three, w_two)

    return jax.shard_map(body, mesh=mesh, in_specs=in_specs, out_specs=tok_spec, check_vma=False)
```

```python
import functools

import jax
import jax.numpy as jnp
from jax import lax
from jax.experimental import pallas as pl
from jax.experimental.pallas import tpu as pltpu
from jax.sharding import PartitionSpec as P

MESH = pl.DeviceIdType.MESH
NORM_EPS = 1e-6
NEG = -1e30
BF = jnp.bfloat16
F32 = jnp.float32
NT = (((1,), (1,)), ((), ()))


def rms_norm(v):
    return v * lax.rsqrt(jnp.mean(v * v, axis=-1, keepdims=True) + NORM_EPS)


def dot(a, b):
    return jnp.dot(a, b, preferred_element_type=F32)


def layers_kernel(dims, len_hbm, x_hbm, ids_hbm, k_hbm, v_hbm, wq_hbm, wk_hbm, wv_hbm, wo_hbm, wr_hbm,
                  w1_hbm, w3_hbm, w2_hbm, out_ref,
                  len_ref, xb, xs, hb, idb, wrb, wqb, wkvb, kvbuf, wob, w1b, w3b, w2b, qrows, kvs, kx, vx, zst, msg, arx, orow, oag,
                  a_s, uperm, xin, act, ys, yrecv, ybf, yret,
                  ld_sem, kv_sem, att_s, att_r, og_s, og_r, dis_s, dis_r, ys_s, ys_r, ret_s, ret_r):
    L, T, D, S, G, HD, NH, NP, NE, TC, K, FF = dims
    QG = NH // G
    SLOTS = T * K
    RE = SLOTS // NE
    CB = D // NP
    SG = S * G
    QW = NH * HD
    KW = G * HD
    TU = TC // 2
    TH = T // 2
    UR = TU * NH
    NU = 2 * NP
    NM = 2 * (NP - 1)
    NX = NE // 2
    BW = 2 * HD
    scale = HD ** -0.5
    p = lax.axis_index("pool")
    e = lax.axis_index("ep")
    chip = lax.div(e, 2)
    core = lax.rem(e, 2)

    def pool_of(d):
        return lax.rem(p + d, NP)

    rel = [(0, 0), (0, 1), (1, 0), (NX - 1, 0)] + [(dx, dc) for dx in range(2, NX - 1) for dc in range(2)] + [(1, 1), (NX - 1, 1)]
    NR = len(rel)
    ups = [(0, 2), (2, 4), (4, NR)]
    groups = [(0, 2), (2, 4), (4, 6), (6, NR)]
    NG = len(groups)
    group_of = [next(g for g in range(len(ups)) if ups[g][0] <= r < ups[g][1]) for r in range(NR)]

    def ep_sender(r):
        return lax.rem(chip + rel[r][0], NX) * 2 + lax.rem(core + rel[r][1], 2)

    def ep_receiver(r):
        return lax.rem(chip + NX - rel[r][0], NX) * 2 + lax.rem(core + rel[r][1], 2)

    def wq_load(l):
        for b in range(2):
            rows = pl.ds(b * (D // 2), D // 2)
            pltpu.make_async_copy(wq_hbm.at[l, rows], wqb.at[rows], ld_sem.at[0]).start()

    def wkv_load(l):
        pltpu.make_async_copy(wk_hbm.at[l], wkvb.at[0], ld_sem.at[1]).start()
        pltpu.make_async_copy(wv_hbm.at[l], wkvb.at[1], ld_sem.at[1]).start()

    def drain(ref, sem):
        pltpu.make_async_copy(ref, ref, sem).wait()

    def unit(it, un):
        z = (it + 1) // 2 % 2
        half = z * (it - 1) + (1 - z) * un
        away = z * (1 + 2 * un) + (1 - z) * (2 - 2 * (it // 3))
        return half, away

    def unit_tok(it, un):
        half, away = unit(it, un)
        return half * TH + lax.rem(p + away, NP) * TU

    def kv_load(l, it, un):
        n = 2 * it + un
        tok = pl.ds(pl.multiple_of(unit_tok(it, un), TU), TU)
        pltpu.make_async_copy(k_hbm.at[l, tok], kvbuf.at[n, 0], kv_sem.at[n]).start()
        pltpu.make_async_copy(v_hbm.at[l, tok], kvbuf.at[n, 1], kv_sem.at[n]).start()

    def wo_copy(l):
        return pltpu.make_async_copy(wo_hbm.at[l], wob, ld_sem.at[2])

    def up_load(l):
        pltpu.make_async_copy(w1_hbm.at[l, 0], w1b, ld_sem.at[3]).start()
        pltpu.make_async_copy(w3_hbm.at[l, 0], w3b, ld_sem.at[4]).start()

    def down_load(l):
        for q in range(NP):
            pltpu.make_async_copy(w2_hbm.at[l, 0, :, pl.ds(q * CB, CB)], w2b.at[q], ld_sem.at[5]).start()

    small = [pltpu.make_async_copy(x_hbm, xb, ld_sem.at[6]),
             pltpu.make_async_copy(ids_hbm, idb, ld_sem.at[7]),
             pltpu.make_async_copy(wr_hbm, wrb, ld_sem.at[8]),
             pltpu.make_async_copy(len_hbm, len_ref, ld_sem.at[9])]
    small[0].start()
    small[3].start()
    wq_load(0)
    for un in range(2):
        kv_load(0, 0, un)
    small[1].start()
    small[2].start()

    barrier = pltpu.get_barrier_semaphore()
    for dp_ in range(NP):
        for de in range(NE):
            if dp_ or de:
                pl.semaphore_signal(barrier, inc=1,
                                    device_id={"pool": pool_of(dp_), "ep": lax.rem(e + de, NE)},
                                    device_id_type=MESH)

    hrow = lax.broadcasted_iota(jnp.int32, (NH, SG), 0)
    pcol = lax.broadcasted_iota(jnp.int32, (NH, SG), 1)
    posm = jnp.where(lax.rem(pcol, G) == lax.div(hrow, QG), lax.div(pcol, G), jnp.int32(1 << 30))
    lane = lax.broadcasted_iota(jnp.int32, (NH, HD), 1)
    hsub = lax.broadcasted_iota(jnp.int32, (NH, HD), 0)
    NEX = wrb.shape[1]
    hlane = lax.rem(lane, UR)
    row_lane = lax.rem(lax.broadcasted_iota(jnp.int32, (UR, HD), 1), UR)
    row_id = lax.broadcasted_iota(jnp.int32, (UR, HD), 0)
    ecol = lax.broadcasted_iota(jnp.int32, (NEX, T), 0)

    zst[...] = jnp.zeros_like(zst)
    small[0].wait()
    xs[...] = xb[...].astype(F32)

    def layer(l, carry):
        more = l + 1 < L
        first = l == 0

        def att_send(it, un):
            half, away = unit(it, un)
            return pltpu.make_async_remote_copy(
                src_ref=msg.at[l, 2 * it + un], dst_ref=arx.at[l, half * (NP - 1) + away - 1], send_sem=att_s,
                recv_sem=att_r.at[half],
                device_id={"pool": pool_of(away), "ep": e}, device_id_type=MESH)

        def own_tok(half):
            return pl.ds(pl.multiple_of(half * TH + p * TU, TU), TU)

        def og_send(half, d):
            return pltpu.make_async_remote_copy(
                src_ref=oag.at[l, own_tok(half)], dst_ref=oag.at[l, own_tok(half)], send_sem=og_s, recv_sem=og_r,
                device_id={"pool": pool_of(d), "ep": e}, device_id_type=MESH)

        def dis_send(r):
            dst = ep_receiver(r)
            return pltpu.make_async_remote_copy(
                src_ref=uperm.at[l, pl.ds(pl.multiple_of(dst * RE, RE), RE)], dst_ref=xin.at[l, pl.ds(r * RE, RE)],
                send_sem=dis_s, recv_sem=dis_r.at[group_of[r]],
                device_id={"pool": p, "ep": dst}, device_id_type=MESH)

        def grows(g):
            return pl.ds(groups[g][0] * RE, (groups[g][1] - groups[g][0]) * RE)

        def ys_send(g, d):
            return pltpu.make_async_remote_copy(
                src_ref=ys.at[l, d - 1, grows(g)], dst_ref=yrecv.at[l, d - 1, grows(g)], send_sem=ys_s.at[g],
                recv_sem=ys_r.at[g], device_id={"pool": pool_of(d), "ep": e}, device_id_type=MESH)

        def ret_send(dp_, r):
            dst = ep_sender(r)
            return pltpu.make_async_remote_copy(
                src_ref=ybf.at[l, pl.ds(r * RE, RE)],
                dst_ref=yret.at[l, pl.ds(pl.multiple_of(p * SLOTS + e * RE, RE), RE)], send_sem=ret_s, recv_sem=ret_r,
                device_id={"pool": pool_of(dp_), "ep": dst}, device_id_type=MESH)

        with jax.named_scope("qkv"):
            hn = rms_norm(xs[...]).astype(BF)
            drain(wqb, ld_sem.at[0])

            @pl.when(first)
            def _():
                small[3].wait()

            for b in range(QW // BW):
                r = dot(hn, wqb[:, b * BW:(b + 1) * BW]).astype(BF).astype(F32)
                for j in range(2):
                    qrows[pl.ds(2 * b + j, T, stride=NH), :] = r[:, j * HD:(j + 1) * HD]
            hb[...] = hn

            @pl.when(first)
            def _():
                for un in range(2):
                    kv_load(l, 1, un)
                for un in range(2):
                    kv_load(l, 2, un)

        def new_scores(half):
            q0 = pl.multiple_of((half * TH + p * TU) * NH, UR)
            krow = pl.ds(half * UR, UR)
            s_new = jnp.sum(qrows[pl.ds(q0, UR), :] * kx[krow, :], axis=1, keepdims=True) * scale
            return jnp.sum(jnp.where(row_lane == row_id, s_new, 0.0), axis=0, keepdims=True)

        def combine(half, s_new):
            m0 = half * (NP - 1)
            drain(arx.at[l, pl.ds(m0, NP - 1)], att_r.at[half])
            parts = [arx.at[l, m0 + i] for i in range(NP - 1)] + [msg.at[l, 2 * (NP - 1) + half]]
            ms = [ref[UR:UR + 1, :] for ref in parts]
            top = s_new
            for m in ms:
                top = jnp.maximum(top, m)
            w = [jnp.exp(m - top) for m in ms] + [jnp.exp(s_new - top)]
            den = w[NP]
            for i in range(NP):
                den = den + w[i] * parts[i][UR + 1:UR + 2, :]
            inv = 1.0 / den
            for i in range(NP + 1):
                zst[i:i + 1, :] = w[i] * inv
            zc = zst[...].T
            out = zc[0:UR, NP:NP + 1] * vx[pl.ds(half * UR, UR), :]
            for i in range(NP):
                out = out + zc[0:UR, i:i + 1] * parts[i][0:UR, :]
            orow[...] = out
            for h in range(NH):
                oag[l, own_tok(half), h * HD:(h + 1) * HD] = orow[pl.ds(h, TU, stride=NH), :].astype(BF)
            for d in (2, 1, 3):
                og_send(half, d).start()

        def attend(it, send):
            for un in range(2):
                n = 2 * it + un
                drain(kvbuf.at[n], kv_sem.at[n])

            @pl.when(jnp.logical_and(first, it == 0))
            def _():
                for un in range(2):
                    kv_load(l, 3, un)

            @pl.when(jnp.logical_and(first, it == 2))
            def _():
                wkv_load(l)
                wo_copy(l).start()
                up_load(l)
                down_load(l)

            for un in range(2):
                n = 2 * it + un
                t0 = unit_tok(it, un)
                sc = []
                for j in range(TU):
                    t = t0 + j
                    qt = qrows[pl.ds(pl.multiple_of(t * NH, NH), NH), :].astype(BF)
                    s = lax.dot_general(qt, kvbuf[n, 0, j], NT, preferred_element_type=F32) * scale
                    sc.append(jnp.where(posm < len_ref[t] - p * S, s, NEG))
                mx = [jnp.max(s, axis=1, keepdims=True) for s in sc]
                pr = [jnp.exp(s - m) for s, m in zip(sc, mx)]
                ls = [jnp.sum(q, axis=1, keepdims=True) for q in pr]
                mrow = jnp.zeros((NH, HD), F32)
                lrow = jnp.zeros((NH, HD), F32)
                for j in range(TU):
                    msg[l, n, j * NH:(j + 1) * NH, :] = dot(pr[j].astype(BF), kvbuf[n, 1, j])
                    here = hlane == hsub + j * NH
                    mrow = jnp.where(here, mx[j], mrow)
                    lrow = jnp.where(here, ls[j], lrow)
                msg[l, n, UR:UR + 1, :] = jnp.sum(mrow, axis=0, keepdims=True)
                msg[l, n, UR + 1:UR + 2, :] = jnp.sum(lrow, axis=0, keepdims=True)
                if send and un == 0:
                    @pl.when(jnp.logical_and(first, it == 0))
                    def _():
                        pl.semaphore_wait(barrier, NP * NE - 1)

                if send:
                    att_send(it, un).start()

        def chunk(it, c2):
            attend(it, True)
            return c2

        with jax.named_scope("attn"):
            lax.fori_loop(0, NP - 1, chunk, 0)
            attend(NP - 1, False)

        with jax.named_scope("kvproj"):
            drain(wkvb, ld_sem.at[1])
            for b in range(2):
                kvs[:, b * KW:(b + 1) * KW] = dot(hb[...], wkvb[b]).astype(BF).astype(F32)

            for half in range(2):
                for h in range(NH):
                    g = h // QG
                    kx[pl.ds(half * UR + h, TU, stride=NH), :] = kvs[own_tok(half), g * HD:(g + 1) * HD]
                    vx[pl.ds(half * UR + h, TU, stride=NH), :] = kvs[own_tok(half), KW + g * HD:KW + (g + 1) * HD]

        new_row = [new_scores(half) for half in range(2)]

        @pl.when(first)
        def _():
            small[1].wait()
            small[2].wait()

        with jax.named_scope("tables"):
            slot_col = lax.broadcasted_iota(jnp.int32, (SLOTS, SLOTS), 0)
            pair_row = lax.broadcasted_iota(jnp.int32, (SLOTS, SLOTS), 1)
            upper = (slot_col < pair_row).astype(F32).astype(BF)
            want_rank = lax.rem(slot_col, RE).astype(F32)
            idrow = jnp.concatenate([idb[l, k:k + 1, :] for k in range(K)], axis=1)
            same = (jnp.broadcast_to(idrow, (SLOTS, SLOTS)) == lax.div(slot_col, RE))
            rank = dot(same.astype(F32).astype(BF), upper)
            pick = jnp.where(jnp.logical_and(same, rank == want_rank), 1.0, 0.0).astype(F32)
            rmat = pick.T.astype(BF)
            dmat = pick[:, 0:T]
            for k in range(1, K):
                dmat = dmat + pick[:, k * T:(k + 1) * T]
            dmat = dmat.astype(BF)
            wr = wrb[l]
            hi = wr.astype(BF).astype(F32)
            mid = (wr - hi).astype(BF).astype(F32)
            lo = wr - hi - mid
            wr3 = jnp.concatenate([hi, mid, lo, jnp.zeros_like(lo)], axis=0).astype(BF)

        with jax.named_scope("comb0"):
            combine(0, new_row[0])
        with jax.named_scope("comb1"):
            combine(1, new_row[1])
        with jax.named_scope("agwait"):
            wo_copy(l).wait()
            drain(oag.at[l, pl.ds(0, NM * TU)], og_r)

        with jax.named_scope("oproj"):
            for b in range(NP):
                cols = slice(b * CB, (b + 1) * CB)
                a_s[:, cols] = (xs[:, cols] + dot(oag[l], wob[:, cols])).astype(BF).astype(F32)

            @pl.when(more)
            def _():
                wo_copy(l + 1).start()

            u = rms_norm(a_s[...]).astype(BF)
            for b in range(NP):
                cols = slice(b * CB, (b + 1) * CB)
                uperm[l, :, cols] = dot(dmat, u[:, cols]).astype(BF)
            for r in range(1, NR):
                dis_send(r).start()
            xin[l, 0:RE, :] = uperm[l, pl.ds(pl.multiple_of(e * RE, RE), RE), :]

        with jax.named_scope("gates"):
            lg3 = lax.dot_general(wr3, u, NT, preferred_element_type=F32)
            lg = lg3[0:NEX] + lg3[NEX:2 * NEX] + lg3[2 * NEX:3 * NEX]
            picked = [jnp.sum(jnp.where(ecol == idb[l, k:k + 1, :], lg, 0.0), axis=0, keepdims=True)
                      for k in range(K)]
            gtop = picked[0]
            for k in range(1, K):
                gtop = jnp.maximum(gtop, picked[k])
            ex = [jnp.exp(v - gtop) for v in picked]
            tot = ex[0]
            for k in range(1, K):
                tot = tot + ex[k]
            grow = jnp.concatenate([v / tot for v in ex], axis=1)
            gcol = jnp.broadcast_to(grow, (SLOTS, SLOTS)).T[:, 0:1]
            drain(w1b, ld_sem.at[3])
            drain(w3b, ld_sem.at[4])

        @pl.when(more)
        def _():
            wq_load(l + 1)
            wkv_load(l + 1)
            for n in range(NU):
                kv_load(l + 1, n // 2, n % 2)

        def up(g):
            r0, r1 = max(1, ups[g][0]), ups[g][1]
            drain(xin.at[l, pl.ds(r0 * RE, (r1 - r0) * RE)], dis_r.at[g])
            rows = pl.ds(ups[g][0] * RE, (r1 - ups[g][0]) * RE)
            xe = xin[l, rows]
            f0 = 0
            while f0 < FF:
                fw = min(BW, FF - f0)
                h1 = dot(xe, w1b[:, f0:f0 + fw])
                h3 = dot(xe, w3b[:, f0:f0 + fw])
                act[rows, f0:f0 + fw] = (h1 * jax.nn.sigmoid(h1) * h3).astype(BF)
                f0 += fw

        def down(g):
            for d in (2, 1, 3, 0):
                ys[l, (d + NP - 1) % NP, grows(g)] = dot(act[grows(g)], w2b[pool_of(d)])
            for d in (2, 1, 3):
                ys_send(g, d).start()

        def finish(g):
            drain(yrecv.at[l, :, grows(g)], ys_r.at[g])
            tot = ys[l, NP - 1, grows(g)]
            for d in range(1, NP):
                tot = tot + yrecv[l, d - 1, grows(g)]
            ybf[l, grows(g)] = tot.astype(BF)
            for dp_ in (2, 1, 3, 0):
                for r in range(groups[g][1] - 1, groups[g][0] - 1, -1):
                    if dp_ or r:
                        ret_send(dp_, r).start()
            if g == 0:
                yret[l, pl.ds(pl.multiple_of(p * SLOTS + e * RE, RE), RE), :] = ybf[l, 0:RE, :]

        for g in range(NG):
            if g < len(ups):
                with jax.named_scope(f"up{g}"):
                    up(g)
            if g == 0:
                drain(w2b, ld_sem.at[5])
            with jax.named_scope(f"down{g}"):
                down(g)

        @pl.when(more)
        def _():
            up_load(l + 1)
            down_load(l + 1)

        for g in range(NG):
            with jax.named_scope(f"finish{g}"):
                finish(g)

        all_ret = yret.at[l, pl.ds(0, (NP * NE - 1) * RE)]
        with jax.named_scope("retwait"):
            drain(all_ret, ret_r)

        with jax.named_scope("gsum"):
            for b in range(NP):
                cols = slice(b * CB, (b + 1) * CB)
                yp = dot(rmat, yret[l, b * SLOTS:(b + 1) * SLOTS]) * gcol
                mixed = yp[0:T]
                for k in range(1, K):
                    mixed = mixed + yp[k * T:(k + 1) * T]
                xs[:, cols] = (a_s[:, cols] + mixed).astype(BF).astype(F32)

        drain(msg.at[l, pl.ds(0, NM)], att_s)
        drain(oag.at[l, pl.ds(0, NM * TU)], og_s)
        drain(uperm.at[l, pl.ds(0, (NR - 1) * RE)], dis_s)
        for g in range(NG):
            drain(ys.at[l, pl.ds(0, NP - 1), grows(g)], ys_s.at[g])
        drain(all_ret, ret_s)
        return carry

    lax.fori_loop(0, L, layer, 0)
    out_ref[...] = xs[...].astype(BF)


def solution(mesh):
    tok_spec = P(("dp", "ep"), None)
    cache_spec = P(None, ("dp", "ep"), "pool", None, None)
    up_spec = P(None, "ep", None, "pool")
    down_spec = P(None, "ep", "pool", None)
    in_specs = (tok_spec, cache_spec, cache_spec, P(("dp", "ep")), P(), P(), P(), P(), P(),
                P(None, ("dp", "ep"), None), up_spec, up_spec, down_spec)
    NP, NE = mesh.shape["pool"], mesh.shape["ep"]

    def body(hidden, k_cache, v_cache, cache_len, w_q, w_k, w_v, w_o, w_router, ids, w_one, w_three, w_two):
        L = w_q.shape[0]
        T, D = hidden.shape
        S, G, HD = k_cache.shape[2:]
        NH = w_q.shape[2] // HD
        K = ids.shape[2]
        FF = w_one.shape[3]
        TC = T // NP
        SLOTS, CB, ROWS, SG, UR = T * K, D // NP, TC * NH, S * G, TC // 2 * NH
        assert w_one.shape[1] == 1 and SLOTS == HD and ROWS == HD and w_router.shape[2] == 8 and NP == 4 and G == 2
        dims = (L, T, D, S, G, HD, NH, NP, NE, TC, K, FF)
        kc = k_cache.reshape(L, T, SG, HD)
        vc = v_cache.reshape(L, T, SG, HD)
        wr_t = jnp.swapaxes(w_router, 1, 2)
        ids_t = jnp.swapaxes(ids, 1, 2)
        NG = 4
        V = pltpu.VMEM
        dma = pltpu.SemaphoreType.DMA
        anyspec = pl.BlockSpec(memory_space=pl.ANY)
        vspec = pl.BlockSpec(memory_space=pltpu.VMEM)
        scratch = [
            pltpu.SMEM((T,), jnp.int32),
            V((T, D), BF), V((T, D), F32), V((T, D), BF), V(ids_t.shape, jnp.int32), V(wr_t.shape, F32),
            V((D, NH * HD), BF), V((2, D, G * HD), BF), V((2 * NP, 2, TC // 2, SG, HD), BF), V((D, D), BF),
            V((D, FF), BF), V((D, FF), BF), V((NP, FF, CB), BF),
            V((T * NH, HD), F32), V((T, 2 * G * HD), F32), V((ROWS, HD), F32), V((ROWS, HD), F32),
            V((ROWS, HD), F32), V((L, 2 * NP, UR + 2, HD), F32), V((L, 2 * NP - 2, UR + 2, HD), F32),
            V((UR, HD), F32), V((L, T, NH * HD), BF),
            V((T, D), F32), V((L, SLOTS, D), BF), V((L, SLOTS, D), BF), V((SLOTS, FF), BF),
            V((L, NP, SLOTS, CB), F32), V((L, NP - 1, SLOTS, CB), F32),
            V((L, SLOTS, CB), BF), V((L, NP * SLOTS, CB), BF),
            dma((10,)), dma((2 * NP,)), dma, dma((2,)), dma, dma, dma, dma((NG,)), dma((NG,)), dma((NG,)), dma, dma,
        ]
        return pl.pallas_call(
            functools.partial(layers_kernel, dims),
            out_shape=pltpu.VMEM((T, D), BF),
            in_specs=[anyspec, anyspec, anyspec, anyspec, anyspec, anyspec, anyspec,
                      anyspec, anyspec, anyspec, anyspec, anyspec, anyspec],
            out_specs=vspec,
            scratch_shapes=scratch,
            name="moe_layers",
            compiler_params=pltpu.CompilerParams(collective_id=0, has_side_effects=True,
                                                 vmem_limit_bytes=60 * 1024 * 1024),
        )(cache_len, hidden, ids_t, kc, vc, w_q, w_k, w_v, w_o, wr_t, w_one, w_three, w_two)

    return jax.shard_map(body, mesh=mesh, in_specs=in_specs, out_specs=tok_spec, check_vma=False)
```
